32 devices in a mesh: wide: 8 (over z, x), narrow: 4 (over y, core).
Axes of the slice: x: 2, y: 2, z: 4, core: 2. Of those that a mesh axis runs over, the one named last changes fastest.
Arguments:
- tokens: bfloat16 [4096, 1024], P(('wide', 'narrow')), may hold values from -6 to 6
- cotangent: bfloat16 [4096, 1024], P(('wide', 'narrow')), may hold values from -0.0625 to 0.0625
- segment_ids: int32 [32, 128], P(('wide', 'narrow')), may hold values from 0 to 7, never falling along the last dimension, each value on 1 to 32 neighbouring positions
- w_qkv: float32 [1024, 3072], P(('wide', 'narrow')), may hold values from -0.1875 to 0.1875
- w_out: float32 [1024, 1024], P(('wide', 'narrow')), may hold values from -0.375 to 0.375
- w_up: float32 [1024, 4096], P(('wide', 'narrow')), may hold values from -0.1875 to 0.1875
- w_down: float32 [4096, 1024], P(('wide', 'narrow')), may hold values from -0.09375 to 0.09375
- vectors: float32 [1024, 12], P(('wide', 'narrow')), as said below
- moments_qkv: float32 [2, 1024, 3072], P(None, ('wide', 'narrow')), as said below
- moments_out: float32 [2, 1024, 1024], P(None, ('wide', 'narrow')), as said below
- moments_up: float32 [2, 1024, 4096], P(None, ('wide', 'narrow')), as said below
- moments_down: float32 [2, 4096, 1024], P(None, ('wide', 'narrow')), as said below
- moments_vec: float32 [2, 1024, 12], P(None, ('wide', 'narrow')), as said below
Outputs:
- block_out: bfloat16 [4096, 1024], P(('wide', 'narrow'))
- input_grad: float32 [4096, 1024], P(('wide', 'narrow'))
- new_qkv: float32 [1024, 3072], P(('wide', 'narrow'))
- new_out: float32 [1024, 1024], P(('wide', 'narrow'))
- new_up: float32 [1024, 4096], P(('wide', 'narrow'))
- new_down: float32 [4096, 1024], P(('wide', 'narrow'))
- new_vectors: float32 [1024, 12], P(('wide', 'narrow'))
- state_qkv: float32 [2, 1024, 3072], P(None, ('wide', 'narrow'))
- state_out: float32 [2, 1024, 1024], P(None, ('wide', 'narrow'))
- state_up: float32 [2, 1024, 4096], P(None, ('wide', 'narrow'))
- state_down: float32 [2, 4096, 1024], P(None, ('wide', 'narrow'))
- state_vectors: float32 [2, 1024, 12], P(None, ('wide', 'narrow'))
- copy_qkv: bfloat16 [1024, 3072], P(('wide', 'narrow'))
- copy_out: bfloat16 [1024, 1024], P(('wide', 'narrow'))
- copy_up: bfloat16 [1024, 4096], P(('wide', 'narrow'))
- copy_down: bfloat16 [4096, 1024], P(('wide', 'narrow'))
- copy_vectors: bfloat16 [1024, 12], P(('wide', 'narrow'))
The draws below stay inside these ranges and needn't reach their ends.
Inputs may be any that keep to these rules, and one draw needn't show every extreme that they name: `segment_ids`: in each sequence the ids never fall, every id is used, each segment has 1 to 32 patches and one has exactly 32. `vectors`: columns 0 and 5 are positive gains; the others are biases of both signs. `moments_qkv`: the second slice is positive. `moments_out`: the second slice is positive. `moments_up`: the second slice is positive. `moments_down`: the second slice is positive. `moments_vec`: the second slice is positive.
All inputs are finite; a program needn't handle non-finite values.
Results may differ from the reference program's by a relative error of at most 0.02.
Values may be sent and summed in bfloat16 or wider, within the bound.
A program may use at most 256 MiB of HBM per device.

```python
import math
from functools import partial
import jax
import jax.numpy as jnp
import numpy as np
from jax import lax

D = 1024
HEADS = 16
FF = 4096
NVEC = 12
SEQ = 128
SEGS = 8
SEG_MOST = 32
STEP = 3
NSEQ = 32
TOKENS = 4096


def draw_vectors(key, part):
    spread_part = jnp.clip(jax.random.normal(jax.random.fold_in(key, 1), (D, NVEC), jnp.float32), -5.0, 5.0) * 0.2
    gain_values = jax.random.uniform(jax.random.fold_in(key, 2), (D, NVEC), jnp.float32, 0.6, 1.4)
    column = jnp.arange(NVEC)[None, :]
    return jnp.where((column == 0) | (column == 5), gain_values, spread_part)


def moment_pair(key, shape, grad_scale):
    first_moment = grad_scale * jnp.clip(jax.random.normal(jax.random.fold_in(key, 11), shape, jnp.float32), -4.0, 4.0)
    factor = jnp.exp(jax.random.uniform(jax.random.fold_in(key, 12), shape, jnp.float32, -math.log(2.0), math.log(2.0)))
    second_moment = 2.0 * factor * grad_scale * grad_scale
    return jnp.stack([first_moment, second_moment])


def draw_moments_qkv(key, part):
    return moment_pair(key, (D, 3 * D), 0.3 * 0.7)


def draw_moments_out(key, part):
    return moment_pair(key, (D, D), 0.3 * 0.7)


def draw_moments_up(key, part):
    return moment_pair(key, (D, FF), 0.35 * 0.7)


def draw_moments_down(key, part):
    return moment_pair(key, (FF, D), 0.65 * 0.7)


def draw_moments_vec(key, part):
    column_scale = jnp.array([0.5, 0.5, 0.33, 2.2, 1.1, 0.7, 0.7, 1.0], jnp.float32)
    up_scale = jnp.full((NVEC - 8,), 0.35, jnp.float32)
    scales = jnp.concatenate([column_scale, up_scale]) * 0.7
    return moment_pair(key, (D, NVEC), scales[None, :])


def levels(rng, dims, cuts, low, largest):
    def one(dim, blocks):
        draws = jax.random.uniform(jax.random.fold_in(jax.random.fold_in(rng, 6), dim), (blocks,), jnp.float32, low / len(cuts), largest / len(cuts))
        return jnp.repeat(jnp.exp(draws), dims[dim] // blocks).reshape((-1,) + (1,) * (len(dims) - dim - 1))

    loudness = one(*cuts[0])
    for cut in cuts[1:]:
        loudness = loudness * one(*cut)
    return loudness


def profile(number_of, total, most, slope):
    weights = [(1 << 20) // math.isqrt(grade ** slope) + 1 for grade in range(2, number_of + 1)]
    rest, holding = total - most - (number_of - 1), [1] * (number_of - 1)
    while rest > 0:
        candidates = [i for i in range(number_of - 1) if holding[i] < most]
        pool, left = sum([weights[i] for i in candidates]), rest
        for i in candidates:
            extra = min(most - holding[i], max(1, left * weights[i] // pool), rest)
            holding[i] = holding[i] + extra
            rest = rest - extra
    return np.array([most] + holding)


def uneven_parts(key, amount, total, bound, skew):
    if amount == 2:
        one = jax.random.randint(key, (), max(1, total - bound), min(bound, total - 1) + 1)
        return jnp.stack([one, total - one])
    lengths = jnp.asarray(profile(amount, total, bound, skew), jnp.int32)
    couples = (amount - 1) // 2
    source_of, sink = lengths[1:1 + 2 * couples:2], lengths[2:2 + 2 * couples:2]
    slack = jnp.minimum(source_of - 1, bound - sink)
    moved = jax.random.randint(jax.random.fold_in(key, 1), (couples,), 0, 1 << 20) % (slack + 1)
    lengths = lengths.at[1:1 + 2 * couples:2].set(source_of - moved).at[2:2 + 2 * couples:2].set(sink + moved)
    return lengths[jax.random.permutation(jax.random.fold_in(key, 2), amount)]


def centred(stream_key, shape, scale, reach, cuts=(), dtype=jnp.bfloat16):
    factor_of = levels(stream_key, shape, cuts, -0.22, 0.18) if cuts else 1.0
    values = jax.random.normal(stream_key, shape, jnp.float32) * scale * factor_of
    return jnp.minimum(jnp.maximum(values, -reach), reach).astype(dtype)


def setup_inputs(seed: int = 0) -> dict:
    arg_keys = jax.random.split(jax.random.key(seed), 14)
    return {
        "tokens": centred(arg_keys[0], (TOKENS, D), 1.0, 6.0, ((0, 32),)),
        "cotangent": centred(arg_keys[1], (TOKENS, D), (0.7 / TOKENS ** 0.5), 0.0625, ((0, 32),)),
        "segment_ids": jax.vmap(lambda own: jnp.searchsorted(jnp.cumsum(uneven_parts(own, SEGS, SEQ, SEG_MOST, 1)), jnp.arange(SEQ), side="right"))(jax.random.split(arg_keys[2], NSEQ)).reshape((NSEQ, SEQ)).astype(jnp.int32),
        "w_qkv": centred(arg_keys[3], (D, 3 * D), D ** -0.5, 0.1875, ((0, 32),), jnp.float32),
        "w_out": centred(arg_keys[4], (D, D), (D // 4) ** -0.5, 0.375, ((0, 32),), jnp.float32),
        "w_up": centred(arg_keys[5], (D, FF), D ** -0.5, 0.1875, ((0, 32),), jnp.float32),
        "w_down": centred(arg_keys[6], (FF, D), FF ** -0.5, 0.09375, ((0, 32),), jnp.float32),
        "vectors": draw_vectors(jax.random.fold_in(arg_keys[13], 71), 0),
        "moments_qkv": draw_moments_qkv(jax.random.fold_in(arg_keys[13], 71), 0),
        "moments_out": draw_moments_out(jax.random.fold_in(arg_keys[13], 71), 0),
        "moments_up": draw_moments_up(jax.random.fold_in(arg_keys[13], 71), 0),
        "moments_down": draw_moments_down(jax.random.fold_in(arg_keys[13], 71), 0),
        "moments_vec": draw_moments_vec(jax.random.fold_in(arg_keys[13], 71), 0),
    }


NORM_EPSILON = 1e-06
MASK_VALUE = -1e+30
MOMENT_DECAY = 0.5
RATE_MATRIX = 0.04
RATE_VECTOR = 0.2
WEIGHT_DECAY = 0.1
ADAM_EPSILON = 1e-08

@jax.custom_vjp
def low(v):
    return lax.optimization_barrier(v.astype(jnp.bfloat16)).astype(jnp.float32)

@jax.custom_vjp
def low_back(v):
    return v

def low_keep(v):
    return (low(v), None)

def low_pass(kept, grad):
    return (grad,)

def back_keep(v):
    return (v, None)

def back_low(kept, grad):
    return (low(grad),)
low.defvjp(low_keep, low_pass)
low_back.defvjp(back_keep, back_low)

def layer_norm(values, scale_row, offset_row):
    center = values - lax.optimization_barrier(jnp.mean(values, axis=-1, keepdims=True))
    spread = lax.optimization_barrier(jnp.mean(center * center, axis=-1, keepdims=True))
    return center * lax.rsqrt(spread + NORM_EPSILON) * scale_row + offset_row

def exact_gelu(values):
    return jax.nn.gelu(values, approximate=False)

def mat_prod(left, right):
    return jnp.einsum('gsd,df->gsf', left, right, precision=lax.Precision.HIGHEST)

def adam_update(master, moments, gradient, rate, decay):
    first_moment = MOMENT_DECAY * moments[0] + (1.0 - MOMENT_DECAY) * gradient
    second_moment = MOMENT_DECAY * moments[1] + (1.0 - MOMENT_DECAY) * gradient * gradient
    correction = 1.0 - MOMENT_DECAY ** STEP
    normalized = first_moment / correction / (jnp.sqrt(second_moment / correction) + ADAM_EPSILON)
    updated = master - rate * (normalized + decay * master)
    return (updated, jnp.stack([first_moment, second_moment]), updated.astype(jnp.bfloat16))

def forward_block(segments, inputs, qkv_weight, out_weight, up_weight, down_weight, packed):
    gain_one = packed[:, 0]
    shift_one = packed[:, 1]
    bias_query = packed[:, 2]
    bias_value = packed[:, 3]
    bias_out = packed[:, 4]
    gain_two = packed[:, 5]
    shift_two = packed[:, 6]
    bias_down = packed[:, 7]
    bias_up = packed[:, 8:].T.reshape(FF)
    head_dim = D // HEADS
    group_size, length = segments.shape
    normed_one = low(layer_norm(inputs, gain_one, shift_one))
    qkv_bias = jnp.concatenate([bias_query, jnp.zeros_like(bias_query), bias_value])
    qkv_value = low(low_back(mat_prod(normed_one, qkv_weight) + qkv_bias))
    queries = qkv_value[..., :D].reshape(group_size, length, HEADS, head_dim)
    keys_all = qkv_value[..., D:2 * D].reshape(group_size, length, HEADS, head_dim)
    values_all = qkv_value[..., 2 * D:].reshape(group_size, length, HEADS, head_dim)
    raw_scores = low_back(jnp.einsum('gqhd,gkhd->ghqk', queries, keys_all, precision=lax.Precision.HIGHEST) * head_dim ** (-0.5))
    same_segment = (segments[:, :, None] == segments[:, None, :])[:, None]
    scores = jnp.where(same_segment, raw_scores, MASK_VALUE)
    highest = lax.optimization_barrier(jnp.max(scores, axis=-1, keepdims=True))
    exp_scores = jnp.exp(scores - highest)
    soft_weights = exp_scores / lax.optimization_barrier(jnp.sum(exp_scores, axis=-1, keepdims=True))
    mixed = jnp.einsum('ghqk,gkhd->gqhd', low(soft_weights), values_all, precision=lax.Precision.HIGHEST)
    mixed = low(low_back(mixed)).reshape(group_size, length, D)
    resid_one = inputs + low_back(mat_prod(mixed, out_weight)) + bias_out
    normed_two = low(layer_norm(resid_one, gain_two, shift_two))
    hidden_pre = low_back(mat_prod(normed_two, up_weight) + bias_up)
    hidden_act = low(exact_gelu(hidden_pre))
    return resid_one + mat_prod(hidden_act, down_weight) + bias_down

def reference(tokens, cotangent, segment_ids, w_qkv, w_out, w_up, w_down, vectors, moments_qkv, moments_out, moments_up, moments_down, moments_vec):
    group_size = min(NSEQ, max(1, 4096 // SEQ))
    group_count = NSEQ // group_size
    weights_low = (low(w_qkv), low(w_out), low(w_up), low(w_down), low(vectors))
    input_groups = tokens.astype(jnp.float32).reshape(group_count, group_size, SEQ, D)
    back_groups = cotangent.astype(jnp.float32).reshape(group_count, group_size, SEQ, D)
    segment_groups = segment_ids.reshape(group_count, group_size, SEQ)

    def step_group(totals, pieces):
        input_group, back_group, segment_group = pieces
        outputs, pull_back = jax.vjp(partial(forward_block, segment_group), input_group, weights_low[0], weights_low[1], weights_low[2], weights_low[3], weights_low[4])
        gradients = pull_back(back_group)
        totals = tuple((total + gradient for total, gradient in zip(totals, gradients[1:])))
        return (totals, (outputs.astype(jnp.bfloat16), gradients[0]))
    start_totals = tuple((jnp.zeros_like(weight) for weight in weights_low))
    totals, (outputs, input_grads) = lax.scan(step_group, start_totals, (input_groups, back_groups, segment_groups))
    block_out = outputs.reshape(NSEQ * SEQ, D)
    input_grad = input_grads.reshape(NSEQ * SEQ, D)
    new_qkv, state_qkv, copy_qkv = adam_update(w_qkv, moments_qkv, totals[0], RATE_MATRIX, WEIGHT_DECAY)
    new_out, state_out, copy_out = adam_update(w_out, moments_out, totals[1], RATE_MATRIX, WEIGHT_DECAY)
    new_up, state_up, copy_up = adam_update(w_up, moments_up, totals[2], RATE_MATRIX, WEIGHT_DECAY)
    new_down, state_down, copy_down = adam_update(w_down, moments_down, totals[3], RATE_MATRIX, WEIGHT_DECAY)
    new_vectors, state_vectors, copy_vectors = adam_update(vectors, moments_vec, totals[4], RATE_VECTOR, 0.0)
    return (block_out, input_grad, new_qkv, new_out, new_up, new_down, new_vectors, state_qkv, state_out, state_up, state_down, state_vectors, copy_qkv, copy_out, copy_up, copy_down, copy_vectors)
```

```python
import types

import jax
import jax.numpy as jnp
from jax import lax
from jax.experimental import pallas as pl
from jax.experimental.pallas import tpu as pltpu
from jax.sharding import PartitionSpec as P

D = 1024
HEADS = 16
FF = 4096
STEP = 3
HEAD = D // HEADS

NORM_EPSILON = 1e-06
MASK_VALUE = -1e30
MOMENT_DECAY = 0.5
RATE_MATRIX = 0.04
RATE_VECTOR = 0.2
WEIGHT_DECAY = 0.1
ADAM_EPSILON = 1e-08

BF = jnp.bfloat16
F32 = jnp.float32
MESH = pl.DeviceIdType.MESH


def adam_update(master, moments, gradient, rate, decay):
    first_moment = MOMENT_DECAY * moments[0] + (1.0 - MOMENT_DECAY) * gradient
    second_moment = MOMENT_DECAY * moments[1] + (1.0 - MOMENT_DECAY) * gradient * gradient
    correction = 1.0 - MOMENT_DECAY**STEP
    normalized = first_moment / correction / (jnp.sqrt(second_moment / correction) + ADAM_EPSILON)
    updated = master - rate * (normalized + decay * master)
    return (updated, jnp.stack([first_moment, second_moment]), updated.astype(BF))


def nn(left, right):
    return jnp.dot(left, right, preferred_element_type=F32)


def nt(left, right):
    return lax.dot_general(left, right, (((1,), (1,)), ((), ())), preferred_element_type=F32)


def tn(left, right):
    return lax.dot_general(left, right, (((0,), (0,)), ((), ())), preferred_element_type=F32)


def loop(count, body):
    def step(index, carry):
        body(index)
        return carry

    lax.fori_loop(0, count, step, 0)


def normalize(rows):
    center = rows - jnp.mean(rows, axis=-1, keepdims=True)
    inverse = lax.rsqrt(jnp.mean(center * center, axis=-1, keepdims=True) + NORM_EPSILON)
    return center * inverse, inverse


def norm_back(grad, unit, inverse, gain):
    scaled = grad * gain
    first = jnp.mean(scaled, axis=-1, keepdims=True)
    second = jnp.mean(scaled * unit, axis=-1, keepdims=True)
    return inverse * (scaled - first - unit * second)


def layout(wide, narrow, length):
    m = types.SimpleNamespace()
    m.W, m.T, m.S = wide, narrow, length
    m.Y = narrow // 2
    m.X = narrow // 2
    m.Z = wide // m.X
    m.L = length * narrow
    m.Q = D // narrow
    m.NQ = 3 * m.Q
    m.F = FF // narrow
    m.RG = D // wide
    m.RD = D // (wide * narrow)
    m.FD = FF // (wide * narrow)
    m.NH = m.Q // HEAD
    m.inside = m.RD % 16 == 0
    return m


def scratch_of(m):
    def weights(name, rows, cols):
        return {
            name: ((m.W, rows, cols), BF),
        }

    def scatter(name, rows, cols):
        return {
            "G" + name: ((m.W, rows, cols), BF),
            "X" + name: ((m.X - 1, m.Z, rows, cols), BF),
            "S" + name: ((m.Z, rows, cols), BF),
            "Z" + name: ((m.Z - 1, rows, cols), BF),
        }

    def spread(name, cols):
        return {
            "T" + name: ((m.T, m.RD, cols), BF),
            "N" + name: ((m.T, m.RD, cols), BF),
        }

    def partial(name):
        return {
            "P" + name: ((m.L, D), BF),
            "C" + name: ((m.Y, m.S, D), BF),
            "M" + name: ((m.Y, m.S, D), BF),
            "A" + name: ((m.S, D), F32),
            "R" + name: ((m.Y - 1, m.S, D), BF),
        }

    out = {}
    out.update(weights("wq", m.RG, m.NQ))
    out["wo"] = ((m.T, m.W, m.RG, m.Q), BF)
    out.update(weights("wu", m.RG, m.F))
    out.update(weights("wd", m.FD, D))
    out.update(weights("wv", 16, D))
    out["vn"] = ((m.T - 1, 16, D), BF)
    out.update(scatter("q", m.RG, m.NQ))
    out.update(scatter("o", m.RG, m.Q))
    out.update(scatter("u", m.RG, m.F))
    out.update(scatter("d", m.FD, D))
    if m.inside:
        out.update(spread("q", m.NQ))
        out.update(spread("o", m.Q))
        out.update(spread("u", m.F))
    for name in ("y", "c", "n"):
        out.update(partial(name))
    for name in ("tok", "dya", "ca"):
        out[name] = ((m.L, D), BF)
    out["oa"] = ((m.T, m.L, m.Q), BF)
    out["sg"] = ((m.T, 8, m.S), F32)
    out["vec"] = ((16, D), F32)
    out["bias"] = ((8, m.NQ), F32)
    out["a"] = ((m.L, D), BF)
    out["at"] = ((D, m.L), BF)
    out["ct"] = ((D, m.L), BF)
    out["ot"] = ((D, m.L), BF)
    out["h"] = ((m.L, m.F), BF)
    out["ht"] = ((m.F, m.L), BF)
    out["u"] = ((m.L, m.F), F32)
    out["du"] = ((m.L, m.F), BF)
    out["qkv"] = ((m.L, m.NQ), BF)
    out["dqkv"] = ((m.L, m.NQ), BF)
    out["prob"] = ((m.T * m.NH, m.S, m.S), F32)
    out["oo"] = ((m.S, D), BF)
    out["r1"] = ((m.S, D), F32)
    out["dr"] = ((m.S, D), F32)
    out["da"] = ((m.S, D), BF)
    out["dob"] = ((m.T, m.S, m.Q), BF)
    out["dab"] = ((m.T, m.S, m.Q), BF)
    out["dof"] = ((m.L, m.Q), BF)
    out["daq"] = ((m.L, m.Q), BF)
    out["sums"] = ((6, 16, D), F32)
    out["vg"] = ((3, 16, D), F32)
    out["vx"] = ((m.X - 1, 16, D), F32)
    out["vz"] = ((m.Z - 1, 16, D), F32)
    out["vt"] = ((m.T - 1, 16, D), F32)
    return out


def semaphores_of(m):
    gather = (m.Z - 1) + m.Z * (m.X - 1)
    scatter = m.Z * (m.X - 1) + (m.Z - 1)
    pair = (m.Y - 1) + m.Y
    direct = m.T - 1
    total = 5 * gather + 4 * scatter + 8 * pair + 10 * direct + (m.X - 1) + (m.Z - 1) + direct
    return 2 * total + 16


def block_kernel(m, names, *refs):
    inputs = ("x", "dy", "seg", "pq", "po", "pu", "pd", "pv")
    outputs = ("bo", "ig", "gq", "go", "gu", "gd", "gv")
    r = types.SimpleNamespace(**dict(zip(inputs + outputs + tuple(names) + ("sem",), refs)))
    w, n = lax.axis_index("wide"), lax.axis_index("narrow")
    z, x = w // m.X, lax.rem(w, m.X)
    y, c = n // 2, lax.rem(n, 2)
    sibling = (w, 2 * y + 1 - c)
    L, S, T, X, Y, Z = m.L, m.S, m.T, m.X, m.Y, m.Z
    sent = []
    used = [0]

    def fresh(count):
        first = used[0]
        used[0] += count
        return [first + k for k in range(count)]

    def copy(src, dst, device, index):
        return pltpu.make_async_remote_copy(
            src_ref=src,
            dst_ref=dst,
            send_sem=r.sem.at[2 * index],
            recv_sem=r.sem.at[2 * index + 1],
            device_id=device,
            device_id_type=MESH,
        )

    def send(src, dst, device, index):
        one = copy(src, dst, device, index)
        one.start()
        sent.append(one)

    def arrive(dst, index):
        copy(dst, dst, sibling, index).wait_recv()

    def up_z(step):
        return lax.rem(z + step, Z)

    def down_z(step):
        return lax.rem(z + Z - step, Z)

    def up_x(step):
        return lax.rem(x + step, X)

    def down_x(step):
        return lax.rem(x + X - step, X)

    def up_n(step):
        return lax.rem(n + step, T)

    def down_n(step):
        return lax.rem(n + T - step, T)

    def at_y(step):
        return lax.rem(y + Y + step, Y)

    def rows_of(index, size):
        return pl.ds(pl.multiple_of(index * size, size), size)

    class Gather:
        def __init__(self, ref):
            self.ref = ref
            self.zi = fresh(Z - 1)
            self.xi = fresh(Z * (X - 1))

        def along_z(self):
            for step in range(1, Z):
                send(self.ref.at[w], self.ref.at[w], (up_z(step) * X + x, n), self.zi[step - 1])

        def forward(self, step):
            block = down_z(step) * X + x if step else w
            for dx in range(1, X):
                send(
                    self.ref.at[block],
                    self.ref.at[block],
                    (z * X + up_x(dx), n),
                    self.xi[step * (X - 1) + dx - 1],
                )

        def relay(self, step):
            arrive(self.ref.at[down_z(step) * X + x], self.zi[step - 1])
            self.forward(step)

        def relays(self):
            for step in range(1, Z):
                self.relay(step)

        def finish(self):
            for step in range(Z):
                for dx in range(1, X):
                    block = (down_z(step) if step else z) * X + down_x(dx)
                    arrive(self.ref.at[block], self.xi[step * (X - 1) + dx - 1])

    class Share:
        def __init__(self, slot):
            self.slot = slot
            self.yi = fresh(Y - 1)
            self.ci = fresh(Y)

        def start(self):
            for step in range(1, Y):
                send(self.slot(n), self.slot(n), (w, 2 * at_y(step) + c), self.yi[step - 1])
            send(self.slot(n), self.slot(n), sibling, self.ci[0])

        def middle(self):
            for step in range(1, Y):
                block = 2 * at_y(-step) + c
                arrive(self.slot(block), self.yi[step - 1])
                send(self.slot(block), self.slot(block), sibling, self.ci[step])

        def finish(self):
            self.middle()
            for step in range(Y):
                block = 2 * at_y(-step) + 1 - c
                arrive(self.slot(block), self.ci[step])

    class Total:
        def __init__(self, name):
            self.part = getattr(r, "P" + name)
            self.core = getattr(r, "C" + name)
            self.mid = getattr(r, "M" + name)
            self.own = getattr(r, "A" + name)
            self.last = getattr(r, "R" + name)
            self.yi = fresh(Y - 1)
            self.ci = fresh(Y)

        def start(self):
            for step in list(range(1, Y)) + [0]:
                block = 2 * at_y(step) + 1 - c
                send(self.part.at[rows_of(block, S)], self.core.at[step], sibling, self.ci[step])

        def middle(self):
            for step in list(range(1, Y)) + [0]:
                block = 2 * at_y(step) + c
                arrive(self.core.at[step], self.ci[step])

                def add(i):
                    rows = rows_of(i, 16)
                    mine = self.part[pl.ds(pl.multiple_of(block * S + i * 16, 16), 16), :]
                    total = mine.astype(F32) + self.core[step, rows, :].astype(F32)
                    if step:
                        self.mid[step, rows, :] = total.astype(BF)
                    else:
                        self.own[rows, :] = total

                loop(S // 16, add)
                if step:
                    send(self.mid.at[step], self.last.at[step - 1], (w, block), self.yi[step - 1])

        def finish(self):
            for step in range(1, Y):
                arrive(self.last.at[step - 1], self.yi[step - 1])

        def rows(self, rows):
            total = self.own[rows, :]
            for step in range(1, Y):
                total = total + self.last[step - 1, rows, :].astype(F32)
            return total

    class Scatter:
        def __init__(self, name, rows, cols):
            self.rows, self.cols = rows, cols
            self.grad = getattr(r, "G" + name)
            self.fromx = getattr(r, "X" + name)
            self.sums = getattr(r, "S" + name)
            self.fromz = getattr(r, "Z" + name)
            self.xi = fresh(Z * (X - 1))
            self.zi = fresh(Z - 1)
            self.chunk = 16 if cols > 512 else 32
            if rows % self.chunk:
                self.chunk = 16

        def order(self):
            return list(range(1, Z)) + [0]

        def multiply(self, step, left, right):
            first = up_z(step) if step else z
            high = X * self.rows
            tile = 256 if self.cols % 256 == 0 else 128

            def one(j):
                cols = rows_of(j, tile)
                value = nn(left[rows_of(first, high), :], right[:, cols]).astype(BF)
                value = value.reshape(X, self.rows, tile)
                self.grad[rows_of(first, X), :, cols] = value

            loop(self.cols // tile, one)

        def along_x(self, step):
            first = up_z(step) if step else z
            for dx in range(1, X):
                other = up_x(dx)
                send(
                    self.grad.at[first * X + other],
                    self.fromx.at[dx - 1, step],
                    (z * X + other, n),
                    self.xi[step * (X - 1) + dx - 1],
                )

        def along_z(self, step):
            block = (up_z(step) if step else z) * X + x
            for dx in range(1, X):
                arrive(self.fromx.at[dx - 1, step], self.xi[step * (X - 1) + dx - 1])

            def add(i):
                rows = rows_of(i, self.chunk)
                total = self.grad[block, rows, :].astype(F32)
                for dx in range(1, X):
                    total = total + self.fromx[dx - 1, step, rows, :].astype(F32)
                self.sums[step, rows, :] = total.astype(BF)

            loop(self.rows // self.chunk, add)
            if step:
                send(self.sums.at[step], self.fromz.at[step - 1], (block, n), self.zi[step - 1])

        def finish(self):
            for step in range(1, Z):
                arrive(self.fromz.at[step - 1], self.zi[step - 1])

        def total(self, rows):
            total = self.sums[0, rows, :].astype(F32)
            for step in range(1, Z):
                total = total + self.fromz[step - 1, rows, :].astype(F32)
            return total

    class Deal:
        def __init__(self, name, scatter, out):
            self.scatter, self.out = scatter, out
            if m.inside:
                self.turn = getattr(r, "T" + name)
                self.got = getattr(r, "N" + name)
                self.ni = fresh(T - 1)

        def start(self):
            self.scatter.finish()
            if not m.inside:
                def store(i):
                    rows = rows_of(i, self.scatter.chunk)
                    self.out[rows, :] = self.scatter.total(rows).astype(BF)

                loop(self.scatter.rows // self.scatter.chunk, store)
                return

            def add(i):
                self.turn[i] = self.scatter.total(rows_of(i, m.RD)).astype(BF)

            loop(T, add)
            for step in range(1, T):
                other = up_n(step)
                send(self.turn.at[other], self.got.at[step], (w, other), self.ni[step - 1])

        def finish(self):
            if not m.inside:
                return
            self.out[n] = self.turn[n]
            for step in range(1, T):
                arrive(self.got.at[step], self.ni[step - 1])
                self.out[down_n(step)] = self.got[step]

    def transpose(target, source, count_rows, count_cols):
        def tile(k):
            i, j = k // count_cols, lax.rem(k, count_cols)
            value = source(rows_of(i, 128), rows_of(j, 128)).astype(F32)
            target[rows_of(j, 128), rows_of(i, 128)] = value.T.astype(BF)

        loop(count_rows * count_cols, tile)

    barrier = pltpu.get_barrier_semaphore()
    peers = [(w, up_n(k)) for k in range(1, T)]
    peers += [(up_z(k) * X + x, n) for k in range(1, Z)]
    peers += [(z * X + up_x(k), n) for k in range(1, X)]
    for peer in peers:
        pl.semaphore_signal(barrier, inc=1, device_id=peer, device_id_type=MESH)
    pl.semaphore_wait(barrier, len(peers))

    gv, gq, gu, gd = Gather(r.wv), Gather(r.wq), Gather(r.wu), Gather(r.wd)
    go = Gather(r.wo.at[n])
    tokens = Share(lambda k: r.tok.at[rows_of(k, S)])
    cotangents = Share(lambda k: r.dya.at[rows_of(k, S)])
    outs = Share(lambda k: r.wo.at[k])
    mixes = Share(lambda k: r.oa.at[k])
    seconds = Share(lambda k: r.ca.at[rows_of(k, S)])
    ty, tc, tin = Total("y"), Total("c"), Total("n")
    sd, su = Scatter("d", m.FD, D), Scatter("u", m.RG, m.F)
    so, sq = Scatter("o", m.RG, m.Q), Scatter("q", m.RG, m.NQ)

    vi, si = fresh(T - 1), fresh(T - 1)
    r.sg[n] = r.seg[...]
    for step in range(1, T):
        send(r.pv, r.vn.at[step - 1], (w, up_n(step)), vi[step - 1])
    shares = []
    if m.inside:
        for part, target in ((r.po, None), (r.pq, r.wq), (r.pu, r.wu)):
            ids = fresh(T - 1)
            own = pl.ds(pl.multiple_of(n * m.RD, m.RD), m.RD)
            for step in range(1, T):
                other = up_n(step)
                there = r.wo.at[other, w, own] if target is None else target.at[w, own]
                send(part.at[other], there, (w, other), ids[step - 1])
            shares.append((target, ids))
            if target is None:
                r.wo[n, w, own, :] = part[n]
            else:
                target[w, own, :] = part[n]
    else:
        r.wo[n, w] = r.po[...]
        r.wq[w] = r.pq[...]
        r.wu[w] = r.pu[...]
    r.wd[w] = r.pd[...]
    own_rows = rows_of(n, S)
    r.tok[own_rows, :] = r.x[...]
    r.dya[own_rows, :] = r.dy[...]
    for step in range(1, T):
        send(r.sg.at[n], r.sg.at[n], (w, up_n(step)), si[step - 1])
    tokens.start()
    cotangents.start()

    vector = r.pv[...].astype(F32)
    for step in range(1, T):
        arrive(r.vn.at[step - 1], vi[step - 1])
        vector = vector + r.vn[step - 1].astype(F32)
    r.wv[w] = vector.astype(BF)
    gv.along_z()
    gv.forward(0)

    def shared(k):
        if m.inside:
            target, ids = shares[k]
            for step in range(1, T):
                got = pl.ds(pl.multiple_of(down_n(step) * m.RD, m.RD), m.RD)
                arrive(r.wo.at[n, w, got] if target is None else target.at[w, got], ids[step - 1])

    shared(0)
    go.along_z()
    go.forward(0)
    shared(1)
    gq.along_z()
    shared(2)
    gu.along_z()
    gd.along_z()
    gv.relays()
    go.relays()
    gq.forward(0)
    tokens.finish()
    gv.finish()
    vector = r.wv[0].astype(F32)
    for k in range(1, m.W):
        vector = vector + r.wv[k].astype(F32)
    r.vec[...] = vector

    heads = rows_of(n, m.Q)
    r.bias[...] = jnp.zeros_like(r.bias)
    r.bias[0:1, 0 : m.Q] = r.vec[2:3, heads]
    r.bias[0:1, 2 * m.Q : 3 * m.Q] = r.vec[3:4, heads]

    def first_norm(i):
        rows = rows_of(i, 16)
        unit, _ = normalize(r.tok[rows, :].astype(F32))
        r.a[rows, :] = (unit * r.vec[0:1, :] + r.vec[1:2, :]).astype(BF)

    loop(L // 16, first_norm)
    cotangents.finish()
    go.finish()
    outs.start()
    transpose(r.at, lambda i, j: r.a[i, j], L // 128, D // 128)
    gq.relays()
    gu.forward(0)
    outs.middle()
    gq.finish()

    tile_q = 256 if m.NQ % 256 == 0 else 128

    def project(j):
        cols = rows_of(j, tile_q)
        value = nn(r.a[...], r.wq[:, :, cols].reshape(D, tile_q)) + r.bias[0:1, cols]
        r.qkv[:, cols] = value.astype(BF)

    loop(m.NQ // tile_q, project)
    for step in range(1, T):
        arrive(r.sg.at[down_n(step)], si[step - 1])

    lane = lax.broadcasted_iota(jnp.int32, (1, 128), 1)
    halves = [(lane // HEAD == k).astype(F32) for k in range(128 // HEAD)]
    scale = HEAD ** (-0.5)
    per = 128 // HEAD

    def pick(values):
        total = values[0] * halves[0]
        for k in range(1, per):
            total = total + values[k] * halves[k]
        return total

    def attend(s):
        rows = rows_of(s, S)
        keys = jnp.broadcast_to(r.sg[s, 0:1, :], (S, S))
        same = keys == keys.T
        for pair in range(m.Q // 128):
            q = r.qkv[rows, pair * 128 : pair * 128 + 128]
            k = r.qkv[rows, m.Q + pair * 128 : m.Q + pair * 128 + 128]
            v = r.qkv[rows, 2 * m.Q + pair * 128 : 2 * m.Q + pair * 128 + 128]
            mixed = []
            for half in range(per):
                score = nt(q * halves[half].astype(BF), k) * scale
                score = jnp.where(same, score, MASK_VALUE)
                power = jnp.exp(score - jnp.max(score, axis=-1, keepdims=True))
                weight = power / jnp.sum(power, axis=-1, keepdims=True)
                r.prob[s * m.NH + pair * per + half] = weight
                mixed.append(nn(weight.astype(BF), v))
            r.oa[n, rows, pair * 128 : pair * 128 + 128] = pick(mixed).astype(BF)

    loop(T, attend)
    mixes.start()
    gu.relay(1)
    for k in range(2, Z - 1):
        gu.relay(k)
    mixes.middle()
    for step in range(Y):
        arrive(outs.slot(2 * at_y(-step) + 1 - c), outs.ci[step])
    for step in range(Y):
        arrive(mixes.slot(2 * at_y(-step) + 1 - c), mixes.ci[step])

    for t in range(T):
        r.oo[:, t * m.Q : (t + 1) * m.Q] = r.oa[t, own_rows, :]
    for t in range(T):
        cols = slice(t * m.Q, (t + 1) * m.Q)
        value = nn(r.oo[...], r.wo[t].reshape(D, m.Q))
        r.r1[:, cols] = r.x[:, cols].astype(F32) + value + r.vec[4:5, cols]

    def second_norm(i):
        rows = rows_of(i, 16)
        unit, _ = normalize(r.r1[rows, :])
        there = pl.ds(pl.multiple_of(n * S + i * 16, 16), 16)
        r.ca[there, :] = (unit * r.vec[5:6, :] + r.vec[6:7, :]).astype(BF)

    loop(S // 16, second_norm)
    seconds.start()
    gu.relay(Z - 1)
    gd.forward(0)
    seconds.middle()
    for t in range(T):
        for k in range(m.Q // 128):
            base = t * m.Q + k * 128

            def turn(i, t=t, k=k, base=base):
                value = r.oa[t, rows_of(i, 128), k * 128 : k * 128 + 128].astype(F32)
                r.ot[base : base + 128, rows_of(i, 128)] = value.T.astype(BF)

            loop(L // 128, turn)
    for step in range(Y):
        arrive(seconds.slot(2 * at_y(-step) + 1 - c), seconds.ci[step])
    transpose(r.ct, lambda i, j: r.ca[i, j], L // 128, D // 128)
    gu.finish()

    def expand(j):
        cols = rows_of(j, 256)
        value = nn(r.ca[...], r.wu[:, :, cols].reshape(D, 256))
        r.u[:, cols] = value + r.vec[pl.ds(8 + n, 1), cols]

    loop(m.F // 256, expand)

    def activate(i):
        rows = rows_of(i, 16)
        value = r.u[rows, :]
        phi = 0.5 * (1.0 + lax.erf(value * (0.5**0.5)))
        r.h[rows, :] = (value * phi).astype(BF)
        r.u[rows, :] = phi + value * (jnp.exp(-0.5 * value * value) * 0.3989422804014327)

    loop(L // 16, activate)
    transpose(r.ht, lambda i, j: r.h[i, j], L // 128, m.F // 128)
    for step in sd.order():
        sd.multiply(step, r.ht, r.dya)
    gd.relays()
    for step in sd.order():
        sd.along_x(step)
    gd.finish()

    group = 256 // m.FD

    def expand_back(j):
        cols = rows_of(j, 256)
        value = nt(r.dya[...], r.wd[rows_of(j, group)].reshape(256, D)) * r.u[:, cols]
        low = value.astype(BF)
        r.du[:, cols] = low
        r.sums[5, 0:1, cols] = jnp.sum(low.astype(F32), axis=0, keepdims=True)

    loop(m.F // 256, expand_back)
    width = 256 // m.RG

    def up_back(j):
        value = nt(r.du[...], r.wu[rows_of(j, width)].reshape(256, m.F))
        r.Pc[:, rows_of(j, 256)] = value.astype(BF)

    loop(D // 256, up_back)
    tc.start()
    for step in su.order():
        su.multiply(step, r.ct, r.du)
        su.along_x(step)
    tc.middle()

    def contract(j):
        cols = rows_of(j, 256)
        r.Py[:, cols] = nn(r.h[...], r.wd[:, :, cols].reshape(m.F, 256)).astype(BF)

    loop(D // 256, contract)
    sd.along_z(1)
    tc.finish()
    r.sums[0:4] = jnp.zeros((4, 16, D), F32)

    def second_back(i):
        rows = rows_of(i, 16)
        grad = tc.rows(rows)
        cot = r.dy[rows, :].astype(F32)
        unit, inverse = normalize(r.r1[rows, :])
        total = cot + norm_back(grad, unit, inverse, r.vec[5:6, :])
        r.dr[rows, :] = total
        r.da[rows, :] = total.astype(BF)
        r.sums[0] += total
        r.sums[1] += grad * unit
        r.sums[2] += grad
        r.sums[3] += cot

    loop(S // 16, second_back)
    oi, ai = fresh(T - 1), fresh(T - 1)
    share = m.Q // m.RG
    for step in list(range(1, T)) + [0]:
        other = up_n(step) if step else n
        value = jnp.zeros((S, m.Q), F32)
        for t in range(T):
            block = r.wo[t, rows_of(other, share)].reshape(m.Q, m.Q)
            value = value + nt(r.da[:, t * m.Q : (t + 1) * m.Q], block)
        if step:
            r.dob[step] = value.astype(BF)
            send(r.dob.at[step], r.dof.at[own_rows], (w, other), oi[step - 1])
        else:
            r.dof[own_rows, :] = value.astype(BF)
    for step in range(1, T):
        other = up_n(step)
        r.dab[step] = r.da[:, rows_of(other, m.Q)]
        send(r.dab.at[step], r.daq.at[own_rows], (w, other), ai[step - 1])
    r.daq[own_rows, :] = r.da[:, rows_of(n, m.Q)]
    ty.start()
    sd.along_z(2 if Z > 2 else 0)
    for step in range(1, T):
        arrive(r.dof.at[rows_of(down_n(step), S)], oi[step - 1])

    def attend_back(s):
        rows = rows_of(s, S)
        for pair in range(m.Q // 128):
            at = [pl.ds(b * m.Q + pair * 128, 128) for b in range(3)]
            q, k, v = r.qkv[rows, at[0]], r.qkv[rows, at[1]], r.qkv[rows, at[2]]
            cot = r.dof[rows, pair * 128 : pair * 128 + 128]
            dq, dk, dv = [], [], []
            for half in range(per):
                weight = r.prob[s * m.NH + pair * per + half]
                grad = nt(cot * halves[half].astype(BF), v)
                inner = jnp.sum(weight * grad, axis=-1, keepdims=True)
                ds = (weight * (grad - inner)).astype(BF)
                dq.append(nn(ds, k))
                dk.append(tn(ds, q))
                dv.append(tn(weight.astype(BF), cot))
            r.dqkv[rows, at[0]] = (pick(dq) * scale).astype(BF)
            r.dqkv[rows, at[1]] = (pick(dk) * scale).astype(BF)
            r.dqkv[rows, at[2]] = pick(dv).astype(BF)

    loop(T, attend_back)

    def project_back(j):
        value = nt(r.dqkv[...], r.wq[rows_of(j, width)].reshape(256, m.NQ))
        r.Pn[:, rows_of(j, 256)] = value.astype(BF)

    loop(D // 256, project_back)
    tin.start()
    for step in range(1, T):
        arrive(r.daq.at[rows_of(down_n(step), S)], ai[step - 1])
    for step in so.order():
        so.multiply(step, r.ot, r.daq)
        so.along_x(step)
    tin.middle()
    for step in sq.order():
        sq.multiply(step, r.at, r.dqkv)
        sq.along_x(step)
    for step in sd.order()[2:]:
        sd.along_z(step)

    r.vg[0] = jnp.zeros((16, D), F32)
    for k, row in enumerate((4, 5, 6, 7)):
        r.vg[0, row : row + 1, :] = jnp.sum(r.sums[k], axis=0, keepdims=True)
    r.vg[0, pl.ds(8 + n, 1), 0 : m.F] = r.sums[5, 0:1, 0 : m.F]

    def column(j):
        cols = rows_of(j, 128)
        there = pl.ds(pl.multiple_of(n * m.Q + j * 128, 128), 128)
        tail = pl.ds(pl.multiple_of(2 * m.Q + j * 128, 128), 128)
        r.vg[0, 2:3, there] = jnp.sum(r.dqkv[:, cols].astype(F32), axis=0, keepdims=True)
        r.vg[0, 3:4, there] = jnp.sum(r.dqkv[:, tail].astype(F32), axis=0, keepdims=True)

    loop(m.Q // 128, column)
    tin.finish()
    r.sums[0:2] = jnp.zeros((2, 16, D), F32)

    def first_back(i):
        rows = rows_of(i, 16)
        grad = tin.rows(rows)
        unit, inverse = normalize(r.x[rows, :].astype(F32))
        r.ig[rows, :] = r.dr[rows, :] + norm_back(grad, unit, inverse, r.vec[0:1, :])
        r.sums[0] += grad * unit
        r.sums[1] += grad

    loop(S // 16, first_back)
    r.vg[0, 0:1, :] = jnp.sum(r.sums[0], axis=0, keepdims=True)
    r.vg[0, 1:2, :] = jnp.sum(r.sums[1], axis=0, keepdims=True)
    vxi, vzi, vti = fresh(X - 1), fresh(Z - 1), fresh(T - 1)
    for dx in range(1, X):
        send(r.vg.at[0], r.vx.at[dx - 1], (z * X + up_x(dx), n), vxi[dx - 1])

    ty.middle()
    for step in su.order():
        su.along_z(step)
    ty.finish()

    def close(i):
        rows = rows_of(i, 16)
        r.bo[rows, :] = (r.r1[rows, :] + ty.rows(rows) + r.vec[7:8, :]).astype(BF)

    loop(S // 16, close)
    sd.finish()

    def keep(i):
        rows = rows_of(i, 16)
        r.gd[rows, :] = sd.total(rows)

    loop(m.FD // 16, keep)
    for step in so.order():
        so.along_z(step)
    du, do, dq = Deal("u", su, r.gu), Deal("o", so, r.go), Deal("q", sq, r.gq)
    du.start()
    for step in sq.order():
        sq.along_z(step)
    total = r.vg[0]
    for dx in range(1, X):
        arrive(r.vx.at[dx - 1], vxi[dx - 1])
        total = total + r.vx[dx - 1]
    r.vg[1] = total
    for step in range(1, Z):
        send(r.vg.at[1], r.vz.at[step - 1], (up_z(step) * X + x, n), vzi[step - 1])
    do.start()
    dq.start()
    total = r.vg[1]
    for step in range(1, Z):
        arrive(r.vz.at[step - 1], vzi[step - 1])
        total = total + r.vz[step - 1]
    r.vg[2] = total
    for step in range(1, T):
        send(r.vg.at[2], r.vt.at[step - 1], (w, up_n(step)), vti[step - 1])
    du.finish()
    do.finish()
    dq.finish()
    total = r.vg[2]
    for step in range(1, T):
        arrive(r.vt.at[step - 1], vti[step - 1])
        total = total + r.vt[step - 1]
    r.gv[...] = total
    for one in sent:
        one.wait_send()


def block_step(m, args):
    scratch = scratch_of(m)
    kept = {"q": m.NQ, "o": m.Q, "u": m.F}
    grads = [
        jax.ShapeDtypeStruct((m.T, m.RD, cols) if m.inside else (m.RG, cols), BF)
        for cols in kept.values()
    ]
    vmem = pl.BlockSpec(memory_space=pltpu.VMEM)

    def kernel(*refs):
        block_kernel(m, list(scratch), *refs)

    return pl.pallas_call(
        kernel,
        out_shape=[
            jax.ShapeDtypeStruct((m.S, D), BF),
            jax.ShapeDtypeStruct((m.S, D), F32),
            *grads,
            jax.ShapeDtypeStruct((m.FD, D), F32),
            jax.ShapeDtypeStruct((16, D), F32),
        ],
        in_specs=[vmem] * len(args),
        out_specs=[vmem] * 7,
        scratch_shapes=[pltpu.VMEM(shape, kind) for shape, kind in scratch.values()]
        + [pltpu.SemaphoreType.DMA((semaphores_of(m),))],
        compiler_params=pltpu.CompilerParams(
            collective_id=0, has_side_effects=True, vmem_limit_bytes=62 * 1024 * 1024
        ),
        name="block_step",
    )(*args)


def body(
    tokens,
    cotangent,
    segment_ids,
    w_qkv,
    w_out,
    w_up,
    w_down,
    vectors,
    moments_qkv,
    moments_out,
    moments_up,
    moments_down,
    moments_vec,
):
    wide, narrow = lax.axis_size("wide"), lax.axis_size("narrow")
    m = layout(wide, narrow, tokens.shape[0])
    device = lax.axis_index("wide") * narrow + lax.axis_index("narrow")
    first_row = device * m.RD

    pq = w_qkv.astype(BF).reshape(m.RD, 3, m.T, m.Q).transpose(2, 0, 1, 3)
    po = w_out.astype(BF).reshape(m.RD, m.T, m.Q).transpose(1, 0, 2)
    pu = w_up.astype(BF).reshape(m.RD, m.W, m.T, m.FD).transpose(2, 0, 1, 3)
    parts = [pq.reshape(m.T, m.RD, m.NQ), po, pu.reshape(m.T, m.RD, m.F)]
    if not m.inside:
        parts = [
            lax.all_to_all(part, "narrow", 0, 0).reshape(m.RG, part.shape[2]) for part in parts
        ]
    low = vectors.astype(BF).T
    spot = jnp.zeros((12, D), BF)
    spot = lax.dynamic_update_slice(spot, low, (0, first_row))
    rise = spot[8:].reshape(m.W, m.T, m.FD).transpose(1, 0, 2).reshape(m.T, m.F)
    rise = jnp.pad(rise, ((0, 8 - m.T), (0, D - m.F)))
    packed = jnp.concatenate([spot[:8], rise], axis=0)
    segments = jnp.broadcast_to(segment_ids.astype(F32), (8, m.S))

    block_out, input_grad, gq, go, gu, gd, gv = block_step(
        m, (tokens, cotangent, segments, *parts, w_down.astype(BF), packed)
    )
    if not m.inside:
        gq, go, gu = [
            lax.all_to_all(g.reshape(m.T, m.RD, g.shape[1]), "narrow", 0, 0) for g in (gq, go, gu)
        ]
    grad_qkv = gq.reshape(m.T, m.RD, 3, m.Q).transpose(1, 2, 0, 3).reshape(m.RD, 3 * D)
    grad_out = go.transpose(1, 0, 2).reshape(m.RD, D)
    grad_up = gu.reshape(m.T, m.RD, m.W, m.FD).transpose(1, 2, 0, 3).reshape(m.RD, FF)
    rise = gv[8 : 8 + m.T, : m.F].reshape(m.T, m.W, m.FD).transpose(1, 0, 2).reshape(FF // D, D)
    grad_vec = lax.dynamic_slice(
        jnp.concatenate([gv[:8], rise], axis=0), (0, first_row), (12, m.RD)
    ).T

    new_qkv, state_qkv, copy_qkv = adam_update(
        w_qkv, moments_qkv, grad_qkv.astype(F32), RATE_MATRIX, WEIGHT_DECAY
    )
    new_out, state_out, copy_out = adam_update(
        w_out, moments_out, grad_out.astype(F32), RATE_MATRIX, WEIGHT_DECAY
    )
    new_up, state_up, copy_up = adam_update(
        w_up, moments_up, grad_up.astype(F32), RATE_MATRIX, WEIGHT_DECAY
    )
    new_down, state_down, copy_down = adam_update(w_down, moments_down, gd, RATE_MATRIX, WEIGHT_DECAY)
    new_vectors, state_vectors, copy_vectors = adam_update(
        vectors, moments_vec, grad_vec, RATE_VECTOR, 0.0
    )
    return (
        block_out,
        input_grad,
        new_qkv,
        new_out,
        new_up,
        new_down,
        new_vectors,
        state_qkv,
        state_out,
        state_up,
        state_down,
        state_vectors,
        copy_qkv,
        copy_out,
        copy_up,
        copy_down,
        copy_vectors,
    )


def solution(mesh):
    flat = P(("wide", "narrow"), None)
    pair = P(None, ("wide", "narrow"), None)
    return jax.shard_map(
        body,
        mesh=mesh,
        in_specs=(flat,) * 8 + (pair,) * 5,
        out_specs=(flat,) * 7 + (pair,) * 5 + (flat,) * 5,
        check_vma=False,
    )
```

```python
import types

import jax
import jax.numpy as jnp
from jax import lax
from jax.experimental import pallas as pl
from jax.experimental.pallas import tpu as pltpu
from jax.sharding import PartitionSpec as P

D = 1024
HEADS = 16
FF = 4096
STEP = 3
HEAD = D // HEADS

NORM_EPSILON = 1e-06
MASK_VALUE = -1e30
MOMENT_DECAY = 0.5
RATE_MATRIX = 0.04
RATE_VECTOR = 0.2
WEIGHT_DECAY = 0.1
ADAM_EPSILON = 1e-08

BF = jnp.bfloat16
F32 = jnp.float32
MESH = pl.DeviceIdType.MESH


def adam_update(master, moments, gradient, rate, decay):
    first_moment = MOMENT_DECAY * moments[0] + (1.0 - MOMENT_DECAY) * gradient
    second_moment = MOMENT_DECAY * moments[1] + (1.0 - MOMENT_DECAY) * gradient * gradient
    correction = 1.0 - MOMENT_DECAY**STEP
    normalized = first_moment / correction / (jnp.sqrt(second_moment / correction) + ADAM_EPSILON)
    updated = master - rate * (normalized + decay * master)
    return (updated, jnp.stack([first_moment, second_moment]), updated.astype(BF))


def nn(left, right):
    return jnp.dot(left, right, preferred_element_type=F32)


def nt(left, right):
    return lax.dot_general(left, right, (((1,), (1,)), ((), ())), preferred_element_type=F32)


def tn(left, right):
    return lax.dot_general(left, right, (((0,), (0,)), ((), ())), preferred_element_type=F32)


def loop(count, body, first=0):
    def step(index, carry):
        body(index)
        return carry

    lax.fori_loop(first, first + count, step, 0)


def normalize(rows):
    center = rows - jnp.mean(rows, axis=-1, keepdims=True)
    inverse = lax.rsqrt(jnp.mean(center * center, axis=-1, keepdims=True) + NORM_EPSILON)
    return center * inverse, inverse


def norm_back(grad, unit, inverse, gain):
    scaled = grad * gain
    first = jnp.mean(scaled, axis=-1, keepdims=True)
    second = jnp.mean(scaled * unit, axis=-1, keepdims=True)
    return inverse * (scaled - first - unit * second)


def layout(wide, narrow, length):
    m = types.SimpleNamespace()
    m.W, m.T, m.S = wide, narrow, length
    m.Y = narrow // 2
    m.X = narrow // 2
    m.Z = wide // m.X
    m.L = length * narrow
    m.Q = D // narrow
    m.NQ = 3 * m.Q
    m.F = FF // narrow
    m.RG = D // wide
    m.RD = D // (wide * narrow)
    m.FD = FF // (wide * narrow)
    m.NH = m.Q // HEAD
    m.inside = m.RD % 16 == 0
    return m


def scratch_of(m):
    def weights(name, rows, cols):
        return {
            name: ((m.W, rows, cols), BF),
        }

    def scatter(name, rows, cols):
        return {
            "G" + name: ((m.W, rows, cols), BF),
            "X" + name: ((m.X - 1, m.Z, rows, cols), BF),
            "S" + name: ((m.Z, rows, cols), BF),
            "Z" + name: ((m.Z - 1, rows, cols), BF),
        }

    def spread(name, cols):
        return {
            "T" + name: ((m.T, m.RD, cols), BF),
            "N" + name: ((m.T, m.RD, cols), BF),
        }

    def partial(name):
        return {
            "P" + name: ((m.L, D), BF),
            "C" + name: ((m.Y, m.S, D), BF),
            "M" + name: ((m.Y, m.S, D), BF),
            "A" + name: ((m.S, D), F32),
            "R" + name: ((m.Y - 1, m.S, D), BF),
        }

    out = {}
    out.update(weights("wq", m.RG, m.NQ))
    out["wo"] = ((m.T, m.W, m.RG, m.Q), BF)
    out.update(weights("wu", m.RG, m.F))
    out.update(weights("wd", m.FD, D))
    out.update(weights("wv", 16, D))
    out["vn"] = ((m.T - 1, 16, D), BF)
    out.update(scatter("q", m.RG, m.NQ))
    out.update(scatter("o", m.RG, m.Q))
    out.update(scatter("u", m.RG, m.F))
    out.update(scatter("d", m.FD, D))
    if m.inside:
        out.update(spread("q", m.NQ))
        out.update(spread("o", m.Q))
        out.update(spread("u", m.F))
    for name in ("y", "c", "n"):
        out.update(partial(name))
    for name in ("tok", "dya", "ca"):
        out[name] = ((m.L, D), BF)
    out["oa"] = ((m.T, m.L, m.Q), BF)
    out["sg"] = ((m.T, 8, m.S), F32)
    out["vec"] = ((16, D), F32)
    out["bias"] = ((8, m.NQ), F32)
    out["a"] = ((m.L, D), BF)
    out["at"] = ((D, m.L), BF)
    out["ct"] = ((D, m.L), BF)
    out["ot"] = ((D, m.L), BF)
    out["h"] = ((m.L, m.F), BF)
    out["ht"] = ((m.F, m.L), BF)
    out["u"] = ((m.L, m.F), F32)
    out["du"] = ((m.L, m.F), BF)
    out["qkv"] = ((m.L, m.NQ), BF)
    out["dqkv"] = ((m.L, m.NQ), BF)
    out["prob"] = ((m.T * m.NH, m.S, m.S), F32)
    out["oo"] = ((m.S, D), BF)
    out["r1"] = ((m.S, D), F32)
    out["dr"] = ((m.S, D), F32)
    out["da"] = ((m.S, D), BF)
    out["dob"] = ((m.T, m.S, m.Q), BF)
    out["dab"] = ((m.T, m.S, m.Q), BF)
    out["dof"] = ((m.L, m.Q), BF)
    out["daq"] = ((m.L, m.Q), BF)
    out["sums"] = ((6, 16, D), F32)
    out["vg"] = ((3, 16, D), F32)
    out["vx"] = ((m.X - 1, 16, D), F32)
    out["vz"] = ((m.Z - 1, 16, D), F32)
    out["vt"] = ((m.T - 1, 16, D), F32)
    return out


def semaphores_of(m):
    gather = (m.Z - 1) + m.Z * (m.X - 1)
    scatter = m.Z * (m.X - 1) + (m.Z - 1)
    pair = (m.Y - 1) + m.Y
    direct = m.T - 1
    total = 5 * gather + 4 * scatter + 8 * pair + 10 * direct + (m.X - 1) + (m.Z - 1) + direct
    return 2 * total + 16


def block_kernel(m, names, *refs):
    inputs = ("x", "dy", "seg", "pq", "po", "pu", "pd", "pv")
    outputs = ("bo", "ig", "gq", "go", "gu", "gd", "gv")
    r = types.SimpleNamespace(**dict(zip(inputs + outputs + tuple(names) + ("sem",), refs)))
    w, n = lax.axis_index("wide"), lax.axis_index("narrow")
    z, x = w // m.X, lax.rem(w, m.X)
    y, c = n // 2, lax.rem(n, 2)
    sibling = (w, 2 * y + 1 - c)
    L, S, T, X, Y, Z = m.L, m.S, m.T, m.X, m.Y, m.Z
    sent = []
    used = [0]

    def fresh(count):
        first = used[0]
        used[0] += count
        return [first + k for k in range(count)]

    def copy(src, dst, device, index):
        return pltpu.make_async_remote_copy(
            src_ref=src,
            dst_ref=dst,
            send_sem=r.sem.at[2 * index],
            recv_sem=r.sem.at[2 * index + 1],
            device_id=device,
            device_id_type=MESH,
        )

    def send(src, dst, device, index):
        one = copy(src, dst, device, index)
        one.start()
        sent.append(one)

    def arrive(dst, index):
        copy(dst, dst, sibling, index).wait_recv()

    def up_z(step):
        return lax.rem(z + step, Z)

    def down_z(step):
        return lax.rem(z + Z - step, Z)

    def up_x(step):
        return lax.rem(x + step, X)

    def down_x(step):
        return lax.rem(x + X - step, X)

    def up_n(step):
        return lax.rem(n + step, T)

    def down_n(step):
        return lax.rem(n + T - step, T)

    def at_y(step):
        return lax.rem(y + Y + step, Y)

    def rows_of(index, size):
        return pl.ds(pl.multiple_of(index * size, size), size)

    class Gather:
        def __init__(self, ref):
            self.ref = ref
            self.zi = fresh(Z - 1)
            self.xi = fresh(Z * (X - 1))

        def along_z(self):
            for k in range(Z - 1):
                step = 1 + lax.rem(k + 1 - lax.rem(z, 2), Z - 1)
                send(self.ref.at[w], self.ref.at[w], (up_z(step) * X + x, n), self.zi[0] + step - 1)

        def forward(self, step):
            block = down_z(step) * X + x
            for dx in range(1, X):
                send(
                    self.ref.at[block],
                    self.ref.at[block],
                    (z * X + up_x(dx), n),
                    self.xi[0] + step * (X - 1) + dx - 1,
                )

        def relay(self, k):
            step = jnp.where(lax.rem(z, 2) == 0, k, Z - k)
            arrive(self.ref.at[down_z(step) * X + x], self.zi[0] + step - 1)
            self.forward(step)

        def relays(self):
            for step in range(1, Z):
                self.relay(step)

        def finish(self):
            for step in range(Z):
                for dx in range(1, X):
                    block = (down_z(step) if step else z) * X + down_x(dx)
                    arrive(self.ref.at[block], self.xi[step * (X - 1) + dx - 1])

    class Share:
        def __init__(self, slot):
            self.slot = slot
            self.yi = fresh(Y - 1)
            self.ci = fresh(Y)

        def start(self):
            for step in range(1, Y):
                send(self.slot(n), self.slot(n), (w, 2 * at_y(step) + c), self.yi[step - 1])
            send(self.slot(n), self.slot(n), sibling, self.ci[0])

        def middle(self):
            for step in range(1, Y):
                block = 2 * at_y(-step) + c
                arrive(self.slot(block), self.yi[step - 1])
                send(self.slot(block), self.slot(block), sibling, self.ci[step])

        def close(self):
            for step in range(Y):
                block = 2 * at_y(-step) + 1 - c
                arrive(self.slot(block), self.ci[step])

    class Total:
        def __init__(self, name):
            self.part = getattr(r, "P" + name)
            self.core = getattr(r, "C" + name)
            self.mid = getattr(r, "M" + name)
            self.own = getattr(r, "A" + name)
            self.last = getattr(r, "R" + name)
            self.yi = fresh(Y - 1)
            self.ci = fresh(Y)

        def start(self):
            for step in list(range(1, Y)) + [0]:
                block = 2 * at_y(step) + 1 - c
                send(self.part.at[rows_of(block, S)], self.core.at[step], sibling, self.ci[step])

        def middle(self):
            for step in list(range(1, Y)) + [0]:
                block = 2 * at_y(step) + c
                arrive(self.core.at[step], self.ci[step])

                def add(i):
                    rows = rows_of(i, 16)
                    mine = self.part[pl.ds(pl.multiple_of(block * S + i * 16, 16), 16), :]
                    total = mine.astype(F32) + self.core[step, rows, :].astype(F32)
                    if step:
                        self.mid[step, rows, :] = total.astype(BF)
                    else:
                        self.own[rows, :] = total

                loop(S // 16, add)
                if step:
                    send(self.mid.at[step], self.last.at[step - 1], (w, block), self.yi[step - 1])

        def finish(self):
            for step in range(1, Y):
                arrive(self.last.at[step - 1], self.yi[step - 1])

        def rows(self, rows):
            total = self.own[rows, :]
            for step in range(1, Y):
                total = total + self.last[step - 1, rows, :].astype(F32)
            return total

    class Scatter:
        def __init__(self, name, rows, cols):
            self.rows, self.cols = rows, cols
            self.grad = getattr(r, "G" + name)
            self.fromx = getattr(r, "X" + name)
            self.sums = getattr(r, "S" + name)
            self.fromz = getattr(r, "Z" + name)
            self.xi = fresh(Z * (X - 1))
            self.zi = fresh(Z - 1)
            self.chunk = 16 if cols > 512 else 32
            if rows % self.chunk:
                self.chunk = 16

        def order(self):
            return [Z // 2] + [k for k in range(1, Z) if k != Z // 2] + [0]

        def multiply(self, step, left, right):
            first = up_z(step) if step else z
            high = X * self.rows
            tile = 256 if self.cols % 256 == 0 else 128

            def one(j):
                cols = rows_of(j, tile)
                value = nn(left[rows_of(first, high), :], right[:, cols]).astype(BF)
                value = value.reshape(X, self.rows, tile)
                self.grad[rows_of(first, X), :, cols] = value

            loop(self.cols // tile, one)

        def along_x(self, step):
            first = up_z(step) if step else z
            for dx in range(1, X):
                other = up_x(dx)
                send(
                    self.grad.at[first * X + other],
                    self.fromx.at[dx - 1, step],
                    (z * X + other, n),
                    self.xi[step * (X - 1) + dx - 1],
                )

        def along_z(self, step):
            block = (up_z(step) if step else z) * X + x
            for dx in range(1, X):
                arrive(self.fromx.at[dx - 1, step], self.xi[step * (X - 1) + dx - 1])

            def add(i):
                rows = rows_of(i, self.chunk)
                total = self.grad[block, rows, :].astype(F32)
                for dx in range(1, X):
                    total = total + self.fromx[dx - 1, step, rows, :].astype(F32)
                self.sums[step, rows, :] = total.astype(BF)

            loop(self.rows // self.chunk, add)
            if step:
                send(self.sums.at[step], self.fromz.at[step - 1], (block, n), self.zi[step - 1])

        def finish(self):
            for step in range(1, Z):
                arrive(self.fromz.at[step - 1], self.zi[step - 1])

        def total(self, rows):
            total = self.sums[0, rows, :].astype(F32)
            for step in range(1, Z):
                total = total + self.fromz[step - 1, rows, :].astype(F32)
            return total

    class Deal:
        def __init__(self, name, scatter, out):
            self.scatter, self.out = scatter, out
            if m.inside:
                self.turn = getattr(r, "T" + name)
                self.got = getattr(r, "N" + name)
                self.ni = fresh(T - 1)

        def start(self):
            self.scatter.finish()
            if not m.inside:
                def store(i):
                    rows = rows_of(i, self.scatter.chunk)
                    self.out[rows, :] = self.scatter.total(rows).astype(BF)

                loop(self.scatter.rows // self.scatter.chunk, store)
                return

            def add(i):
                self.turn[i] = self.scatter.total(rows_of(i, m.RD)).astype(BF)

            loop(T, add)
            for step in range(1, T):
                other = up_n(step)
                send(self.turn.at[other], self.got.at[step], (w, other), self.ni[step - 1])

        def finish(self):
            if not m.inside:
                return
            self.out[n] = self.turn[n]
            for step in range(1, T):
                arrive(self.got.at[step], self.ni[step - 1])
                self.out[down_n(step)] = self.got[step]

    def transpose(target, source, count_rows, count_cols):
        def tile(k):
            i, j = k // count_cols, lax.rem(k, count_cols)
            value = source(rows_of(i, 128), rows_of(j, 128)).astype(F32)
            target[rows_of(j, 128), rows_of(i, 128)] = value.T.astype(BF)

        loop(count_rows * count_cols, tile)

    barrier = pltpu.get_barrier_semaphore()
    peers = [(w, up_n(k)) for k in range(1, T)]
    peers += [(up_z(k) * X + x, n) for k in range(1, Z)]
    peers += [(z * X + up_x(k), n) for k in range(1, X)]
    for peer in peers:
        pl.semaphore_signal(barrier, inc=1, device_id=peer, device_id_type=MESH)
    pl.semaphore_wait(barrier, len(peers))

    gv, gq, gu, gd = Gather(r.wv), Gather(r.wq), Gather(r.wu), Gather(r.wd)
    go = Gather(r.wo.at[n])
    tokens = Share(lambda k: r.tok.at[rows_of(k, S)])
    cotangents = Share(lambda k: r.dya.at[rows_of(k, S)])
    outs = Share(lambda k: r.wo.at[k])
    mixes = Share(lambda k: r.oa.at[k])
    seconds = Share(lambda k: r.ca.at[rows_of(k, S)])
    ty, tc, tin = Total("y"), Total("c"), Total("n")
    sd, su = Scatter("d", m.FD, D), Scatter("u", m.RG, m.F)
    so, sq = Scatter("o", m.RG, m.Q), Scatter("q", m.RG, m.NQ)

    vi, si = fresh(T - 1), fresh(T - 1)
    for step in range(1, T):
        send(r.pv, r.vn.at[step - 1], (w, up_n(step)), vi[step - 1])
    r.wd[w] = r.pd[...]
    gd.forward(0)

    class Rows:
        def __init__(self, part, target):
            self.part, self.target = part, target
            self.ids = fresh(T - 1) if m.inside else []

        def at(self, k, rows):
            return r.wo.at[k, w, rows] if self.target is None else self.target.at[w, rows]

        def start(self):
            if m.inside:
                own = pl.ds(pl.multiple_of(n * m.RD, m.RD), m.RD)
                for step in range(1, T):
                    other = up_n(step)
                    send(self.part.at[other], self.at(other, own), (w, other), self.ids[step - 1])
                self.at(n, own)[...] = self.part[n]
            elif self.target is None:
                r.wo[n, w] = self.part[...]
            else:
                self.target[w] = self.part[...]

        def finish(self):
            if m.inside:
                for step in range(1, T):
                    got = pl.ds(pl.multiple_of(down_n(step) * m.RD, m.RD), m.RD)
                    arrive(self.at(n, got), self.ids[step - 1])

    ro, rq, ru = Rows(r.po, None), Rows(r.pq, r.wq), Rows(r.pu, r.wu)
    ro.start()
    rq.start()
    own_rows = rows_of(n, S)
    r.tok[own_rows, :] = r.x[...]
    tokens.start()
    r.sg[n] = r.seg[...]
    for step in range(1, T):
        send(r.sg.at[n], r.sg.at[n], (w, up_n(step)), si[step - 1])
    ru.start()
    r.dya[own_rows, :] = r.dy[...]
    cotangents.start()

    vector = r.pv[...].astype(F32)
    for step in range(1, T):
        arrive(r.vn.at[step - 1], vi[step - 1])
        vector = vector + r.vn[step - 1].astype(F32)
    r.wv[w] = vector.astype(BF)
    gv.along_z()
    gv.forward(0)
    ro.finish()
    go.along_z()
    go.forward(0)
    rq.finish()
    gq.along_z()
    gv.relays()
    tokens.middle()
    ru.finish()
    gu.along_z()
    gd.along_z()
    go.relays()
    gq.forward(0)
    tokens.close()
    gv.finish()
    vector = r.wv[0].astype(F32)
    for k in range(1, m.W):
        vector = vector + r.wv[k].astype(F32)
    r.vec[...] = vector

    heads = rows_of(n, m.Q)
    r.bias[...] = jnp.zeros_like(r.bias)
    r.bias[0:1, 0 : m.Q] = r.vec[2:3, heads]
    r.bias[0:1, 2 * m.Q : 3 * m.Q] = r.vec[3:4, heads]

    def first_norm(i):
        rows = rows_of(i, 16)
        unit, _ = normalize(r.tok[rows, :].astype(F32))
        r.a[rows, :] = (unit * r.vec[0:1, :] + r.vec[1:2, :]).astype(BF)

    half = L // 32
    loop(half, first_norm)
    cotangents.middle()
    go.finish()
    outs.start()
    gq.relay(1)
    loop(half, first_norm, half)
    for k in range(2, Z - 1):
        gq.relay(k)
    transpose(r.at, lambda i, j: r.a[i, j], L // 128, D // 128)
    gq.relay(Z - 1)
    gu.forward(0)
    cotangents.close()
    gq.finish()

    tile_q = 256 if m.NQ % 256 == 0 else 128

    def project(j):
        cols = rows_of(j, tile_q)
        value = nn(r.a[...], r.wq[:, :, cols].reshape(D, tile_q)) + r.bias[0:1, cols]
        r.qkv[:, cols] = value.astype(BF)

    loop(m.NQ // tile_q, project)
    for step in range(1, T):
        arrive(r.sg.at[down_n(step)], si[step - 1])
    gu.relay(1)
    outs.middle()

    lane = lax.broadcasted_iota(jnp.int32, (1, 128), 1)
    halves = [(lane // HEAD == k).astype(F32) for k in range(128 // HEAD)]
    scale = HEAD ** (-0.5)
    per = 128 // HEAD

    def pick(values):
        total = values[0] * halves[0]
        for k in range(1, per):
            total = total + values[k] * halves[k]
        return total

    def attend(s):
        rows = rows_of(s, S)
        keys = jnp.broadcast_to(r.sg[s, 0:1, :], (S, S))
        same = keys == keys.T
        for pair in range(m.Q // 128):
            q = r.qkv[rows, pair * 128 : pair * 128 + 128]
            k = r.qkv[rows, m.Q + pair * 128 : m.Q + pair * 128 + 128]
            v = r.qkv[rows, 2 * m.Q + pair * 128 : 2 * m.Q + pair * 128 + 128]
            mixed = []
            for half in range(per):
                score = nt(q * halves[half].astype(BF), k) * scale
                score = jnp.where(same, score, MASK_VALUE)
                power = jnp.exp(score - jnp.max(score, axis=-1, keepdims=True))
                weight = power / jnp.sum(power, axis=-1, keepdims=True)
                r.prob[s * m.NH + pair * per + half] = weight
                mixed.append(nn(weight.astype(BF), v))
            r.oa[n, rows, pair * 128 : pair * 128 + 128] = pick(mixed).astype(BF)

    loop(T, attend)
    mixes.start()
    for k in range(2, Z - 1):
        gu.relay(k)
    outs.close()
    mixes.middle()
    gu.relay(Z - 1)
    mixes.close()

    for t in range(T):
        r.oo[:, t * m.Q : (t + 1) * m.Q] = r.oa[t, own_rows, :]
    for t in range(T):
        cols = slice(t * m.Q, (t + 1) * m.Q)
        value = nn(r.oo[...], r.wo[t].reshape(D, m.Q))
        r.r1[:, cols] = r.x[:, cols].astype(F32) + value + r.vec[4:5, cols]

    def second_norm(i):
        rows = rows_of(i, 16)
        unit, _ = normalize(r.r1[rows, :])
        there = pl.ds(pl.multiple_of(n * S + i * 16, 16), 16)
        r.ca[there, :] = (unit * r.vec[5:6, :] + r.vec[6:7, :]).astype(BF)

    loop(S // 16, second_norm)
    seconds.start()
    for k in range(1, Z - 1):
        gd.relay(k)
    seconds.middle()
    for t in range(T):
        for k in range(m.Q // 128):
            base = t * m.Q + k * 128

            def turn(i, t=t, k=k, base=base):
                value = r.oa[t, rows_of(i, 128), k * 128 : k * 128 + 128].astype(F32)
                r.ot[base : base + 128, rows_of(i, 128)] = value.T.astype(BF)

            loop(L // 128, turn)
    seconds.close()
    gd.relay(Z - 1)
    transpose(r.ct, lambda i, j: r.ca[i, j], L // 128, D // 128)
    gu.finish()

    def expand(j):
        cols = rows_of(j, 256)
        value = nn(r.ca[...], r.wu[:, :, cols].reshape(D, 256))
        r.u[:, cols] = value + r.vec[pl.ds(8 + n, 1), cols]

    loop(m.F // 256, expand)

    def activate(i):
        rows = rows_of(i, 16)
        value = r.u[rows, :]
        phi = 0.5 * (1.0 + lax.erf(value * (0.5**0.5)))
        r.h[rows, :] = (value * phi).astype(BF)
        r.u[rows, :] = phi + value * (jnp.exp(-0.5 * value * value) * 0.3989422804014327)

    loop(L // 16, activate)
    transpose(r.ht, lambda i, j: r.h[i, j], L // 128, m.F // 128)
    sd.multiply(sd.order()[0], r.ht, r.dya)
    sd.along_x(sd.order()[0])
    for step in sd.order()[1:]:
        sd.multiply(step, r.ht, r.dya)
        sd.along_x(step)
    sd.along_z(sd.order()[0])
    gd.finish()

    group = 256 // m.FD

    def expand_back(j):
        cols = rows_of(j, 256)
        value = nt(r.dya[...], r.wd[rows_of(j, group)].reshape(256, D)) * r.u[:, cols]
        low = value.astype(BF)
        r.du[:, cols] = low
        r.sums[5, 0:1, cols] = jnp.sum(low.astype(F32), axis=0, keepdims=True)

    loop(m.F // 256, expand_back)
    width = 256 // m.RG

    def up_back(j):
        value = nt(r.du[...], r.wu[rows_of(j, width)].reshape(256, m.F))
        r.Pc[:, rows_of(j, 256)] = value.astype(BF)

    loop(D // 256, up_back)
    tc.start()
    for step in su.order():
        su.multiply(step, r.ct, r.du)
        su.along_x(step)
    tc.middle()

    def contract(j):
        cols = rows_of(j, 256)
        r.Py[:, cols] = nn(r.h[...], r.wd[:, :, cols].reshape(m.F, 256)).astype(BF)

    loop(D // 256, contract)
    ty.start()
    sd.along_z(sd.order()[1])
    tc.finish()
    r.sums[0:4] = jnp.zeros((4, 16, D), F32)

    def second_back(i):
        rows = rows_of(i, 16)
        grad = tc.rows(rows)
        cot = r.dy[rows, :].astype(F32)
        unit, inverse = normalize(r.r1[rows, :])
        total = cot + norm_back(grad, unit, inverse, r.vec[5:6, :])
        r.dr[rows, :] = total
        r.da[rows, :] = total.astype(BF)
        r.sums[0] += total
        r.sums[1] += grad * unit
        r.sums[2] += grad
        r.sums[3] += cot

    loop(S // 16, second_back)
    oi, ai = fresh(T - 1), fresh(T - 1)
    share = m.Q // m.RG
    for step in list(range(1, T)) + [0]:
        other = up_n(step) if step else n
        value = jnp.zeros((S, m.Q), F32)
        for t in range(T):
            block = r.wo[t, rows_of(other, share)].reshape(m.Q, m.Q)
            value = value + nt(r.da[:, t * m.Q : (t + 1) * m.Q], block)
        if step:
            r.dob[step] = value.astype(BF)
            send(r.dob.at[step], r.dof.at[own_rows], (w, other), oi[step - 1])
        else:
            r.dof[own_rows, :] = value.astype(BF)
    for step in range(1, T):
        other = up_n(step)
        r.dab[step] = r.da[:, rows_of(other, m.Q)]
        send(r.dab.at[step], r.daq.at[own_rows], (w, other), ai[step - 1])
    r.daq[own_rows, :] = r.da[:, rows_of(n, m.Q)]
    for step in sd.order()[2:-1]:
        sd.along_z(step)
    for step in range(1, T):
        arrive(r.dof.at[rows_of(down_n(step), S)], oi[step - 1])

    def attend_back(s):
        rows = rows_of(s, S)
        for pair in range(m.Q // 128):
            at = [pl.ds(b * m.Q + pair * 128, 128) for b in range(3)]
            q, k, v = r.qkv[rows, at[0]], r.qkv[rows, at[1]], r.qkv[rows, at[2]]
            cot = r.dof[rows, pair * 128 : pair * 128 + 128]
            dq, dk, dv = [], [], []
            for half in range(per):
                weight = r.prob[s * m.NH + pair * per + half]
                grad = nt(cot * halves[half].astype(BF), v)
                inner = jnp.sum(weight * grad, axis=-1, keepdims=True)
                ds = (weight * (grad - inner)).astype(BF)
                dq.append(nn(ds, k))
                dk.append(tn(ds, q))
                dv.append(tn(weight.astype(BF), cot))
            r.dqkv[rows, at[0]] = (pick(dq) * scale).astype(BF)
            r.dqkv[rows, at[1]] = (pick(dk) * scale).astype(BF)
            r.dqkv[rows, at[2]] = pick(dv).astype(BF)

    loop(T // 2, attend_back)
    su.along_z(su.order()[0])
    loop(T - T // 2, attend_back, T // 2)
    sd.along_z(sd.order()[-1])
    ty.middle()

    def project_back(j):
        value = nt(r.dqkv[...], r.wq[rows_of(j, width)].reshape(256, m.NQ))
        r.Pn[:, rows_of(j, 256)] = value.astype(BF)

    loop(D // 256, project_back)
    tin.start()
    for step in range(1, T):
        arrive(r.daq.at[rows_of(down_n(step), S)], ai[step - 1])
    for step in so.order():
        so.multiply(step, r.ot, r.daq)
        so.along_x(step)
    tin.middle()
    su.along_z(su.order()[1])
    for step in sq.order():
        sq.multiply(step, r.at, r.dqkv)
    for step in su.order()[2:-1]:
        su.along_z(step)

    r.vg[0] = jnp.zeros((16, D), F32)
    for k, row in enumerate((4, 5, 6, 7)):
        r.vg[0, row : row + 1, :] = jnp.sum(r.sums[k], axis=0, keepdims=True)
    r.vg[0, pl.ds(8 + n, 1), 0 : m.F] = r.sums[5, 0:1, 0 : m.F]

    def column(j):
        cols = rows_of(j, 128)
        there = pl.ds(pl.multiple_of(n * m.Q + j * 128, 128), 128)
        tail = pl.ds(pl.multiple_of(2 * m.Q + j * 128, 128), 128)
        r.vg[0, 2:3, there] = jnp.sum(r.dqkv[:, cols].astype(F32), axis=0, keepdims=True)
        r.vg[0, 3:4, there] = jnp.sum(r.dqkv[:, tail].astype(F32), axis=0, keepdims=True)

    loop(m.Q // 128, column)
    tin.finish()
    r.sums[0:2] = jnp.zeros((2, 16, D), F32)

    def first_back(i):
        rows = rows_of(i, 16)
        grad = tin.rows(rows)
        unit, inverse = normalize(r.x[rows, :].astype(F32))
        r.ig[rows, :] = r.dr[rows, :] + norm_back(grad, unit, inverse, r.vec[0:1, :])
        r.sums[0] += grad * unit
        r.sums[1] += grad

    loop(S // 16, first_back)
    r.vg[0, 0:1, :] = jnp.sum(r.sums[0], axis=0, keepdims=True)
    r.vg[0, 1:2, :] = jnp.sum(r.sums[1], axis=0, keepdims=True)
    vxi, vzi, vti = fresh(X - 1), fresh(Z - 1), fresh(T - 1)
    for dx in range(1, X):
        send(r.vg.at[0], r.vx.at[dx - 1], (z * X + up_x(dx), n), vxi[dx - 1])

    for step in sq.order():
        sq.along_x(step)
    su.along_z(su.order()[-1])
    ty.finish()

    def close(i):
        rows = rows_of(i, 16)
        r.bo[rows, :] = (r.r1[rows, :] + ty.rows(rows) + r.vec[7:8, :]).astype(BF)

    loop(S // 16, close)
    for step in so.order():
        so.along_z(step)
    total = r.vg[0]
    for dx in range(1, X):
        arrive(r.vx.at[dx - 1], vxi[dx - 1])
        total = total + r.vx[dx - 1]
    r.vg[1] = total
    for step in range(1, Z):
        send(r.vg.at[1], r.vz.at[step - 1], (up_z(step) * X + x, n), vzi[step - 1])
    sd.finish()

    def keep(i):
        rows = rows_of(i, 16)
        r.gd[rows, :] = sd.total(rows)

    loop(m.FD // 16, keep)
    du, do, dq = Deal("u", su, r.gu), Deal("o", so, r.go), Deal("q", sq, r.gq)
    for step in sq.order()[:2]:
        sq.along_z(step)
    du.start()
    for step in sq.order()[2:]:
        sq.along_z(step)
    do.start()
    dq.start()
    total = r.vg[1]
    for step in range(1, Z):
        arrive(r.vz.at[step - 1], vzi[step - 1])
        total = total + r.vz[step - 1]
    r.vg[2] = total
    for step in range(1, T):
        send(r.vg.at[2], r.vt.at[step - 1], (w, up_n(step)), vti[step - 1])
    du.finish()
    do.finish()
    dq.finish()
    total = r.vg[2]
    for step in range(1, T):
        arrive(r.vt.at[step - 1], vti[step - 1])
        total = total + r.vt[step - 1]
    r.gv[...] = total
    for one in sent:
        one.wait_send()


def block_step(m, args):
    scratch = scratch_of(m)
    kept = {"q": m.NQ, "o": m.Q, "u": m.F}
    grads = [
        jax.ShapeDtypeStruct((m.T, m.RD, cols) if m.inside else (m.RG, cols), BF)
        for cols in kept.values()
    ]
    vmem = pl.BlockSpec(memory_space=pltpu.VMEM)

    def kernel(*refs):
        block_kernel(m, list(scratch), *refs)

    return pl.pallas_call(
        kernel,
        out_shape=[
            jax.ShapeDtypeStruct((m.S, D), BF),
            jax.ShapeDtypeStruct((m.S, D), F32),
            *grads,
            jax.ShapeDtypeStruct((m.FD, D), F32),
            jax.ShapeDtypeStruct((16, D), F32),
        ],
        in_specs=[vmem] * len(args),
        out_specs=[vmem] * 7,
        scratch_shapes=[pltpu.VMEM(shape, kind) for shape, kind in scratch.values()]
        + [pltpu.SemaphoreType.DMA((semaphores_of(m),))],
        compiler_params=pltpu.CompilerParams(
            collective_id=0, has_side_effects=True, vmem_limit_bytes=62 * 1024 * 1024
        ),
        name="block_step",
    )(*args)


def body(
    tokens,
    cotangent,
    segment_ids,
    w_qkv,
    w_out,
    w_up,
    w_down,
    vectors,
    moments_qkv,
    moments_out,
    moments_up,
    moments_down,
    moments_vec,
):
    wide, narrow = lax.axis_size("wide"), lax.axis_size("narrow")
    m = layout(wide, narrow, tokens.shape[0])
    device = lax.axis_index("wide") * narrow + lax.axis_index("narrow")
    first_row = device * m.RD

    pq = w_qkv.astype(BF).reshape(m.RD, 3, m.T, m.Q).transpose(2, 0, 1, 3)
    po = w_out.astype(BF).reshape(m.RD, m.T, m.Q).transpose(1, 0, 2)
    pu = w_up.astype(BF).reshape(m.RD, m.W, m.T, m.FD).transpose(2, 0, 1, 3)
    parts = [pq.reshape(m.T, m.RD, m.NQ), po, pu.reshape(m.T, m.RD, m.F)]
    if not m.inside:
        parts = [
            lax.all_to_all(part, "narrow", 0, 0).reshape(m.RG, part.shape[2]) for part in parts
        ]
    low = vectors.astype(BF).T
    spot = jnp.zeros((12, D), BF)
    spot = lax.dynamic_update_slice(spot, low, (0, first_row))
    rise = spot[8:].reshape(m.W, m.T, m.FD).transpose(1, 0, 2).reshape(m.T, m.F)
    rise = jnp.pad(rise, ((0, 8 - m.T), (0, D - m.F)))
    packed = jnp.concatenate([spot[:8], rise], axis=0)
    segments = jnp.broadcast_to(segment_ids.astype(F32), (8, m.S))

    block_out, input_grad, gq, go, gu, gd, gv = block_step(
        m, (tokens, cotangent, segments, *parts, w_down.astype(BF), packed)
    )
    if not m.inside:
        gq, go, gu = [
            lax.all_to_all(g.reshape(m.T, m.RD, g.shape[1]), "narrow", 0, 0) for g in (gq, go, gu)
        ]
    grad_qkv = gq.reshape(m.T, m.RD, 3, m.Q).transpose(1, 2, 0, 3).reshape(m.RD, 3 * D)
    grad_out = go.transpose(1, 0, 2).reshape(m.RD, D)
    grad_up = gu.reshape(m.T, m.RD, m.W, m.FD).transpose(1, 2, 0, 3).reshape(m.RD, FF)
    rise = gv[8 : 8 + m.T, : m.F].reshape(m.T, m.W, m.FD).transpose(1, 0, 2).reshape(FF // D, D)
    grad_vec = lax.dynamic_slice(
        jnp.concatenate([gv[:8], rise], axis=0), (0, first_row), (12, m.RD)
    ).T

    new_qkv, state_qkv, copy_qkv = adam_update(
        w_qkv, moments_qkv, grad_qkv.astype(F32), RATE_MATRIX, WEIGHT_DECAY
    )
    new_out, state_out, copy_out = adam_update(
        w_out, moments_out, grad_out.astype(F32), RATE_MATRIX, WEIGHT_DECAY
    )
    new_up, state_up, copy_up = adam_update(
        w_up, moments_up, grad_up.astype(F32), RATE_MATRIX, WEIGHT_DECAY
    )
    new_down, state_down, copy_down = adam_update(w_down, moments_down, gd, RATE_MATRIX, WEIGHT_DECAY)
    new_vectors, state_vectors, copy_vectors = adam_update(
        vectors, moments_vec, grad_vec, RATE_VECTOR, 0.0
    )
    return (
        block_out,
        input_grad,
        new_qkv,
        new_out,
        new_up,
        new_down,
        new_vectors,
        state_qkv,
        state_out,
        state_up,
        state_down,
        state_vectors,
        copy_qkv,
        copy_out,
        copy_up,
        copy_down,
        copy_vectors,
    )


def solution(mesh):
    flat = P(("wide", "narrow"), None)
    pair = P(None, ("wide", "narrow"), None)
    return jax.shard_map(
        body,
        mesh=mesh,
        in_specs=(flat,) * 8 + (pair,) * 5,
        out_specs=(flat,) * 7 + (pair,) * 5 + (flat,) * 5,
        check_vma=False,
    )
```

```python
import types

import jax
import jax.numpy as jnp
from jax import lax
from jax.experimental import pallas as pl
from jax.experimental.pallas import tpu as pltpu
from jax.sharding import PartitionSpec as P

D = 1024
HEADS = 16
FF = 4096
STEP = 3
HEAD = D // HEADS

NORM_EPSILON = 1e-06
MASK_VALUE = -1e30
MOMENT_DECAY = 0.5
RATE_MATRIX = 0.04
RATE_VECTOR = 0.2
WEIGHT_DECAY = 0.1
ADAM_EPSILON = 1e-08

BF = jnp.bfloat16
F32 = jnp.float32
MESH = pl.DeviceIdType.MESH


def adam_update(master, moments, gradient, rate, decay):
    first_moment = MOMENT_DECAY * moments[0] + (1.0 - MOMENT_DECAY) * gradient
    second_moment = MOMENT_DECAY * moments[1] + (1.0 - MOMENT_DECAY) * gradient * gradient
    correction = 1.0 - MOMENT_DECAY**STEP
    normalized = first_moment / correction / (jnp.sqrt(second_moment / correction) + ADAM_EPSILON)
    updated = master - rate * (normalized + decay * master)
    return (updated, jnp.stack([first_moment, second_moment]), updated.astype(BF))


def nn(left, right):
    return jnp.dot(left, right, preferred_element_type=F32)


def nt(left, right):
    return lax.dot_general(left, right, (((1,), (1,)), ((), ())), preferred_element_type=F32)


def tn(left, right):
    return lax.dot_general(left, right, (((0,), (0,)), ((), ())), preferred_element_type=F32)


def loop(count, body, first=0):
    def step(index, carry):
        body(index)
        return carry

    lax.fori_loop(first, first + count, step, 0)


def normalize(rows):
    center = rows - jnp.mean(rows, axis=-1, keepdims=True)
    inverse = lax.rsqrt(jnp.mean(center * center, axis=-1, keepdims=True) + NORM_EPSILON)
    return center * inverse, inverse


def norm_back(grad, unit, inverse, gain):
    scaled = grad * gain
    first = jnp.mean(scaled, axis=-1, keepdims=True)
    second = jnp.mean(scaled * unit, axis=-1, keepdims=True)
    return inverse * (scaled - first - unit * second)


def layout(wide, narrow, length):
    m = types.SimpleNamespace()
    m.W, m.T, m.S = wide, narrow, length
    m.Y = narrow // 2
    m.X = narrow // 2
    m.Z = wide // m.X
    m.L = length * narrow
    m.Q = D // narrow
    m.NQ = 3 * m.Q
    m.F = FF // narrow
    m.RG = D // wide
    m.RD = D // (wide * narrow)
    m.FD = FF // (wide * narrow)
    m.NH = m.Q // HEAD
    m.inside = m.RD % 16 == 0
    m.line = m.Z == 4
    return m


def scratch_of(m):
    def weights(name, rows, cols):
        return {
            name: ((m.W, rows, cols), BF),
        }

    def scatter(name, rows, cols):
        return {
            "G" + name: ((m.W, rows, cols), BF),
            "X" + name: ((m.X - 1, m.Z, rows, cols), BF),
            "S" + name: ((m.Z, rows, cols), BF),
            "Z" + name: ((m.Z if m.line else m.Z - 1, rows, cols), BF),
        }

    def spread(name, cols):
        return {
            "T" + name: ((m.T, m.RD, cols), BF),
            "N" + name: ((m.T, m.RD, cols), BF),
        }

    def partial(name):
        return {
            "P" + name: ((m.L, D), BF),
            "C" + name: ((m.Y, m.S, D), BF),
            "M" + name: ((m.Y, m.S, D), BF),
            "A" + name: ((m.S, D), F32),
            "R" + name: ((m.Y - 1, m.S, D), BF),
        }

    out = {}
    out.update(weights("wq", m.RG, m.NQ))
    out["wo"] = ((m.T, m.W, m.RG, m.Q), BF)
    out.update(weights("wu", m.RG, m.F))
    out.update(weights("wd", m.FD, D))
    out.update(weights("wv", 16, D))
    out["vn"] = ((m.T - 1, 16, D), BF)
    out.update(scatter("q", m.RG, m.NQ))
    out.update(scatter("o", m.RG, m.Q))
    out.update(scatter("u", m.RG, m.F))
    out.update(scatter("d", m.FD, D))
    if m.inside:
        out.update(spread("q", m.NQ))
        out.update(spread("o", m.Q))
        out.update(spread("u", m.F))
    for name in ("y", "c", "n"):
        out.update(partial(name))
    for name in ("tok", "dya", "ca"):
        out[name] = ((m.L, D), BF)
    out["oa"] = ((m.T, m.L, m.Q), BF)
    out["sg"] = ((m.T, 8, m.S), F32)
    out["vec"] = ((16, D), F32)
    out["bias"] = ((8, m.NQ), F32)
    out["a"] = ((m.L, D), BF)
    out["at"] = ((D, m.L), BF)
    out["ct"] = ((D, m.L), BF)
    out["ot"] = ((D, m.L), BF)
    out["h"] = ((m.L, m.F), BF)
    out["ht"] = ((m.F, m.L), BF)
    out["u"] = ((m.L, m.F), F32)
    out["du"] = ((m.L, m.F), BF)
    out["qkv"] = ((m.L, m.NQ), BF)
    out["dqkv"] = ((m.L, m.NQ), BF)
    out["prob"] = ((m.T * m.NH, m.S, m.S), F32)
    out["oo"] = ((m.S, D), BF)
    out["r1"] = ((m.S, D), F32)
    out["dr"] = ((m.S, D), F32)
    out["da"] = ((m.S, D), BF)
    out["dob"] = ((m.T, m.S, m.Q), BF)
    out["dab"] = ((m.T, m.S, m.Q), BF)
    out["dof"] = ((m.L, m.Q), BF)
    out["daq"] = ((m.L, m.Q), BF)
    out["sums"] = ((6, 16, D), F32)
    out["vg"] = ((3, 16, D), F32)
    out["vx"] = ((m.X - 1, 16, D), F32)
    out["vz"] = ((m.Z - 1, 16, D), F32)
    out["vt"] = ((m.T - 1, 16, D), F32)
    return out


def semaphores_of(m):
    gather = 2 * m.Z + m.Z * (m.X - 1)
    scatter = m.Z * (m.X - 1) + 2 * m.Z
    pair = (m.Y - 1) + m.Y
    direct = m.T - 1
    total = 5 * gather + 4 * scatter + 8 * pair + 10 * direct + (m.X - 1) + (m.Z - 1) + direct
    return 2 * total + 16


def block_kernel(m, names, *refs):
    inputs = ("x", "dy", "seg", "pq", "po", "pu", "pd", "pv")
    outputs = ("bo", "ig", "gq", "go", "gu", "gd", "gv")
    r = types.SimpleNamespace(**dict(zip(inputs + outputs + tuple(names) + ("sem",), refs)))
    w, n = lax.axis_index("wide"), lax.axis_index("narrow")
    z, x = w // m.X, lax.rem(w, m.X)
    y, c = n // 2, lax.rem(n, 2)
    sibling = (w, 2 * y + 1 - c)
    L, S, T, X, Y, Z = m.L, m.S, m.T, m.X, m.Y, m.Z
    sent = []
    used = [0]

    def fresh(count):
        first = used[0]
        used[0] += count
        return [first + k for k in range(count)]

    inner = (z == 1) | (z == 2)
    mate = jnp.where(z < 2, 1 - z, 5 - z)
    fin, fend = jnp.where(z < 2, 2, 1), jnp.where(z < 2, 3, 0)

    def copy(src, dst, device, index, out=None):
        return pltpu.make_async_remote_copy(
            src_ref=src,
            dst_ref=dst,
            send_sem=r.sem.at[2 * (index if out is None else out)],
            recv_sem=r.sem.at[2 * index + 1],
            device_id=device,
            device_id_type=MESH,
        )

    def send(src, dst, device, index, out=None, only=None):
        one = copy(src, dst, device, index, out)
        if only is None:
            one.start()
        else:
            pl.when(only)(one.start)
        sent.append((one, only))

    def arrive(dst, index):
        copy(dst, dst, sibling, index).wait_recv()

    def up_z(step):
        return lax.rem(z + step, Z)

    def down_z(step):
        return lax.rem(z + Z - step, Z)

    def up_x(step):
        return lax.rem(x + step, X)

    def down_x(step):
        return lax.rem(x + X - step, X)

    def up_n(step):
        return lax.rem(n + step, T)

    def down_n(step):
        return lax.rem(n + T - step, T)

    def at_y(step):
        return lax.rem(y + Y + step, Y)

    def rows_of(index, size):
        return pl.ds(pl.multiple_of(index * size, size), size)

    class Gather:
        def __init__(self, ref):
            self.ref = ref
            self.zi = fresh(Z - 1)[0]
            self.out = fresh(4)
            self.xi = fresh(Z * (X - 1))[0]

        def to_z(self, block, there, index, out, only=None):
            send(self.ref.at[block], self.ref.at[block], (there * X + x, n), self.zi + index, out, only)

        def along_z(self):
            if m.line:
                self.to_z(w, fin, jnp.where(inner, 1, 2), self.out[0])
                self.to_z(w, mate, 0, self.out[1])
                return
            for step in range(1, Z):
                self.to_z(w, up_z(step), step - 1, None)

        def forward(self, step, only=None):
            block = down_z(step) * X + x
            for dx in range(1, X):
                send(
                    self.ref.at[block],
                    self.ref.at[block],
                    (z * X + up_x(dx), n),
                    self.xi + step * (X - 1) + dx - 1,
                    only=only,
                )

        def relay(self, k, who):
            if not m.line and who == "end":
                return
            only = None
            if m.line:
                only = inner if who == "inner" else jnp.logical_not(inner)
            step, index = k, k - 1
            if m.line:
                index = jnp.where(inner, k % 3, k - 1)
                there = jnp.where(index == 0, mate, jnp.where(index == 1, fin, fend))
                step = lax.rem(z + Z - there, Z)
            block = down_z(step) * X + x
            if only is None:
                arrive(self.ref.at[block], self.zi + index)
            else:
                pl.when(only)(lambda: arrive(self.ref.at[block], self.zi + index))
            if m.line and k < 3 and who == "inner":
                self.to_z(block, mate, index, self.out[1 + k], inner)
            self.forward(step, only)

        def inside(self, steps):
            for k in steps:
                self.relay(k, "inner")

        def ends(self, steps):
            for k in steps:
                self.relay(k, "end")

        def finish(self):
            for step in range(Z):
                for dx in range(1, X):
                    block = (down_z(step) if step else z) * X + down_x(dx)
                    arrive(self.ref.at[block], self.xi + step * (X - 1) + dx - 1)

    class Share:
        def __init__(self, slot):
            self.slot = slot
            self.yi = fresh(Y - 1)
            self.ci = fresh(Y)

        def start(self):
            for step in range(1, Y):
                send(self.slot(n), self.slot(n), (w, 2 * at_y(step) + c), self.yi[step - 1])
            send(self.slot(n), self.slot(n), sibling, self.ci[0])

        def middle(self):
            for step in range(1, Y):
                block = 2 * at_y(-step) + c
                arrive(self.slot(block), self.yi[step - 1])
                send(self.slot(block), self.slot(block), sibling, self.ci[step])

        def close(self):
            for step in range(Y):
                block = 2 * at_y(-step) + 1 - c
                arrive(self.slot(block), self.ci[step])

    class Total:
        def __init__(self, name):
            self.part = getattr(r, "P" + name)
            self.core = getattr(r, "C" + name)
            self.mid = getattr(r, "M" + name)
            self.own = getattr(r, "A" + name)
            self.last = getattr(r, "R" + name)
            self.yi = fresh(Y - 1)
            self.ci = fresh(Y)

        def start(self):
            for step in list(range(1, Y)) + [0]:
                block = 2 * at_y(step) + 1 - c
                send(self.part.at[rows_of(block, S)], self.core.at[step], sibling, self.ci[step])

        def middle(self):
            for step in list(range(1, Y)) + [0]:
                block = 2 * at_y(step) + c
                arrive(self.core.at[step], self.ci[step])

                def add(i):
                    rows = rows_of(i, 16)
                    mine = self.part[pl.ds(pl.multiple_of(block * S + i * 16, 16), 16), :]
                    total = mine.astype(F32) + self.core[step, rows, :].astype(F32)
                    if step:
                        self.mid[step, rows, :] = total.astype(BF)
                    else:
                        self.own[rows, :] = total

                loop(S // 16, add)
                if step:
                    send(self.mid.at[step], self.last.at[step - 1], (w, block), self.yi[step - 1])

        def finish(self):
            for step in range(1, Y):
                arrive(self.last.at[step - 1], self.yi[step - 1])

        def rows(self, rows):
            total = self.own[rows, :]
            for step in range(1, Y):
                total = total + self.last[step - 1, rows, :].astype(F32)
            return total

    class Scatter:
        def __init__(self, name, rows, cols):
            self.rows, self.cols = rows, cols
            self.grad = getattr(r, "G" + name)
            self.fromx = getattr(r, "X" + name)
            self.sums = getattr(r, "S" + name)
            self.fromz = getattr(r, "Z" + name)
            self.xi = fresh(Z * (X - 1))
            self.zi = fresh(Z)[0]
            self.out = fresh(Z - 1)
            self.chunk = 16 if cols > 512 else 32
            if rows % self.chunk:
                self.chunk = 16

        def order(self):
            return list(range(Z))

        def there(self, k):
            if k == Z - 1:
                return z
            return (fin, fend, mate)[k] if m.line else up_z(k + 1)

        def multiply(self, k, left, right):
            first = self.there(k)
            high = X * self.rows
            tile = 256 if self.cols % 256 == 0 else 128

            def one(j):
                cols = rows_of(j, tile)
                value = nn(left[rows_of(first, high), :], right[:, cols]).astype(BF)
                value = value.reshape(X, self.rows, tile)
                self.grad[rows_of(first, X), :, cols] = value

            loop(self.cols // tile, one)

        def along_x(self, k):
            first = self.there(k)
            for dx in range(1, X):
                other = up_x(dx)
                send(
                    self.grad.at[first * X + other],
                    self.fromx.at[dx - 1, k],
                    (z * X + other, n),
                    self.xi[k * (X - 1) + dx - 1],
                )

        def along_z(self, k):
            block = self.there(k) * X + x
            for dx in range(1, X):
                arrive(self.fromx.at[dx - 1, k], self.xi[k * (X - 1) + dx - 1])

            def add(i):
                rows = rows_of(i, self.chunk)
                total = self.grad[block, rows, :].astype(F32)
                for dx in range(1, X):
                    total = total + self.fromx[dx - 1, k, rows, :].astype(F32)
                self.sums[k, rows, :] = total.astype(BF)

            loop(self.rows // self.chunk, add)
            if k == Z - 1:
                return
            if not m.line:
                self.to_z(k, block, k)
            elif k == 2:
                self.to_z(k, mate * X + x, 2)
            else:
                self.to_z(k, mate * X + x, k, z != jnp.where(z < 2, 1, 2))

        def to_z(self, k, block, slot, only=None):
            send(self.sums.at[k], self.fromz.at[slot], (block, n), self.zi + slot, self.out[k], only)

        def join(self, k):
            if not m.line:
                return

            @pl.when(inner)
            def _():
                arrive(self.fromz.at[k], self.zi + k)

                def add(i):
                    rows = rows_of(i, self.chunk)
                    total = self.sums[k, rows, :].astype(F32) + self.fromz[k, rows, :].astype(F32)
                    self.sums[k, rows, :] = total.astype(BF)

                loop(self.rows // self.chunk, add)
                copy(
                    self.sums.at[k], self.fromz.at[3], (self.there(k) * X + x, n), self.zi + 3, self.out[k]
                ).start()

            sent.append(
                (
                    copy(
                        self.sums.at[k], self.fromz.at[3], (self.there(k) * X + x, n), self.zi + 3, self.out[k]
                    ),
                    inner,
                )
            )

        def last(self):
            return [2, 3] if m.line else list(range(Z - 1))

        def finish(self):
            for slot in self.last():
                arrive(self.fromz.at[slot], self.zi + slot)

        def total(self, rows):
            total = self.sums[Z - 1, rows, :].astype(F32)
            for slot in self.last():
                total = total + self.fromz[slot, rows, :].astype(F32)
            return total

    class Deal:
        def __init__(self, name, scatter, out):
            self.scatter, self.out = scatter, out
            if m.inside:
                self.turn = getattr(r, "T" + name)
                self.got = getattr(r, "N" + name)
                self.ni = fresh(T - 1)

        def start(self):
            self.scatter.finish()
            if not m.inside:
                def store(i):
                    rows = rows_of(i, self.scatter.chunk)
                    self.out[rows, :] = self.scatter.total(rows).astype(BF)

                loop(self.scatter.rows // self.scatter.chunk, store)
                return

            def add(i):
                self.turn[i] = self.scatter.total(rows_of(i, m.RD)).astype(BF)

            loop(T, add)
            for step in range(1, T):
                other = up_n(step)
                send(self.turn.at[other], self.got.at[step], (w, other), self.ni[step - 1])

        def finish(self):
            if not m.inside:
                return
            self.out[n] = self.turn[n]
            for step in range(1, T):
                arrive(self.got.at[step], self.ni[step - 1])
                self.out[down_n(step)] = self.got[step]

    def transpose(target, source, count_rows, count_cols):
        def tile(k):
            i, j = k // count_cols, lax.rem(k, count_cols)
            value = source(rows_of(i, 128), rows_of(j, 128)).astype(F32)
            target[rows_of(j, 128), rows_of(i, 128)] = value.T.astype(BF)

        loop(count_rows * count_cols, tile)

    barrier = pltpu.get_barrier_semaphore()
    peers = [(w, up_n(k)) for k in range(1, T)]
    peers += [(up_z(k) * X + x, n) for k in range(1, Z)]
    peers += [(z * X + up_x(k), n) for k in range(1, X)]
    for peer in peers:
        pl.semaphore_signal(barrier, inc=1, device_id=peer, device_id_type=MESH)
    pl.semaphore_wait(barrier, len(peers))

    gv, gq, gu, gd = Gather(r.wv), Gather(r.wq), Gather(r.wu), Gather(r.wd)
    go = Gather(r.wo.at[n])
    tokens = Share(lambda k: r.tok.at[rows_of(k, S)])
    cotangents = Share(lambda k: r.dya.at[rows_of(k, S)])
    outs = Share(lambda k: r.wo.at[k])
    mixes = Share(lambda k: r.oa.at[k])
    seconds = Share(lambda k: r.ca.at[rows_of(k, S)])
    ty, tc, tin = Total("y"), Total("c"), Total("n")
    sd, su = Scatter("d", m.FD, D), Scatter("u", m.RG, m.F)
    so, sq = Scatter("o", m.RG, m.Q), Scatter("q", m.RG, m.NQ)

    vi, si = fresh(T - 1), fresh(T - 1)
    for step in range(1, T):
        send(r.pv, r.vn.at[step - 1], (w, up_n(step)), vi[step - 1])
    r.wd[w] = r.pd[...]
    gd.forward(0)

    class Rows:
        def __init__(self, part, target):
            self.part, self.target = part, target
            self.ids = fresh(T - 1) if m.inside else []

        def at(self, k, rows):
            return r.wo.at[k, w, rows] if self.target is None else self.target.at[w, rows]

        def start(self):
            if m.inside:
                own = pl.ds(pl.multiple_of(n * m.RD, m.RD), m.RD)
                for step in range(1, T):
                    other = up_n(step)
                    send(self.part.at[other], self.at(other, own), (w, other), self.ids[step - 1])
                self.at(n, own)[...] = self.part[n]
            elif self.target is None:
                r.wo[n, w] = self.part[...]
            else:
                self.target[w] = self.part[...]

        def finish(self):
            if m.inside:
                for step in range(1, T):
                    got = pl.ds(pl.multiple_of(down_n(step) * m.RD, m.RD), m.RD)
                    arrive(self.at(n, got), self.ids[step - 1])

    ro, rq, ru = Rows(r.po, None), Rows(r.pq, r.wq), Rows(r.pu, r.wu)
    ro.start()
    rq.start()
    own_rows = rows_of(n, S)
    r.tok[own_rows, :] = r.x[...]
    tokens.start()
    r.sg[n] = r.seg[...]
    for step in range(1, T):
        send(r.sg.at[n], r.sg.at[n], (w, up_n(step)), si[step - 1])
    ru.start()
    r.dya[own_rows, :] = r.dy[...]
    cotangents.start()

    vector = r.pv[...].astype(F32)
    for step in range(1, T):
        arrive(r.vn.at[step - 1], vi[step - 1])
        vector = vector + r.vn[step - 1].astype(F32)
    r.wv[w] = vector.astype(BF)
    early, late = range(1, Z - 1), range(Z - 1, Z)
    gv.along_z()
    gv.forward(0)
    ro.finish()
    go.along_z()
    go.forward(0)
    gv.inside(early)
    rq.finish()
    gq.along_z()
    gq.forward(0)
    go.inside(early)
    tokens.middle()
    ru.finish()
    gv.inside(late)
    gv.ends(range(1, Z))
    tokens.close()
    gv.finish()
    vector = r.wv[0].astype(F32)
    for k in range(1, m.W):
        vector = vector + r.wv[k].astype(F32)
    r.vec[...] = vector

    heads = rows_of(n, m.Q)
    r.bias[...] = jnp.zeros_like(r.bias)
    r.bias[0:1, 0 : m.Q] = r.vec[2:3, heads]
    r.bias[0:1, 2 * m.Q : 3 * m.Q] = r.vec[3:4, heads]

    def first_norm(i):
        rows = rows_of(i, 16)
        unit, _ = normalize(r.tok[rows, :].astype(F32))
        r.a[rows, :] = (unit * r.vec[0:1, :] + r.vec[1:2, :]).astype(BF)

    half = L // 32
    gq.inside(early)
    gu.along_z()
    go.inside(late)
    go.ends(range(1, Z))
    loop(half, first_norm)
    cotangents.middle()
    gq.inside(late)
    gq.ends(range(1, 2))
    go.finish()
    outs.start()
    loop(half, first_norm, half)
    gq.ends(range(2, Z - 1))
    transpose(r.at, lambda i, j: r.a[i, j], L // 128, D // 128)
    gq.ends(late)
    gu.forward(0)
    cotangents.close()
    gq.finish()

    tile_q = 256 if m.NQ % 256 == 0 else 128

    def project(j):
        cols = rows_of(j, tile_q)
        value = nn(r.a[...], r.wq[:, :, cols].reshape(D, tile_q)) + r.bias[0:1, cols]
        r.qkv[:, cols] = value.astype(BF)

    loop(m.NQ // tile_q, project)
    for step in range(1, T):
        arrive(r.sg.at[down_n(step)], si[step - 1])
    gu.inside(early)
    gd.along_z()
    gu.ends(range(1, 2))
    outs.middle()

    lane = lax.broadcasted_iota(jnp.int32, (1, 128), 1)
    halves = [(lane // HEAD == k).astype(F32) for k in range(128 // HEAD)]
    scale = HEAD ** (-0.5)
    per = 128 // HEAD

    def pick(values):
        total = values[0] * halves[0]
        for k in range(1, per):
            total = total + values[k] * halves[k]
        return total

    def attend(s):
        rows = rows_of(s, S)
        keys = jnp.broadcast_to(r.sg[s, 0:1, :], (S, S))
        same = keys == keys.T
        for pair in range(m.Q // 128):
            q = r.qkv[rows, pair * 128 : pair * 128 + 128]
            k = r.qkv[rows, m.Q + pair * 128 : m.Q + pair * 128 + 128]
            v = r.qkv[rows, 2 * m.Q + pair * 128 : 2 * m.Q + pair * 128 + 128]
            mixed = []
            for half in range(per):
                score = nt(q * halves[half].astype(BF), k) * scale
                score = jnp.where(same, score, MASK_VALUE)
                power = jnp.exp(score - jnp.max(score, axis=-1, keepdims=True))
                weight = power / jnp.sum(power, axis=-1, keepdims=True)
                r.prob[s * m.NH + pair * per + half] = weight
                mixed.append(nn(weight.astype(BF), v))
            r.oa[n, rows, pair * 128 : pair * 128 + 128] = pick(mixed).astype(BF)

    loop(T, attend)
    mixes.start()
    gu.inside(late)
    gu.ends(range(2, Z - 1))
    outs.close()
    mixes.middle()
    gu.ends(late)
    mixes.close()

    for t in range(T):
        r.oo[:, t * m.Q : (t + 1) * m.Q] = r.oa[t, own_rows, :]
    for t in range(T):
        cols = slice(t * m.Q, (t + 1) * m.Q)
        value = nn(r.oo[...], r.wo[t].reshape(D, m.Q))
        r.r1[:, cols] = r.x[:, cols].astype(F32) + value + r.vec[4:5, cols]

    def second_norm(i):
        rows = rows_of(i, 16)
        unit, _ = normalize(r.r1[rows, :])
        there = pl.ds(pl.multiple_of(n * S + i * 16, 16), 16)
        r.ca[there, :] = (unit * r.vec[5:6, :] + r.vec[6:7, :]).astype(BF)

    loop(S // 16, second_norm)
    seconds.start()
    gd.inside(early)
    gd.ends(range(1, 2))
    seconds.middle()
    for t in range(T):
        for k in range(m.Q // 128):
            base = t * m.Q + k * 128

            def turn(i, t=t, k=k, base=base):
                value = r.oa[t, rows_of(i, 128), k * 128 : k * 128 + 128].astype(F32)
                r.ot[base : base + 128, rows_of(i, 128)] = value.T.astype(BF)

            loop(L // 128, turn)
    seconds.close()
    gd.inside(late)
    gd.ends(range(2, Z - 1))
    transpose(r.ct, lambda i, j: r.ca[i, j], L // 128, D // 128)
    gd.ends(late)
    gu.finish()

    def expand(j):
        cols = rows_of(j, 256)
        value = nn(r.ca[...], r.wu[:, :, cols].reshape(D, 256))
        r.u[:, cols] = value + r.vec[pl.ds(8 + n, 1), cols]

    loop(m.F // 256, expand)

    def activate(i):
        rows = rows_of(i, 16)
        value = r.u[rows, :]
        phi = 0.5 * (1.0 + lax.erf(value * (0.5**0.5)))
        r.h[rows, :] = (value * phi).astype(BF)
        r.u[rows, :] = phi + value * (jnp.exp(-0.5 * value * value) * 0.3989422804014327)

    loop(L // 16, activate)
    transpose(r.ht, lambda i, j: r.h[i, j], L // 128, m.F // 128)
    sd.multiply(sd.order()[0], r.ht, r.dya)
    sd.along_x(sd.order()[0])
    for step in sd.order()[1:]:
        sd.multiply(step, r.ht, r.dya)
        sd.along_x(step)
    sd.along_z(sd.order()[0])
    gd.finish()

    group = 256 // m.FD

    def expand_back(j):
        cols = rows_of(j, 256)
        value = nt(r.dya[...], r.wd[rows_of(j, group)].reshape(256, D)) * r.u[:, cols]
        low = value.astype(BF)
        r.du[:, cols] = low
        r.sums[5, 0:1, cols] = jnp.sum(low.astype(F32), axis=0, keepdims=True)

    loop(m.F // 256, expand_back)
    width = 256 // m.RG

    def up_back(j):
        value = nt(r.du[...], r.wu[rows_of(j, width)].reshape(256, m.F))
        r.Pc[:, rows_of(j, 256)] = value.astype(BF)

    loop(D // 256, up_back)
    tc.start()
    for step in su.order():
        su.multiply(step, r.ct, r.du)
        su.along_x(step)
    tc.middle()

    def contract(j):
        cols = rows_of(j, 256)
        r.Py[:, cols] = nn(r.h[...], r.wd[:, :, cols].reshape(m.F, 256)).astype(BF)

    loop(D // 256, contract)
    ty.start()
    sd.along_z(1)
    tc.finish()
    r.sums[0:4] = jnp.zeros((4, 16, D), F32)

    def second_back(i):
        rows = rows_of(i, 16)
        grad = tc.rows(rows)
        cot = r.dy[rows, :].astype(F32)
        unit, inverse = normalize(r.r1[rows, :])
        total = cot + norm_back(grad, unit, inverse, r.vec[5:6, :])
        r.dr[rows, :] = total
        r.da[rows, :] = total.astype(BF)
        r.sums[0] += total
        r.sums[1] += grad * unit
        r.sums[2] += grad
        r.sums[3] += cot

    loop(S // 16, second_back)
    oi, ai = fresh(T - 1), fresh(T - 1)
    share = m.Q // m.RG
    for step in list(range(1, T)) + [0]:
        other = up_n(step) if step else n
        value = jnp.zeros((S, m.Q), F32)
        for t in range(T):
            block = r.wo[t, rows_of(other, share)].reshape(m.Q, m.Q)
            value = value + nt(r.da[:, t * m.Q : (t + 1) * m.Q], block)
        if step:
            r.dob[step] = value.astype(BF)
            send(r.dob.at[step], r.dof.at[own_rows], (w, other), oi[step - 1])
        else:
            r.dof[own_rows, :] = value.astype(BF)
    for step in range(1, T):
        other = up_n(step)
        r.dab[step] = r.da[:, rows_of(other, m.Q)]
        send(r.dab.at[step], r.daq.at[own_rows], (w, other), ai[step - 1])
    r.daq[own_rows, :] = r.da[:, rows_of(n, m.Q)]
    for step in sd.order()[2:-1]:
        sd.along_z(step)
    sd.join(0)
    for step in range(1, T):
        arrive(r.dof.at[rows_of(down_n(step), S)], oi[step - 1])

    def attend_back(s):
        rows = rows_of(s, S)
        for pair in range(m.Q // 128):
            at = [pl.ds(b * m.Q + pair * 128, 128) for b in range(3)]
            q, k, v = r.qkv[rows, at[0]], r.qkv[rows, at[1]], r.qkv[rows, at[2]]
            cot = r.dof[rows, pair * 128 : pair * 128 + 128]
            dq, dk, dv = [], [], []
            for half in range(per):
                weight = r.prob[s * m.NH + pair * per + half]
                grad = nt(cot * halves[half].astype(BF), v)
                inner = jnp.sum(weight * grad, axis=-1, keepdims=True)
                ds = (weight * (grad - inner)).astype(BF)
                dq.append(nn(ds, k))
                dk.append(tn(ds, q))
                dv.append(tn(weight.astype(BF), cot))
            r.dqkv[rows, at[0]] = (pick(dq) * scale).astype(BF)
            r.dqkv[rows, at[1]] = (pick(dk) * scale).astype(BF)
            r.dqkv[rows, at[2]] = pick(dv).astype(BF)

    loop(T // 2, attend_back)
    su.along_z(su.order()[0])
    loop(T - T // 2, attend_back, T // 2)
    sd.along_z(sd.order()[-1])
    sd.join(1)
    ty.middle()

    def project_back(j):
        value = nt(r.dqkv[...], r.wq[rows_of(j, width)].reshape(256, m.NQ))
        r.Pn[:, rows_of(j, 256)] = value.astype(BF)

    loop(D // 256, project_back)
    tin.start()
    for step in range(1, T):
        arrive(r.daq.at[rows_of(down_n(step), S)], ai[step - 1])
    for step in so.order():
        so.multiply(step, r.ot, r.daq)
        so.along_x(step)
    tin.middle()
    su.along_z(1)
    for step in sq.order():
        sq.multiply(step, r.at, r.dqkv)
    for step in su.order()[2:-1]:
        su.along_z(step)
    su.join(0)

    r.vg[0] = jnp.zeros((16, D), F32)
    for k, row in enumerate((4, 5, 6, 7)):
        r.vg[0, row : row + 1, :] = jnp.sum(r.sums[k], axis=0, keepdims=True)
    r.vg[0, pl.ds(8 + n, 1), 0 : m.F] = r.sums[5, 0:1, 0 : m.F]

    def column(j):
        cols = rows_of(j, 128)
        there = pl.ds(pl.multiple_of(n * m.Q + j * 128, 128), 128)
        tail = pl.ds(pl.multiple_of(2 * m.Q + j * 128, 128), 128)
        r.vg[0, 2:3, there] = jnp.sum(r.dqkv[:, cols].astype(F32), axis=0, keepdims=True)
        r.vg[0, 3:4, there] = jnp.sum(r.dqkv[:, tail].astype(F32), axis=0, keepdims=True)

    loop(m.Q // 128, column)
    tin.finish()
    r.sums[0:2] = jnp.zeros((2, 16, D), F32)

    def first_back(i):
        rows = rows_of(i, 16)
        grad = tin.rows(rows)
        unit, inverse = normalize(r.x[rows, :].astype(F32))
        r.ig[rows, :] = r.dr[rows, :] + norm_back(grad, unit, inverse, r.vec[0:1, :])
        r.sums[0] += grad * unit
        r.sums[1] += grad

    loop(S // 16, first_back)
    r.vg[0, 0:1, :] = jnp.sum(r.sums[0], axis=0, keepdims=True)
    r.vg[0, 1:2, :] = jnp.sum(r.sums[1], axis=0, keepdims=True)
    vxi, vzi, vti = fresh(X - 1), fresh(Z - 1), fresh(T - 1)
    for dx in range(1, X):
        send(r.vg.at[0], r.vx.at[dx - 1], (z * X + up_x(dx), n), vxi[dx - 1])

    for step in sq.order():
        sq.along_x(step)
    su.join(1)
    su.along_z(su.order()[-1])
    ty.finish()

    def close(i):
        rows = rows_of(i, 16)
        r.bo[rows, :] = (r.r1[rows, :] + ty.rows(rows) + r.vec[7:8, :]).astype(BF)

    loop(S // 16, close)
    for step in so.order():
        so.along_z(step)
    so.join(0)
    so.join(1)
    total = r.vg[0]
    for dx in range(1, X):
        arrive(r.vx.at[dx - 1], vxi[dx - 1])
        total = total + r.vx[dx - 1]
    r.vg[1] = total
    for step in range(1, Z):
        send(r.vg.at[1], r.vz.at[step - 1], (up_z(step) * X + x, n), vzi[step - 1])
    sd.finish()

    def keep(i):
        rows = rows_of(i, 16)
        r.gd[rows, :] = sd.total(rows)

    loop(m.FD // 16, keep)
    du, do, dq = Deal("u", su, r.gu), Deal("o", so, r.go), Deal("q", sq, r.gq)
    for step in sq.order()[:2]:
        sq.along_z(step)
    sq.join(0)
    for step in sq.order()[2:-1]:
        sq.along_z(step)
    sq.join(1)
    du.start()
    sq.along_z(Z - 1)
    do.start()
    dq.start()
    total = r.vg[1]
    for step in range(1, Z):
        arrive(r.vz.at[step - 1], vzi[step - 1])
        total = total + r.vz[step - 1]
    r.vg[2] = total
    for step in range(1, T):
        send(r.vg.at[2], r.vt.at[step - 1], (w, up_n(step)), vti[step - 1])
    du.finish()
    do.finish()
    dq.finish()
    total = r.vg[2]
    for step in range(1, T):
        arrive(r.vt.at[step - 1], vti[step - 1])
        total = total + r.vt[step - 1]
    r.gv[...] = total
    for one, only in sent:
        if only is None:
            one.wait_send()
        else:
            pl.when(only)(one.wait_send)


def block_step(m, args):
    scratch = scratch_of(m)
    kept = {"q": m.NQ, "o": m.Q, "u": m.F}
    grads = [
        jax.ShapeDtypeStruct((m.T, m.RD, cols) if m.inside else (m.RG, cols), BF)
        for cols in kept.values()
    ]
    vmem = pl.BlockSpec(memory_space=pltpu.VMEM)

    def kernel(*refs):
        block_kernel(m, list(scratch), *refs)

    return pl.pallas_call(
        kernel,
        out_shape=[
            jax.ShapeDtypeStruct((m.S, D), BF),
            jax.ShapeDtypeStruct((m.S, D), F32),
            *grads,
            jax.ShapeDtypeStruct((m.FD, D), F32),
            jax.ShapeDtypeStruct((16, D), F32),
        ],
        in_specs=[vmem] * len(args),
        out_specs=[vmem] * 7,
        scratch_shapes=[pltpu.VMEM(shape, kind) for shape, kind in scratch.values()]
        + [pltpu.SemaphoreType.DMA((semaphores_of(m),))],
        compiler_params=pltpu.CompilerParams(
            collective_id=0, has_side_effects=True, vmem_limit_bytes=62 * 1024 * 1024
        ),
        name="block_step",
    )(*args)


def update_kernel(pieces, passed, *refs):
    count = len(pieces)
    ins, outs = refs[: 3 * count + passed], refs[3 * count + passed :]
    for k, parts in enumerate(pieces):
        grad, master, moments = ins[3 * k : 3 * k + 3]
        new, state, low = outs[3 * k : 3 * k + 3]
        rows = min(16, master.shape[0])

        def one(i, parts=parts, grad=grad, master=master, moments=moments, new=new, state=state, low=low, rows=rows):
            own = pl.ds(pl.multiple_of(i * rows, rows), rows)
            for block, source, column, width in parts:
                cols = pl.ds(column, width)
                value = grad[block, own, pl.ds(source, width)].astype(F32)
                first = MOMENT_DECAY * moments[0, own, cols] + (1.0 - MOMENT_DECAY) * value
                second = MOMENT_DECAY * moments[1, own, cols] + (1.0 - MOMENT_DECAY) * value * value
                correction = 1.0 - MOMENT_DECAY**STEP
                scaled = first / correction / (jnp.sqrt(second / correction) + ADAM_EPSILON)
                old = master[own, cols]
                updated = old - RATE_MATRIX * (scaled + WEIGHT_DECAY * old)
                new[own, cols] = updated
                state[0, own, cols] = first
                state[1, own, cols] = second
                low[own, cols] = updated.astype(BF)

        loop(master.shape[0] // rows, one)
    for source, target in zip(ins[3 * count :], outs[3 * count :]):
        target[...] = source[...]


def update_step(m, grads, masters, moments, passed):
    pieces = [
        [(t, b * m.Q, b * D + t * m.Q, m.Q) for b in range(3) for t in range(m.T)],
        [(t, 0, t * m.Q, m.Q) for t in range(m.T)],
        [(t, k * m.FD, (k * m.T + t) * m.FD, m.FD) for t in range(m.T) for k in range(m.W)],
        [(0, k * 256, k * 256, 256) for k in range(D // 256)],
    ]
    if m.FD % 128:
        pieces[2] = [(0, k * 256, k * 256, 256) for k in range(FF // 256)]
    steps = 2 if m.RD % 32 == 0 else 1
    args, specs, outs, out_specs = [], [], [], []

    def spec(shape):
        axis = len(shape) - 2
        block = tuple(s // steps if k == axis else s for k, s in enumerate(shape))
        return pl.BlockSpec(block, lambda i: tuple(i if k == axis else 0 for k in range(axis + 2)))

    for grad, master, moment in zip(grads, masters, moments):
        args += [grad, master, moment]
        specs += [spec(a.shape) for a in (grad, master, moment)]
        for shape, kind in ((master.shape, F32), (moment.shape, F32), (master.shape, BF)):
            outs.append(jax.ShapeDtypeStruct(shape, kind))
            out_specs.append(spec(shape))
    for one in passed:
        args.append(one)
        specs.append(spec(one.shape))
        outs.append(jax.ShapeDtypeStruct(one.shape, one.dtype))
        out_specs.append(spec(one.shape))

    def kernel(*refs):
        update_kernel(pieces, len(passed), *refs)

    return pl.pallas_call(
        kernel,
        grid=(steps,),
        out_shape=outs,
        in_specs=specs,
        out_specs=out_specs,
        name="update_step",
    )(*args)


def body(
    tokens,
    cotangent,
    segment_ids,
    w_qkv,
    w_out,
    w_up,
    w_down,
    vectors,
    moments_qkv,
    moments_out,
    moments_up,
    moments_down,
    moments_vec,
):
    wide, narrow = lax.axis_size("wide"), lax.axis_size("narrow")
    m = layout(wide, narrow, tokens.shape[0])
    device = lax.axis_index("wide") * narrow + lax.axis_index("narrow")
    first_row = device * m.RD

    pq = w_qkv.astype(BF).reshape(m.RD, 3, m.T, m.Q).transpose(2, 0, 1, 3)
    po = w_out.astype(BF).reshape(m.RD, m.T, m.Q).transpose(1, 0, 2)
    pu = w_up.astype(BF).reshape(m.RD, m.W, m.T, m.FD).transpose(2, 0, 1, 3)
    parts = [pq.reshape(m.T, m.RD, m.NQ), po, pu.reshape(m.T, m.RD, m.F)]
    if not m.inside:
        parts = [
            lax.all_to_all(part, "narrow", 0, 0).reshape(m.RG, part.shape[2]) for part in parts
        ]
    low = vectors.astype(BF).T
    spot = jnp.zeros((12, D), BF)
    spot = lax.dynamic_update_slice(spot, low, (0, first_row))
    rise = spot[8:].reshape(m.W, m.T, m.FD).transpose(1, 0, 2).reshape(m.T, m.F)
    rise = jnp.pad(rise, ((0, 8 - m.T), (0, D - m.F)))
    packed = jnp.concatenate([spot[:8], rise], axis=0)
    segments = jnp.broadcast_to(segment_ids.astype(F32), (8, m.S))

    block_out, input_grad, gq, go, gu, gd, gv = block_step(
        m, (tokens, cotangent, segments, *parts, w_down.astype(BF), packed)
    )
    if not m.inside:
        gq, go, gu = [
            lax.all_to_all(g.reshape(m.T, m.RD, g.shape[1]), "narrow", 0, 0) for g in (gq, go, gu)
        ]
    if m.FD % 128:
        gu = gu.reshape(m.T, m.RD, m.W, m.FD).transpose(1, 2, 0, 3).reshape(1, m.RD, FF)
    rise = gv[8 : 8 + m.T, : m.F].reshape(m.T, m.W, m.FD).transpose(1, 0, 2).reshape(FF // D, D)
    grad_vec = lax.dynamic_slice(
        jnp.concatenate([gv[:8], rise], axis=0), (0, first_row), (12, m.RD)
    ).T

    results = update_step(
        m,
        (gq, go, gu, gd.reshape(1, m.FD, D)),
        (w_qkv, w_out, w_up, w_down),
        (moments_qkv, moments_out, moments_up, moments_down),
        (block_out, input_grad),
    )
    new_qkv, state_qkv, copy_qkv, new_out, state_out, copy_out = results[:6]
    new_up, state_up, copy_up, new_down, state_down, copy_down = results[6:12]
    block_out, input_grad = results[12:]
    new_vectors, state_vectors, copy_vectors = adam_update(
        vectors, moments_vec, grad_vec, RATE_VECTOR, 0.0
    )
    return (
        block_out,
        input_grad,
        new_qkv,
        new_out,
        new_up,
        new_down,
        new_vectors,
        state_qkv,
        state_out,
        state_up,
        state_down,
        state_vectors,
        copy_qkv,
        copy_out,
        copy_up,
        copy_down,
        copy_vectors,
    )


def solution(mesh):
    flat = P(("wide", "narrow"), None)
    pair = P(None, ("wide", "narrow"), None)
    return jax.shard_map(
        body,
        mesh=mesh,
        in_specs=(flat,) * 8 + (pair,) * 5,
        out_specs=(flat,) * 7 + (pair,) * 5 + (flat,) * 5,
        check_vma=False,
    )
```

```python
import types

import jax
import jax.numpy as jnp
from jax import lax
from jax.experimental import pallas as pl
from jax.experimental.pallas import tpu as pltpu
from jax.sharding import PartitionSpec as P

D = 1024
HEADS = 16
FF = 4096
STEP = 3
HEAD = D // HEADS

NORM_EPSILON = 1e-06
MASK_VALUE = -1e30
MOMENT_DECAY = 0.5
RATE_MATRIX = 0.04
RATE_VECTOR = 0.2
WEIGHT_DECAY = 0.1
ADAM_EPSILON = 1e-08

BF = jnp.bfloat16
F32 = jnp.float32
MESH = pl.DeviceIdType.MESH


def adam_update(master, moments, gradient, rate, decay):
    first_moment = MOMENT_DECAY * moments[0] + (1.0 - MOMENT_DECAY) * gradient
    second_moment = MOMENT_DECAY * moments[1] + (1.0 - MOMENT_DECAY) * gradient * gradient
    correction = 1.0 - MOMENT_DECAY**STEP
    normalized = first_moment / correction / (jnp.sqrt(second_moment / correction) + ADAM_EPSILON)
    updated = master - rate * (normalized + decay * master)
    return (updated, jnp.stack([first_moment, second_moment]), updated.astype(BF))


def nn(left, right):
    return jnp.dot(left, right, preferred_element_type=F32)


def nt(left, right):
    return lax.dot_general(left, right, (((1,), (1,)), ((), ())), preferred_element_type=F32)


def tn(left, right):
    return lax.dot_general(left, right, (((0,), (0,)), ((), ())), preferred_element_type=F32)


def loop(count, body, first=0):
    def step(index, carry):
        body(index)
        return carry

    lax.fori_loop(first, first + count, step, 0)


def normalize(rows):
    center = rows - jnp.mean(rows, axis=-1, keepdims=True)
    inverse = lax.rsqrt(jnp.mean(center * center, axis=-1, keepdims=True) + NORM_EPSILON)
    return center * inverse, inverse


def norm_back(grad, unit, inverse, gain):
    scaled = grad * gain
    first = jnp.mean(scaled, axis=-1, keepdims=True)
    second = jnp.mean(scaled * unit, axis=-1, keepdims=True)
    return inverse * (scaled - first - unit * second)


def layout(wide, narrow, length):
    m = types.SimpleNamespace()
    m.W, m.T, m.S = wide, narrow, length
    m.Y = narrow // 2
    m.X = narrow // 2
    m.Z = wide // m.X
    m.L = length * narrow
    m.Q = D // narrow
    m.NQ = 3 * m.Q
    m.F = FF // narrow
    m.RG = D // wide
    m.RD = D // (wide * narrow)
    m.FD = FF // (wide * narrow)
    m.NH = m.Q // HEAD
    m.inside = m.RD % 16 == 0
    m.line = m.Z == 4
    return m


def scratch_of(m):
    def weights(name, rows, cols):
        return {
            name: ((m.W, rows, cols), BF),
        }

    def scatter(name, rows, cols):
        return {
            "G" + name: ((m.W, rows, cols), BF),
            "X" + name: ((m.X - 1, m.Z, rows, cols), BF),
            "S" + name: ((m.Z, rows, cols), BF),
            "Z" + name: ((m.Z if m.line else m.Z - 1, rows, cols), BF),
        }

    def spread(name, cols):
        return {
            "T" + name: ((m.T, m.RD, cols), BF),
            "N" + name: ((m.T, m.RD, cols), BF),
        }

    def partial(name):
        return {
            "P" + name: ((m.L, D), BF),
            "C" + name: ((m.Y, m.S, D), BF),
            "M" + name: ((m.Y, m.S, D), BF),
            "A" + name: ((m.S, D), F32),
            "R" + name: ((m.Y - 1, m.S, D), BF),
        }

    out = {}
    out.update(weights("wq", m.RG, m.NQ))
    out["wo"] = ((m.T, m.W, m.RG, m.Q), BF)
    out.update(weights("wu", m.RG, m.F))
    out.update(weights("wd", m.FD, D))
    out.update(weights("wv", 16, D))
    out["vn"] = ((m.T - 1, 16, D), BF)
    out.update(scatter("q", m.RG, m.NQ))
    out.update(scatter("o", m.RG, m.Q))
    out.update(scatter("u", m.RG, m.F))
    out.update(scatter("d", m.FD, D))
    if m.inside:
        out["pq"] = ((m.T, m.RD, m.NQ), BF)
        out["po"] = ((m.T, m.RD, m.Q), BF)
        out["pu"] = ((m.T, m.RD, m.F), BF)
        out.update(spread("q", m.NQ))
        out.update(spread("o", m.Q))
        out.update(spread("u", m.F))
    for name in ("y", "c", "n"):
        out.update(partial(name))
    for name in ("tok", "dya", "ca"):
        out[name] = ((m.L, D), BF)
    out["oa"] = ((m.T, m.L, m.Q), BF)
    out["sg"] = ((m.T, 8, m.S), F32)
    out["vec"] = ((16, D), F32)
    out["bias"] = ((8, m.NQ), F32)
    out["a"] = ((m.L, D), BF)
    out["at"] = ((D, m.L), BF)
    out["ct"] = ((D, m.L), BF)
    out["ot"] = ((D, m.L), BF)
    out["h"] = ((m.L, m.F), BF)
    out["ht"] = ((m.F, m.L), BF)
    out["u"] = ((m.L, m.F), F32)
    out["du"] = ((m.L, m.F), BF)
    out["qkv"] = ((m.L, m.NQ), BF)
    out["dqkv"] = ((m.L, m.NQ), BF)
    out["prob"] = ((m.T * m.NH, m.S, m.S), F32)
    out["oo"] = ((m.S, D), BF)
    out["r1"] = ((m.S, D), F32)
    out["dr"] = ((m.S, D), F32)
    out["da"] = ((m.S, D), BF)
    out["dob"] = ((m.T, m.S, m.Q), BF)
    out["dab"] = ((m.T, m.S, m.Q), BF)
    out["dof"] = ((m.L, m.Q), BF)
    out["daq"] = ((m.L, m.Q), BF)
    out["sums"] = ((6, 16, D), F32)
    out["bo"] = ((m.S, D), BF)
    out["ig"] = ((m.S, D), F32)
    out["gq"] = ((m.T, m.RD, m.NQ) if m.inside else (m.RG, m.NQ), BF)
    out["go"] = ((m.T, m.RD, m.Q) if m.inside else (m.RG, m.Q), BF)
    out["gu"] = ((m.T, m.RD, m.F) if m.inside else (m.RG, m.F), BF)
    out["gd"] = ((m.FD, D), F32)
    out["gv"] = ((16, D), F32)
    out["vg"] = ((3, 16, D), F32)
    out["vb"] = ((3, 16, D), BF)
    out["vx"] = ((m.X - 1, 16, D), BF)
    out["vz"] = ((m.Z - 1, 16, D), BF)
    out["vt"] = ((m.T - 1, 16, D), BF)
    return out


def semaphores_of(m):
    gather = 2 * m.Z + m.Z * (m.X - 1)
    scatter = m.Z * (m.X - 1) + 2 * m.Z
    pair = (m.Y - 1) + m.Y
    direct = m.T - 1
    total = 5 * gather + 4 * scatter + 8 * pair + 10 * direct + (m.X - 1) + (m.Z - 1) + direct
    return 2 * total + 16


def block_kernel(m, names, *refs):
    inputs = ("x", "dy", "seg", "pq", "po", "pu", "pd", "pv")
    if m.inside:
        inputs = ("x", "dy", "seg", "fq", "fo", "fu", "fd", "pv")
    outputs = ("bo", "ig", "gq", "go", "gu", "gd", "gv")
    homes = tuple("h" + name for name in outputs)
    r = types.SimpleNamespace(**dict(zip(inputs + homes + tuple(names) + ("sem", "done"), refs)))

    def put(name):
        k = outputs.index(name)
        return pltpu.make_async_copy(getattr(r, name), getattr(r, "h" + name), r.done.at[k])

    w, n = lax.axis_index("wide"), lax.axis_index("narrow")
    z, x = w // m.X, lax.rem(w, m.X)
    y, c = n // 2, lax.rem(n, 2)
    sibling = (w, 2 * y + 1 - c)
    L, S, T, X, Y, Z = m.L, m.S, m.T, m.X, m.Y, m.Z
    sent = []
    used = [0]

    def fresh(count):
        first = used[0]
        used[0] += count
        return [first + k for k in range(count)]

    inner = (z == 1) | (z == 2)
    mate = jnp.where(z < 2, 1 - z, 5 - z)
    fin, fend = jnp.where(z < 2, 2, 1), jnp.where(z < 2, 3, 0)

    def copy(src, dst, device, index, out=None):
        return pltpu.make_async_remote_copy(
            src_ref=src,
            dst_ref=dst,
            send_sem=r.sem.at[2 * (index if out is None else out)],
            recv_sem=r.sem.at[2 * index + 1],
            device_id=device,
            device_id_type=MESH,
        )

    def send(src, dst, device, index, out=None, only=None):
        one = copy(src, dst, device, index, out)
        if only is None:
            one.start()
        else:
            pl.when(only)(one.start)
        sent.append((one, only))

    def drain(count):
        for one, only in sent[:count]:
            if only is None:
                one.wait_send()
            else:
                pl.when(only)(one.wait_send)
        del sent[:count]

    def arrive(dst, index):
        copy(dst, dst, sibling, index).wait_recv()

    def up_z(step):
        return lax.rem(z + step, Z)

    def down_z(step):
        return lax.rem(z + Z - step, Z)

    def up_x(step):
        return lax.rem(x + step, X)

    def down_x(step):
        return lax.rem(x + X - step, X)

    def up_n(step):
        return lax.rem(n + step, T)

    def down_n(step):
        return lax.rem(n + T - step, T)

    def at_y(step):
        return lax.rem(y + Y + step, Y)

    def rows_of(index, size):
        return pl.ds(pl.multiple_of(index * size, size), size)

    class Gather:
        def __init__(self, ref):
            self.ref = ref
            self.zi = fresh(Z - 1)[0]
            self.out = fresh(4)
            self.xi = fresh(Z * (X - 1))[0]

        def to_z(self, block, there, index, out, only=None):
            send(self.ref.at[block], self.ref.at[block], (there * X + x, n), self.zi + index, out, only)

        def along_z(self):
            if m.line:
                self.to_z(w, fin, jnp.where(inner, 1, 2), self.out[0])
                self.to_z(w, mate, 0, self.out[1])
                return
            for step in range(1, Z):
                self.to_z(w, up_z(step), step - 1, None)

        def forward(self, step, only=None):
            block = down_z(step) * X + x
            for dx in range(1, X):
                send(
                    self.ref.at[block],
                    self.ref.at[block],
                    (z * X + up_x(dx), n),
                    self.xi + step * (X - 1) + dx - 1,
                    only=only,
                )

        def relay(self, k, who):
            if not m.line and who == "end":
                return
            only = None
            if m.line:
                only = inner if who == "inner" else jnp.logical_not(inner)
            step, index = k, k - 1
            if m.line:
                index = jnp.where(inner, k % 3, k - 1)
                there = jnp.where(index == 0, mate, jnp.where(index == 1, fin, fend))
                step = lax.rem(z + Z - there, Z)
            block = down_z(step) * X + x
            if only is None:
                arrive(self.ref.at[block], self.zi + index)
            else:
                pl.when(only)(lambda: arrive(self.ref.at[block], self.zi + index))
            if m.line and k < 3 and who == "inner":
                self.to_z(block, mate, index, self.out[1 + k], inner)
            self.forward(step, only)

        def inside(self, steps):
            for k in steps:
                self.relay(k, "inner")

        def ends(self, steps):
            for k in steps:
                self.relay(k, "end")

        def finish(self):
            for step in range(Z):
                for dx in range(1, X):
                    block = (down_z(step) if step else z) * X + down_x(dx)
                    arrive(self.ref.at[block], self.xi + step * (X - 1) + dx - 1)

    class Share:
        def __init__(self, slot):
            self.slot = slot
            self.yi = fresh(Y - 1)
            self.ci = fresh(Y)

        def start(self):
            for step in range(1, Y):
                send(self.slot(n), self.slot(n), (w, 2 * at_y(step) + c), self.yi[step - 1])
            send(self.slot(n), self.slot(n), sibling, self.ci[0])

        def middle(self):
            for step in range(1, Y):
                block = 2 * at_y(-step) + c
                arrive(self.slot(block), self.yi[step - 1])
                send(self.slot(block), self.slot(block), sibling, self.ci[step])

        def close(self):
            for step in range(Y):
                block = 2 * at_y(-step) + 1 - c
                arrive(self.slot(block), self.ci[step])

    class Total:
        def __init__(self, name):
            self.part = getattr(r, "P" + name)
            self.core = getattr(r, "C" + name)
            self.mid = getattr(r, "M" + name)
            self.own = getattr(r, "A" + name)
            self.last = getattr(r, "R" + name)
            self.yi = fresh(Y - 1)
            self.ci = fresh(Y)

        def start(self):
            for step in list(range(1, Y)) + [0]:
                block = 2 * at_y(step) + 1 - c
                send(self.part.at[rows_of(block, S)], self.core.at[step], sibling, self.ci[step])

        def middle(self):
            for step in list(range(1, Y)) + [0]:
                block = 2 * at_y(step) + c
                arrive(self.core.at[step], self.ci[step])

                def add(i):
                    rows = rows_of(i, 16)
                    mine = self.part[pl.ds(pl.multiple_of(block * S + i * 16, 16), 16), :]
                    total = mine.astype(F32) + self.core[step, rows, :].astype(F32)
                    if step:
                        self.mid[step, rows, :] = total.astype(BF)
                    else:
                        self.own[rows, :] = total

                loop(S // 16, add)
                if step:
                    send(self.mid.at[step], self.last.at[step - 1], (w, block), self.yi[step - 1])

        def finish(self):
            for step in range(1, Y):
                arrive(self.last.at[step - 1], self.yi[step - 1])

        def rows(self, rows):
            total = self.own[rows, :]
            for step in range(1, Y):
                total = total + self.last[step - 1, rows, :].astype(F32)
            return total

    class Scatter:
        def __init__(self, name, rows, cols):
            self.rows, self.cols = rows, cols
            self.grad = getattr(r, "G" + name)
            self.fromx = getattr(r, "X" + name)
            self.sums = getattr(r, "S" + name)
            self.fromz = getattr(r, "Z" + name)
            self.xi = fresh(Z * (X - 1))
            self.zi = fresh(Z)[0]
            self.out = fresh(Z - 1)
            self.chunk = 16 if cols > 512 else 32
            if rows % self.chunk:
                self.chunk = 16

        def order(self):
            return list(range(Z))

        def there(self, k):
            if k == Z - 1:
                return z
            return (fin, fend, mate)[k] if m.line else up_z(k + 1)

        def multiply(self, k, left, right):
            first = self.there(k)
            high = X * self.rows
            tile = 256 if self.cols % 256 == 0 else 128

            def one(j):
                cols = rows_of(j, tile)
                value = nn(left[rows_of(first, high), :], right[:, cols]).astype(BF)
                value = value.reshape(X, self.rows, tile)
                self.grad[rows_of(first, X), :, cols] = value

            loop(self.cols // tile, one)

        def along_x(self, k):
            first = self.there(k)
            for dx in range(1, X):
                other = up_x(dx)
                send(
                    self.grad.at[first * X + other],
                    self.fromx.at[dx - 1, k],
                    (z * X + other, n),
                    self.xi[k * (X - 1) + dx - 1],
                )

        def along_z(self, k):
            block = self.there(k) * X + x
            for dx in range(1, X):
                arrive(self.fromx.at[dx - 1, k], self.xi[k * (X - 1) + dx - 1])

            def add(i):
                rows = rows_of(i, self.chunk)
                total = self.grad[block, rows, :].astype(F32)
                for dx in range(1, X):
                    total = total + self.fromx[dx - 1, k, rows, :].astype(F32)
                self.sums[k, rows, :] = total.astype(BF)

            loop(self.rows // self.chunk, add)
            if k == Z - 1:
                return
            if not m.line:
                self.to_z(k, block, k)
            elif k == 2:
                self.to_z(k, mate * X + x, 2)
            else:
                self.to_z(k, mate * X + x, k, z != jnp.where(z < 2, 1, 2))

        def to_z(self, k, block, slot, only=None):
            send(self.sums.at[k], self.fromz.at[slot], (block, n), self.zi + slot, self.out[k], only)

        def join(self, k):
            if not m.line:
                return

            @pl.when(inner)
            def _():
                arrive(self.fromz.at[k], self.zi + k)

                def add(i):
                    rows = rows_of(i, self.chunk)
                    total = self.sums[k, rows, :].astype(F32) + self.fromz[k, rows, :].astype(F32)
                    self.sums[k, rows, :] = total.astype(BF)

                loop(self.rows // self.chunk, add)
                copy(
                    self.sums.at[k], self.fromz.at[3], (self.there(k) * X + x, n), self.zi + 3, self.out[k]
                ).start()

            sent.append(
                (
                    copy(
                        self.sums.at[k], self.fromz.at[3], (self.there(k) * X + x, n), self.zi + 3, self.out[k]
                    ),
                    inner,
                )
            )

        def last(self):
            return [2, 3] if m.line else list(range(Z - 1))

        def finish(self):
            for slot in self.last():
                arrive(self.fromz.at[slot], self.zi + slot)

        def total(self, rows):
            total = self.sums[Z - 1, rows, :].astype(F32)
            for slot in self.last():
                total = total + self.fromz[slot, rows, :].astype(F32)
            return total

    class Deal:
        def __init__(self, name, scatter, out):
            self.scatter, self.out = scatter, out
            if m.inside:
                self.turn = getattr(r, "T" + name)
                self.got = getattr(r, "N" + name)
                self.ni = fresh(T - 1)

        def start(self):
            self.scatter.finish()
            if not m.inside:
                def store(i):
                    rows = rows_of(i, self.scatter.chunk)
                    self.out[rows, :] = self.scatter.total(rows).astype(BF)

                loop(self.scatter.rows // self.scatter.chunk, store)
                return

            def add(i):
                self.turn[i] = self.scatter.total(rows_of(i, m.RD)).astype(BF)

            loop(T, add)
            for step in range(1, T):
                other = up_n(step)
                send(self.turn.at[other], self.got.at[step], (w, other), self.ni[step - 1])

        def finish(self):
            if not m.inside:
                return
            self.out[n] = self.turn[n]
            for step in range(1, T):
                arrive(self.got.at[step], self.ni[step - 1])
                self.out[down_n(step)] = self.got[step]

    def transpose(target, source, count_rows, count_cols):
        def tile(k):
            i, j = k // count_cols, lax.rem(k, count_cols)
            target[rows_of(j, 128), rows_of(i, 128)] = source(rows_of(i, 128), rows_of(j, 128)).T

        loop(count_rows * count_cols, tile)

    if m.inside:
        for k in range(T):
            r.po[k] = r.fo[:, k * m.Q : (k + 1) * m.Q].astype(BF)
            for b in range(3):
                first = b * D + k * m.Q
                r.pq[k, :, b * m.Q : (b + 1) * m.Q] = r.fq[:, first : first + m.Q].astype(BF)
            for j in range(m.W):
                first = (j * T + k) * m.FD
                r.pu[k, :, j * m.FD : (j + 1) * m.FD] = r.fu[:, first : first + m.FD].astype(BF)

    barrier = pltpu.get_barrier_semaphore()
    peers = [(w, up_n(k)) for k in range(1, T)]
    peers += [(up_z(k) * X + x, n) for k in range(1, Z)]
    peers += [(z * X + up_x(k), n) for k in range(1, X)]
    for peer in peers:
        pl.semaphore_signal(barrier, inc=1, device_id=peer, device_id_type=MESH)
    pl.semaphore_wait(barrier, len(peers))

    gv, gq, gu, gd = Gather(r.wv), Gather(r.wq), Gather(r.wu), Gather(r.wd)
    go = Gather(r.wo.at[n])
    tokens = Share(lambda k: r.tok.at[rows_of(k, S)])
    cotangents = Share(lambda k: r.dya.at[rows_of(k, S)])
    outs = Share(lambda k: r.wo.at[k])
    mixes = Share(lambda k: r.oa.at[k])
    seconds = Share(lambda k: r.ca.at[rows_of(k, S)])
    ty, tc, tin = Total("y"), Total("c"), Total("n")
    sd, su = Scatter("d", m.FD, D), Scatter("u", m.RG, m.F)
    so, sq = Scatter("o", m.RG, m.Q), Scatter("q", m.RG, m.NQ)

    vi, si = fresh(T - 1), fresh(T - 1)
    for step in range(1, T):
        send(r.pv, r.vn.at[step - 1], (w, up_n(step)), vi[step - 1])
    r.wd[w] = r.fd[...].astype(BF) if m.inside else r.pd[...]
    gd.forward(0)

    class Rows:
        def __init__(self, part, target):
            self.part, self.target = part, target
            self.ids = fresh(T - 1) if m.inside else []

        def at(self, k, rows):
            return r.wo.at[k, w, rows] if self.target is None else self.target.at[w, rows]

        def start(self):
            if m.inside:
                own = pl.ds(pl.multiple_of(n * m.RD, m.RD), m.RD)
                for step in range(1, T):
                    other = up_n(step)
                    send(self.part.at[other], self.at(other, own), (w, other), self.ids[step - 1])
                self.at(n, own)[...] = self.part[n]
            elif self.target is None:
                r.wo[n, w] = self.part[...]
            else:
                self.target[w] = self.part[...]

        def finish(self):
            if m.inside:
                for step in range(1, T):
                    got = pl.ds(pl.multiple_of(down_n(step) * m.RD, m.RD), m.RD)
                    arrive(self.at(n, got), self.ids[step - 1])

    ro, rq, ru = Rows(r.po, None), Rows(r.pq, r.wq), Rows(r.pu, r.wu)
    ro.start()
    rq.start()
    own_rows = rows_of(n, S)
    r.tok[own_rows, :] = r.x[...]
    tokens.start()
    r.sg[n] = jnp.broadcast_to(r.seg[...].astype(F32), (8, S))
    for step in range(1, T):
        send(r.sg.at[n], r.sg.at[n], (w, up_n(step)), si[step - 1])
    ru.start()
    r.dya[own_rows, :] = r.dy[...]
    cotangents.start()

    vector = r.pv[...].astype(F32)
    for step in range(1, T):
        arrive(r.vn.at[step - 1], vi[step - 1])
        vector = vector + r.vn[step - 1].astype(F32)
    r.wv[w] = vector.astype(BF)
    early, late = range(1, Z - 1), range(Z - 1, Z)
    gv.along_z()
    gv.forward(0)
    ro.finish()
    go.along_z()
    go.forward(0)
    gv.inside(early)
    rq.finish()
    gq.along_z()
    gq.forward(0)
    go.inside(early)
    tokens.middle()
    ru.finish()
    gv.inside(late)
    gv.ends(range(1, Z))
    tokens.close()
    gv.finish()
    vector = r.wv[0].astype(F32)
    for k in range(1, m.W):
        vector = vector + r.wv[k].astype(F32)
    r.vec[...] = vector

    heads = rows_of(n, m.Q)
    r.bias[...] = jnp.zeros_like(r.bias)
    r.bias[0:1, 0 : m.Q] = r.vec[2:3, heads]
    r.bias[0:1, 2 * m.Q : 3 * m.Q] = r.vec[3:4, heads]

    def first_norm(i):
        rows = rows_of(i, 16)
        unit, _ = normalize(r.tok[rows, :].astype(F32))
        r.a[rows, :] = (unit * r.vec[0:1, :] + r.vec[1:2, :]).astype(BF)

    half = L // 32
    gq.inside(early)
    gu.along_z()
    go.inside(late)
    go.ends(range(1, Z))
    loop(half, first_norm)
    cotangents.middle()
    gq.inside(late)
    gq.ends(range(1, 2))
    go.finish()
    outs.start()
    loop(half, first_norm, half)
    gq.ends(range(2, Z - 1))
    transpose(r.at, lambda i, j: r.a[i, j], L // 128, D // 128)
    gq.ends(late)
    gu.forward(0)
    cotangents.close()
    gq.finish()

    tile_q = 256 if m.NQ % 256 == 0 else 128

    def project(j):
        cols = rows_of(j, tile_q)
        value = nn(r.a[...], r.wq[:, :, cols].reshape(D, tile_q)) + r.bias[0:1, cols]
        r.qkv[:, cols] = value.astype(BF)

    loop(m.NQ // tile_q, project)
    for step in range(1, T):
        arrive(r.sg.at[down_n(step)], si[step - 1])
    gu.inside(early)
    gd.along_z()
    gu.ends(range(1, 2))
    outs.middle()

    lane = lax.broadcasted_iota(jnp.int32, (1, 128), 1)
    halves = [(lane // HEAD == k).astype(F32) for k in range(128 // HEAD)]
    scale = HEAD ** (-0.5)
    per = 128 // HEAD

    def pick(values):
        total = values[0] * halves[0]
        for k in range(1, per):
            total = total + values[k] * halves[k]
        return total

    def attend(s):
        rows = rows_of(s, S)
        keys = jnp.broadcast_to(r.sg[s, 0:1, :], (S, S))
        same = keys == keys.T
        for pair in range(m.Q // 128):
            q = r.qkv[rows, pair * 128 : pair * 128 + 128]
            k = r.qkv[rows, m.Q + pair * 128 : m.Q + pair * 128 + 128]
            v = r.qkv[rows, 2 * m.Q + pair * 128 : 2 * m.Q + pair * 128 + 128]
            mixed = []
            for half in range(per):
                score = nt(q * halves[half].astype(BF), k) * scale
                score = jnp.where(same, score, MASK_VALUE)
                power = jnp.exp(score - jnp.max(score, axis=-1, keepdims=True))
                weight = power / jnp.sum(power, axis=-1, keepdims=True)
                r.prob[s * m.NH + pair * per + half] = weight
                mixed.append(nn(weight.astype(BF), v))
            r.oa[n, rows, pair * 128 : pair * 128 + 128] = pick(mixed).astype(BF)

    loop(T, attend)
    mixes.start()
    gu.inside(late)
    gu.ends(range(2, Z - 1))
    outs.close()
    mixes.middle()
    gu.ends(late)
    mixes.close()

    for t in range(T):
        r.oo[:, t * m.Q : (t + 1) * m.Q] = r.oa[t, own_rows, :]
    for t in range(T):
        cols = slice(t * m.Q, (t + 1) * m.Q)
        value = nn(r.oo[...], r.wo[t].reshape(D, m.Q))
        r.r1[:, cols] = r.x[:, cols].astype(F32) + value + r.vec[4:5, cols]

    def second_norm(i):
        rows = rows_of(i, 16)
        unit, _ = normalize(r.r1[rows, :])
        there = pl.ds(pl.multiple_of(n * S + i * 16, 16), 16)
        r.ca[there, :] = (unit * r.vec[5:6, :] + r.vec[6:7, :]).astype(BF)

    loop(S // 16, second_norm)
    seconds.start()
    gd.inside(early)
    gd.ends(range(1, 2))
    for t in range(T):
        for k in range(m.Q // 128):
            base = t * m.Q + k * 128

            def turn(i, t=t, k=k, base=base):
                value = r.oa[t, rows_of(i, 128), k * 128 : k * 128 + 128].astype(F32)
                r.ot[base : base + 128, rows_of(i, 128)] = value.T.astype(BF)

            loop(L // 128, turn)
    seconds.middle()
    seconds.close()
    gd.inside(late)
    gd.ends(range(2, Z - 1))
    gd.ends(late)
    gu.finish()

    def expand(j):
        cols = rows_of(j, 256)
        value = nn(r.ca[...], r.wu[:, :, cols].reshape(D, 256))
        r.u[:, cols] = value + r.vec[pl.ds(8 + n, 1), cols]

    loop(m.F // 256, expand)

    def activate(i):
        rows = rows_of(i, 16)
        value = r.u[rows, :]
        phi = 0.5 * (1.0 + lax.erf(value * (0.5**0.5)))
        r.h[rows, :] = (value * phi).astype(BF)
        r.u[rows, :] = phi + value * (jnp.exp(-0.5 * value * value) * 0.3989422804014327)

    loop(L // 16, activate)
    transpose(r.ht, lambda i, j: r.h[i, j], L // 128, m.F // 128)
    sd.multiply(sd.order()[0], r.ht, r.dya)
    sd.along_x(sd.order()[0])
    for step in sd.order()[1:]:
        sd.multiply(step, r.ht, r.dya)
        sd.along_x(step)
    transpose(r.ct, lambda i, j: r.ca[i, j], L // 128, D // 128)
    sd.along_z(0)
    gd.finish()
    early_sends = len(sent)

    group = 256 // m.FD

    def expand_back(j):
        cols = rows_of(j, 256)
        value = nt(r.dya[...], r.wd[rows_of(j, group)].reshape(256, D)) * r.u[:, cols]
        low = value.astype(BF)
        r.du[:, cols] = low
        r.sums[5, 0:1, cols] = jnp.sum(low.astype(F32), axis=0, keepdims=True)

    loop(m.F // 256, expand_back)
    width = 256 // m.RG

    def up_back(j):
        value = nt(r.du[...], r.wu[rows_of(j, width)].reshape(256, m.F))
        r.Pc[:, rows_of(j, 256)] = value.astype(BF)

    loop(D // 256, up_back)
    tc.start()
    for step in su.order():
        su.multiply(step, r.ct, r.du)
        su.along_x(step)
    tc.middle()

    def contract(j):
        cols = rows_of(j, 256)
        r.Py[:, cols] = nn(r.h[...], r.wd[:, :, cols].reshape(m.F, 256)).astype(BF)

    loop(D // 256, contract)
    ty.start()
    sd.along_z(1)
    tc.finish()
    r.sums[0:4] = jnp.zeros((4, 16, D), F32)

    def second_back(i):
        rows = rows_of(i, 16)
        grad = tc.rows(rows)
        cot = r.dy[rows, :].astype(F32)
        unit, inverse = normalize(r.r1[rows, :])
        total = cot + norm_back(grad, unit, inverse, r.vec[5:6, :])
        r.dr[rows, :] = total
        r.da[rows, :] = total.astype(BF)
        r.sums[0] += total
        r.sums[1] += grad * unit
        r.sums[2] += grad
        r.sums[3] += cot

    loop(S // 16, second_back)
    oi, ai = fresh(T - 1), fresh(T - 1)
    share = m.Q // m.RG
    for step in list(range(1, T)) + [0]:
        other = up_n(step) if step else n
        value = jnp.zeros((S, m.Q), F32)
        for t in range(T):
            block = r.wo[t, rows_of(other, share)].reshape(m.Q, m.Q)
            value = value + nt(r.da[:, t * m.Q : (t + 1) * m.Q], block)
        if step:
            r.dob[step] = value.astype(BF)
            send(r.dob.at[step], r.dof.at[own_rows], (w, other), oi[step - 1])
        else:
            r.dof[own_rows, :] = value.astype(BF)
    for step in range(1, T):
        other = up_n(step)
        r.dab[step] = r.da[:, rows_of(other, m.Q)]
        send(r.dab.at[step], r.daq.at[own_rows], (w, other), ai[step - 1])
    r.daq[own_rows, :] = r.da[:, rows_of(n, m.Q)]
    for step in sd.order()[2:-1]:
        sd.along_z(step)
    sd.join(0)
    for step in range(1, T):
        arrive(r.dof.at[rows_of(down_n(step), S)], oi[step - 1])

    def attend_back(s):
        rows = rows_of(s, S)
        for pair in range(m.Q // 128):
            at = [pl.ds(b * m.Q + pair * 128, 128) for b in range(3)]
            q, k, v = r.qkv[rows, at[0]], r.qkv[rows, at[1]], r.qkv[rows, at[2]]
            cot = r.dof[rows, pair * 128 : pair * 128 + 128]
            dq, dk, dv = [], [], []
            for half in range(per):
                weight = r.prob[s * m.NH + pair * per + half]
                grad = nt(cot * halves[half].astype(BF), v)
                inner = jnp.sum(weight * grad, axis=-1, keepdims=True)
                ds = (weight * (grad - inner)).astype(BF)
                dq.append(nn(ds, k))
                dk.append(tn(ds, q))
                dv.append(tn(weight.astype(BF), cot))
            r.dqkv[rows, at[0]] = (pick(dq) * scale).astype(BF)
            r.dqkv[rows, at[1]] = (pick(dk) * scale).astype(BF)
            r.dqkv[rows, at[2]] = pick(dv).astype(BF)

    loop(T // 2, attend_back)
    su.along_z(su.order()[0])
    loop(T - T // 2, attend_back, T // 2)
    sd.along_z(sd.order()[-1])
    sd.join(1)
    ty.middle()

    def project_back(j):
        value = nt(r.dqkv[...], r.wq[rows_of(j, width)].reshape(256, m.NQ))
        r.Pn[:, rows_of(j, 256)] = value.astype(BF)

    loop(D // 256, project_back)
    tin.start()
    for step in range(1, T):
        arrive(r.daq.at[rows_of(down_n(step), S)], ai[step - 1])
    tin.middle()
    su.along_z(1)
    for step in sq.order():
        sq.multiply(step, r.at, r.dqkv)
        sq.along_x(step)
    for step in su.order()[2:-1]:
        su.along_z(step)
    su.join(0)

    r.vg[0] = jnp.zeros((16, D), F32)
    for k, row in enumerate((4, 5, 6, 7)):
        r.vg[0, row : row + 1, :] = jnp.sum(r.sums[k], axis=0, keepdims=True)
    r.vg[0, pl.ds(8 + n, 1), 0 : m.F] = r.sums[5, 0:1, 0 : m.F]

    def column(j):
        cols = rows_of(j, 128)
        there = pl.ds(pl.multiple_of(n * m.Q + j * 128, 128), 128)
        tail = pl.ds(pl.multiple_of(2 * m.Q + j * 128, 128), 128)
        r.vg[0, 2:3, there] = jnp.sum(r.dqkv[:, cols].astype(F32), axis=0, keepdims=True)
        r.vg[0, 3:4, there] = jnp.sum(r.dqkv[:, tail].astype(F32), axis=0, keepdims=True)

    loop(m.Q // 128, column)
    tin.finish()
    r.sums[0:2] = jnp.zeros((2, 16, D), F32)

    def first_back(i):
        rows = rows_of(i, 16)
        grad = tin.rows(rows)
        unit, inverse = normalize(r.x[rows, :].astype(F32))
        r.ig[rows, :] = r.dr[rows, :] + norm_back(grad, unit, inverse, r.vec[0:1, :])
        r.sums[0] += grad * unit
        r.sums[1] += grad

    loop(S // 16, first_back)
    put("ig").start()
    r.vg[0, 0:1, :] = jnp.sum(r.sums[0], axis=0, keepdims=True)
    r.vg[0, 1:2, :] = jnp.sum(r.sums[1], axis=0, keepdims=True)
    r.vb[0] = r.vg[0].astype(BF)
    vxi, vzi, vti = fresh(X - 1), fresh(Z - 1), fresh(T - 1)
    for dx in range(1, X):
        send(r.vb.at[0], r.vx.at[dx - 1], (z * X + up_x(dx), n), vxi[dx - 1])

    for step in so.order():
        so.multiply(step, r.ot, r.daq)
        so.along_x(step)
    su.join(1)
    su.along_z(su.order()[-1])
    ty.finish()

    def close(i):
        rows = rows_of(i, 16)
        r.bo[rows, :] = (r.r1[rows, :] + ty.rows(rows) + r.vec[7:8, :]).astype(BF)

    loop(S // 16, close)
    put("bo").start()
    drain(early_sends)
    sd.finish()

    def keep(i):
        rows = rows_of(i, 16)
        r.gd[rows, :] = sd.total(rows)

    loop(m.FD // 16, keep)
    put("gd").start()
    du, do, dq = Deal("u", su, r.gu), Deal("o", so, r.go), Deal("q", sq, r.gq)
    for step in sq.order()[:2]:
        sq.along_z(step)
    sq.join(0)
    for step in sq.order()[2:-1]:
        sq.along_z(step)
    sq.join(1)
    du.start()
    sq.along_z(Z - 1)
    for step in so.order()[:-1]:
        so.along_z(step)
    so.join(0)
    so.join(1)
    so.along_z(Z - 1)
    total = r.vg[0]
    for dx in range(1, X):
        arrive(r.vx.at[dx - 1], vxi[dx - 1])
        total = total + r.vx[dx - 1].astype(F32)
    r.vg[1] = total
    r.vb[1] = total.astype(BF)
    for step in range(1, Z):
        send(r.vb.at[1], r.vz.at[step - 1], (up_z(step) * X + x, n), vzi[step - 1])
    dq.start()
    do.start()
    total = r.vg[1]
    for step in range(1, Z):
        arrive(r.vz.at[step - 1], vzi[step - 1])
        total = total + r.vz[step - 1].astype(F32)
    r.vg[2] = total
    r.vb[2] = total.astype(BF)
    for step in range(1, T):
        send(r.vb.at[2], r.vt.at[step - 1], (w, up_n(step)), vti[step - 1])
    du.finish()
    put("gu").start()
    dq.finish()
    put("gq").start()
    do.finish()
    put("go").start()
    total = r.vg[2]
    for step in range(1, T):
        arrive(r.vt.at[step - 1], vti[step - 1])
        total = total + r.vt[step - 1].astype(F32)
    r.gv[...] = total
    put("gv").start()
    drain(len(sent))
    for name in outputs:
        put(name).wait()


def block_step(m, args):
    scratch = scratch_of(m)
    kept = {"q": m.NQ, "o": m.Q, "u": m.F}
    grads = [
        jax.ShapeDtypeStruct((m.T, m.RD, cols) if m.inside else (m.RG, cols), BF)
        for cols in kept.values()
    ]
    vmem = pl.BlockSpec(memory_space=pltpu.VMEM)

    def kernel(*refs):
        block_kernel(m, list(scratch), *refs)

    return pl.pallas_call(
        kernel,
        out_shape=[
            jax.ShapeDtypeStruct((m.S, D), BF),
            jax.ShapeDtypeStruct((m.S, D), F32),
            *grads,
            jax.ShapeDtypeStruct((m.FD, D), F32),
            jax.ShapeDtypeStruct((16, D), F32),
        ],
        in_specs=[vmem] * len(args),
        out_specs=[pl.BlockSpec(memory_space=pl.ANY)] * 7,
        scratch_shapes=[pltpu.VMEM(shape, kind) for shape, kind in scratch.values()]
        + [pltpu.SemaphoreType.DMA((semaphores_of(m),)), pltpu.SemaphoreType.DMA((7,))],
        compiler_params=pltpu.CompilerParams(
            collective_id=0, has_side_effects=True, vmem_limit_bytes=62 * 1024 * 1024
        ),
        name="block_step",
    )(*args)


def update_kernel(pieces, passed, *refs):
    count = len(pieces)
    ins, outs = refs[: 3 * count + passed], refs[3 * count + passed :]
    for k, parts in enumerate(pieces):
        grad, master, moments = ins[3 * k : 3 * k + 3]
        new, state, low = outs[3 * k : 3 * k + 3]
        rows = min(16, master.shape[0])

        def one(i, parts=parts, grad=grad, master=master, moments=moments, new=new, state=state, low=low, rows=rows):
            own = pl.ds(pl.multiple_of(i * rows, rows), rows)
            for block, source, column, width in parts:
                cols = pl.ds(column, width)
                value = grad[block, own, pl.ds(source, width)].astype(F32)
                first = MOMENT_DECAY * moments[0, own, cols] + (1.0 - MOMENT_DECAY) * value
                second = MOMENT_DECAY * moments[1, own, cols] + (1.0 - MOMENT_DECAY) * value * value
                correction = 1.0 - MOMENT_DECAY**STEP
                scaled = first / correction / (jnp.sqrt(second / correction) + ADAM_EPSILON)
                old = master[own, cols]
                updated = old - RATE_MATRIX * (scaled + WEIGHT_DECAY * old)
                new[own, cols] = updated
                state[0, own, cols] = first
                state[1, own, cols] = second
                low[own, cols] = updated.astype(BF)

        loop(master.shape[0] // rows, one)
    for source, target in zip(ins[3 * count :], outs[3 * count :]):
        target[...] = source[...]


def update_step(m, grads, masters, moments, passed):
    pieces = [
        [(t, b * m.Q, b * D + t * m.Q, m.Q) for b in range(3) for t in range(m.T)],
        [(t, 0, t * m.Q, m.Q) for t in range(m.T)],
        [(t, k * m.FD, (k * m.T + t) * m.FD, m.FD) for t in range(m.T) for k in range(m.W)],
        [(0, k * 256, k * 256, 256) for k in range(D // 256)],
    ]
    if m.FD % 128:
        pieces[2] = [(0, k * 256, k * 256, 256) for k in range(FF // 256)]
    steps = 2 if m.RD % 32 == 0 else 1
    args, specs, outs, out_specs = [], [], [], []

    def spec(shape):
        axis = len(shape) - 2
        block = tuple(s // steps if k == axis else s for k, s in enumerate(shape))
        return pl.BlockSpec(block, lambda i: tuple(i if k == axis else 0 for k in range(axis + 2)))

    for grad, master, moment in zip(grads, masters, moments):
        args += [grad, master, moment]
        specs += [spec(a.shape) for a in (grad, master, moment)]
        for shape, kind in ((master.shape, F32), (moment.shape, F32), (master.shape, BF)):
            outs.append(jax.ShapeDtypeStruct(shape, kind))
            out_specs.append(spec(shape))
    for one in passed:
        args.append(one)
        specs.append(spec(one.shape))
        outs.append(jax.ShapeDtypeStruct(one.shape, one.dtype))
        out_specs.append(spec(one.shape))

    def kernel(*refs):
        update_kernel(pieces, len(passed), *refs)

    return pl.pallas_call(
        kernel,
        grid=(steps,),
        out_shape=outs,
        in_specs=specs,
        out_specs=out_specs,
        name="update_step",
    )(*args)


def body(
    tokens,
    cotangent,
    segment_ids,
    w_qkv,
    w_out,
    w_up,
    w_down,
    vectors,
    moments_qkv,
    moments_out,
    moments_up,
    moments_down,
    moments_vec,
):
    wide, narrow = lax.axis_size("wide"), lax.axis_size("narrow")
    m = layout(wide, narrow, tokens.shape[0])
    device = lax.axis_index("wide") * narrow + lax.axis_index("narrow")
    first_row = device * m.RD

    parts = [w_qkv, w_out, w_up, w_down]
    if not m.inside:
        pq = w_qkv.astype(BF).reshape(m.RD, 3, m.T, m.Q).transpose(2, 0, 1, 3)
        po = w_out.astype(BF).reshape(m.RD, m.T, m.Q).transpose(1, 0, 2)
        pu = w_up.astype(BF).reshape(m.RD, m.W, m.T, m.FD).transpose(2, 0, 1, 3)
        parts = [pq.reshape(m.T, m.RD, m.NQ), po, pu.reshape(m.T, m.RD, m.F)]
        parts = [
            lax.all_to_all(part, "narrow", 0, 0).reshape(m.RG, part.shape[2]) for part in parts
        ]
        parts.append(w_down.astype(BF))
    low = vectors.astype(BF).T
    spot = jnp.zeros((12, D), BF)
    spot = lax.dynamic_update_slice(spot, low, (0, first_row))
    rise = spot[8:].reshape(m.W, m.T, m.FD).transpose(1, 0, 2).reshape(m.T, m.F)
    rise = jnp.pad(rise, ((0, 8 - m.T), (0, D - m.F)))
    packed = jnp.concatenate([spot[:8], rise], axis=0)

    block_out, input_grad, gq, go, gu, gd, gv = block_step(
        m, (tokens, cotangent, segment_ids, *parts, packed)
    )
    if not m.inside:
        gq, go, gu = [
            lax.all_to_all(g.reshape(m.T, m.RD, g.shape[1]), "narrow", 0, 0) for g in (gq, go, gu)
        ]
    if m.FD % 128:
        gu = gu.reshape(m.T, m.RD, m.W, m.FD).transpose(1, 2, 0, 3).reshape(1, m.RD, FF)
    rise = gv[8 : 8 + m.T, : m.F].reshape(m.T, m.W, m.FD).transpose(1, 0, 2).reshape(FF // D, D)
    grad_vec = lax.dynamic_slice(
        jnp.concatenate([gv[:8], rise], axis=0), (0, first_row), (12, m.RD)
    ).T

    results = update_step(
        m,
        (gq, go, gu, gd.reshape(1, m.FD, D)),
        (w_qkv, w_out, w_up, w_down),
        (moments_qkv, moments_out, moments_up, moments_down),
        (block_out, input_grad),
    )
    new_qkv, state_qkv, copy_qkv, new_out, state_out, copy_out = results[:6]
    new_up, state_up, copy_up, new_down, state_down, copy_down = results[6:12]
    block_out, input_grad = results[12:]
    new_vectors, state_vectors, copy_vectors = adam_update(
        vectors, moments_vec, grad_vec, RATE_VECTOR, 0.0
    )
    return (
        block_out,
        input_grad,
        new_qkv,
        new_out,
        new_up,
        new_down,
        new_vectors,
        state_qkv,
        state_out,
        state_up,
        state_down,
        state_vectors,
        copy_qkv,
        copy_out,
        copy_up,
        copy_down,
        copy_vectors,
    )


def solution(mesh):
    flat = P(("wide", "narrow"), None)
    pair = P(None, ("wide", "narrow"), None)
    return jax.shard_map(
        body,
        mesh=mesh,
        in_specs=(flat,) * 8 + (pair,) * 5,
        out_specs=(flat,) * 7 + (pair,) * 5 + (flat,) * 5,
        check_vma=False,
    )
```

```python
import types

import jax
import jax.numpy as jnp
from jax import lax
from jax.experimental import pallas as pl
from jax.experimental.pallas import tpu as pltpu
from jax.sharding import PartitionSpec as P

D = 1024
HEADS = 16
FF = 4096
STEP = 3
HEAD = D // HEADS

NORM_EPSILON = 1e-06
MASK_VALUE = -1e30
MOMENT_DECAY = 0.5
RATE_MATRIX = 0.04
RATE_VECTOR = 0.2
WEIGHT_DECAY = 0.1
ADAM_EPSILON = 1e-08

BF = jnp.bfloat16
F32 = jnp.float32
MESH = pl.DeviceIdType.MESH


def adam_update(master, moments, gradient, rate, decay):
    first_moment = MOMENT_DECAY * moments[0] + (1.0 - MOMENT_DECAY) * gradient
    second_moment = MOMENT_DECAY * moments[1] + (1.0 - MOMENT_DECAY) * gradient * gradient
    correction = 1.0 - MOMENT_DECAY**STEP
    normalized = first_moment / correction / (jnp.sqrt(second_moment / correction) + ADAM_EPSILON)
    updated = master - rate * (normalized + decay * master)
    return (updated, jnp.stack([first_moment, second_moment]), updated.astype(BF))


def nn(left, right):
    return jnp.dot(left, right, preferred_element_type=F32)


def nt(left, right):
    return lax.dot_general(left, right, (((1,), (1,)), ((), ())), preferred_element_type=F32)


def tn(left, right):
    return lax.dot_general(left, right, (((0,), (0,)), ((), ())), preferred_element_type=F32)


def loop(count, body, first=0):
    def step(index, carry):
        body(index)
        return carry

    lax.fori_loop(first, first + count, step, 0)


def normalize(rows):
    center = rows - jnp.mean(rows, axis=-1, keepdims=True)
    inverse = lax.rsqrt(jnp.mean(center * center, axis=-1, keepdims=True) + NORM_EPSILON)
    return center * inverse, inverse


def norm_back(grad, unit, inverse, gain):
    scaled = grad * gain
    first = jnp.mean(scaled, axis=-1, keepdims=True)
    second = jnp.mean(scaled * unit, axis=-1, keepdims=True)
    return inverse * (scaled - first - unit * second)


def layout(wide, narrow, length):
    m = types.SimpleNamespace()
    m.W, m.T, m.S = wide, narrow, length
    m.Y = narrow // 2
    m.X = narrow // 2
    m.Z = wide // m.X
    m.L = length * narrow
    m.Q = D // narrow
    m.NQ = 3 * m.Q
    m.F = FF // narrow
    m.RG = D // wide
    m.RD = D // (wide * narrow)
    m.FD = FF // (wide * narrow)
    m.NH = m.Q // HEAD
    m.inside = m.RD % 16 == 0
    m.line = m.Z == 4
    m.compact = m.inside and m.RG == 128 and m.FD == 128
    m.V = m.RG if m.compact else D
    return m


def scratch_of(m):
    def weights(name, rows, cols):
        return {
            name: ((m.W, rows, cols), BF),
        }

    def scatter(name, rows, cols):
        return {
            "G" + name: ((m.W, rows, cols), BF),
            "X" + name: ((m.X - 1, m.Z, rows, cols), BF),
            "S" + name: ((m.Z, rows, cols), BF),
            "Z" + name: ((m.Z if m.line else m.Z - 1, rows, cols), BF),
        }

    def spread(name, cols):
        return {
            "T" + name: ((m.T, m.RD, cols), BF),
            "N" + name: ((m.T, m.RD, cols), BF),
        }

    def partial(name):
        return {
            "P" + name: ((m.L, D), BF),
            "C" + name: ((m.Y, m.S, D), BF),
            "M" + name: ((m.Y, m.S, D), BF),
            "A" + name: ((m.S, D), F32),
            "R" + name: ((m.Y - 1, m.S, D), BF),
        }

    out = {}
    out.update(weights("wq", m.RG, m.NQ))
    out["wo"] = ((m.T, m.W, m.RG, m.Q), BF)
    out.update(weights("wu", m.RG, m.F))
    out.update(weights("wd", m.FD, D))
    out.update(weights("wv", 16, m.V))
    out["vn"] = ((m.T - 1, 16, m.V), BF)
    out.update(scatter("q", m.RG, m.NQ))
    out.update(scatter("o", m.RG, m.Q))
    out.update(scatter("u", m.RG, m.F))
    out.update(scatter("d", m.FD, D))
    if m.inside:
        out["pq"] = ((m.T, m.RD, m.NQ), BF)
        out["po"] = ((m.T, m.RD, m.Q), BF)
        out["pu"] = ((m.T, m.RD, m.F), BF)
        out.update(spread("q", m.NQ))
        out.update(spread("o", m.Q))
        out.update(spread("u", m.F))
    for name in ("y", "c", "n"):
        out.update(partial(name))
    for name in ("tok", "dya", "ca"):
        out[name] = ((m.L, D), BF)
    out["oa"] = ((m.T, m.L, m.Q), BF)
    out["sg"] = ((m.T, 8, m.S), F32)
    out["vec"] = ((16, D), F32)
    out["bias"] = ((8, m.NQ), F32)
    out["a"] = ((m.L, D), BF)
    out["at"] = ((D, m.L), BF)
    out["ct"] = ((D, m.L), BF)
    out["ot"] = ((D, m.L), BF)
    out["h"] = ((m.L, m.F), BF)
    out["ht"] = ((m.F, m.L), BF)
    out["u"] = ((m.L, m.F), F32)
    out["du"] = ((m.L, m.F), BF)
    out["qkv"] = ((m.L, m.NQ), BF)
    out["dqkv"] = ((m.L, m.NQ), BF)
    out["prob"] = ((m.T * m.NH, m.S, m.S), F32)
    out["oo"] = ((m.S, D), BF)
    out["r1"] = ((m.S, D), F32)
    out["dr"] = ((m.S, D), F32)
    out["da"] = ((m.S, D), BF)
    out["dob"] = ((m.T, m.S, m.Q), BF)
    out["dab"] = ((m.T, m.S, m.Q), BF)
    out["dof"] = ((m.L, m.Q), BF)
    out["daq"] = ((m.L, m.Q), BF)
    out["sums"] = ((6, 16, D), F32)
    out["bo"] = ((m.S, D), BF)
    out["ig"] = ((m.S, D), F32)
    out["gq"] = ((m.T, m.RD, m.NQ) if m.inside else (m.RG, m.NQ), BF)
    out["go"] = ((m.T, m.RD, m.Q) if m.inside else (m.RG, m.Q), BF)
    out["gu"] = ((m.T, m.RD, m.F) if m.inside else (m.RG, m.F), BF)
    out["gd"] = ((m.FD, D), F32)
    out["gv"] = ((16, m.V), F32)
    out["vg"] = ((3, 16, D), F32)
    out["vb"] = ((3, 16, D), BF)
    out["vx"] = ((m.X - 1, 16, D), BF)
    out["vz"] = ((m.Z - 1, 16, D), BF)
    out["vt"] = ((m.T - 1, 16, D), BF)
    return out


def semaphores_of(m):
    gather = 2 * m.Z + m.Z * (m.X - 1)
    scatter = m.Z * (m.X - 1) + 2 * m.Z
    pair = (m.Y - 1) + m.Y
    direct = m.T - 1
    total = 5 * gather + 4 * scatter + 8 * pair + 10 * direct + (m.X - 1) + (m.Z - 1) + direct
    return 2 * total + 16


def block_kernel(m, names, *refs):
    inputs = ("x", "dy", "seg", "pq", "po", "pu", "pd", "pv")
    if m.inside:
        inputs = ("x", "dy", "seg", "fq", "fo", "fu", "fd", "pv")
    outputs = ("bo", "ig", "gq", "go", "gu", "gd", "gv")
    homes = tuple("h" + name for name in outputs)
    r = types.SimpleNamespace(**dict(zip(inputs + homes + tuple(names) + ("sem", "done"), refs)))

    def put(name):
        k = outputs.index(name)
        return pltpu.make_async_copy(getattr(r, name), getattr(r, "h" + name), r.done.at[k])

    w, n = lax.axis_index("wide"), lax.axis_index("narrow")
    z, x = w // m.X, lax.rem(w, m.X)
    y, c = n // 2, lax.rem(n, 2)
    sibling = (w, 2 * y + 1 - c)
    L, S, T, X, Y, Z = m.L, m.S, m.T, m.X, m.Y, m.Z
    sent = []
    used = [0]

    def fresh(count):
        first = used[0]
        used[0] += count
        return [first + k for k in range(count)]

    inner = (z == 1) | (z == 2)
    mate = jnp.where(z < 2, 1 - z, 5 - z)
    fin, fend = jnp.where(z < 2, 2, 1), jnp.where(z < 2, 3, 0)

    def copy(src, dst, device, index, out=None):
        return pltpu.make_async_remote_copy(
            src_ref=src,
            dst_ref=dst,
            send_sem=r.sem.at[2 * (index if out is None else out)],
            recv_sem=r.sem.at[2 * index + 1],
            device_id=device,
            device_id_type=MESH,
        )

    def send(src, dst, device, index, out=None, only=None):
        one = copy(src, dst, device, index, out)
        if only is None:
            one.start()
        else:
            pl.when(only)(one.start)
        sent.append((one, only))

    def drain(count):
        for one, only in sent[:count]:
            if only is None:
                one.wait_send()
            else:
                pl.when(only)(one.wait_send)
        del sent[:count]

    def arrive(dst, index):
        copy(dst, dst, sibling, index).wait_recv()

    def up_z(step):
        return lax.rem(z + step, Z)

    def down_z(step):
        return lax.rem(z + Z - step, Z)

    def up_x(step):
        return lax.rem(x + step, X)

    def down_x(step):
        return lax.rem(x + X - step, X)

    def up_n(step):
        return lax.rem(n + step, T)

    def down_n(step):
        return lax.rem(n + T - step, T)

    def at_y(step):
        return lax.rem(y + Y + step, Y)

    def rows_of(index, size):
        return pl.ds(pl.multiple_of(index * size, size), size)

    class Gather:
        def __init__(self, ref):
            self.ref = ref
            self.zi = fresh(Z - 1)[0]
            self.out = fresh(4)
            self.xi = fresh(Z * (X - 1))[0]

        def to_z(self, block, there, index, out, only=None):
            send(self.ref.at[block], self.ref.at[block], (there * X + x, n), self.zi + index, out, only)

        def along_z(self):
            if m.line:
                self.to_z(w, fin, jnp.where(inner, 1, 2), self.out[0])
                self.to_z(w, mate, 0, self.out[1])
                return
            for step in range(1, Z):
                self.to_z(w, up_z(step), step - 1, None)

        def forward(self, step, only=None):
            block = down_z(step) * X + x
            for dx in range(1, X):
                send(
                    self.ref.at[block],
                    self.ref.at[block],
                    (z * X + up_x(dx), n),
                    self.xi + step * (X - 1) + dx - 1,
                    only=only,
                )

        def relay(self, k, who):
            if not m.line and who == "end":
                return
            only = None
            if m.line:
                only = inner if who == "inner" else jnp.logical_not(inner)
            step, index = k, k - 1
            if m.line:
                index = jnp.where(inner, k % 3, k - 1)
                there = jnp.where(index == 0, mate, jnp.where(index == 1, fin, fend))
                step = lax.rem(z + Z - there, Z)
            block = down_z(step) * X + x
            if only is None:
                arrive(self.ref.at[block], self.zi + index)
            else:
                pl.when(only)(lambda: arrive(self.ref.at[block], self.zi + index))
            if m.line and k < 3 and who == "inner":
                self.to_z(block, mate, index, self.out[1 + k], inner)
            self.forward(step, only)

        def inside(self, steps):
            for k in steps:
                self.relay(k, "inner")

        def ends(self, steps):
            for k in steps:
                self.relay(k, "end")

        def finish(self):
            for step in range(Z):
                for dx in range(1, X):
                    block = (down_z(step) if step else z) * X + down_x(dx)
                    arrive(self.ref.at[block], self.xi + step * (X - 1) + dx - 1)

    class Share:
        def __init__(self, slot):
            self.slot = slot
            self.yi = fresh(Y - 1)
            self.ci = fresh(Y)

        def start(self):
            for step in range(1, Y):
                send(self.slot(n), self.slot(n), (w, 2 * at_y(step) + c), self.yi[step - 1])
            send(self.slot(n), self.slot(n), sibling, self.ci[0])

        def middle(self):
            for step in range(1, Y):
                block = 2 * at_y(-step) + c
                arrive(self.slot(block), self.yi[step - 1])
                send(self.slot(block), self.slot(block), sibling, self.ci[step])

        def close(self):
            for step in range(Y):
                block = 2 * at_y(-step) + 1 - c
                arrive(self.slot(block), self.ci[step])

    class Total:
        def __init__(self, name):
            self.part = getattr(r, "P" + name)
            self.core = getattr(r, "C" + name)
            self.mid = getattr(r, "M" + name)
            self.own = getattr(r, "A" + name)
            self.last = getattr(r, "R" + name)
            self.yi = fresh(Y - 1)
            self.ci = fresh(Y)

        def start(self):
            for step in list(range(1, Y)) + [0]:
                block = 2 * at_y(step) + 1 - c
                send(self.part.at[rows_of(block, S)], self.core.at[step], sibling, self.ci[step])

        def middle(self):
            for step in list(range(1, Y)) + [0]:
                block = 2 * at_y(step) + c
                arrive(self.core.at[step], self.ci[step])

                def add(i):
                    rows = rows_of(i, 16)
                    mine = self.part[pl.ds(pl.multiple_of(block * S + i * 16, 16), 16), :]
                    total = mine.astype(F32) + self.core[step, rows, :].astype(F32)
                    if step:
                        self.mid[step, rows, :] = total.astype(BF)
                    else:
                        self.own[rows, :] = total

                loop(S // 16, add)
                if step:
                    send(self.mid.at[step], self.last.at[step - 1], (w, block), self.yi[step - 1])

        def finish(self):
            for step in range(1, Y):
                arrive(self.last.at[step - 1], self.yi[step - 1])

        def rows(self, rows):
            total = self.own[rows, :]
            for step in range(1, Y):
                total = total + self.last[step - 1, rows, :].astype(F32)
            return total

    class Scatter:
        def __init__(self, name, rows, cols):
            self.rows, self.cols = rows, cols
            self.grad = getattr(r, "G" + name)
            self.fromx = getattr(r, "X" + name)
            self.sums = getattr(r, "S" + name)
            self.fromz = getattr(r, "Z" + name)
            self.xi = fresh(Z * (X - 1))
            self.zi = fresh(Z)[0]
            self.out = fresh(Z - 1)
            self.chunk = 16 if cols > 512 else 32
            if rows % self.chunk:
                self.chunk = 16

        def order(self):
            return list(range(Z))

        def there(self, k):
            if k == Z - 1:
                return z
            return (fin, fend, mate)[k] if m.line else up_z(k + 1)

        def multiply(self, k, left, right):
            first = self.there(k)
            high = X * self.rows
            tile = 256 if self.cols % 256 == 0 else 128

            def one(j):
                cols = rows_of(j, tile)
                value = nn(left[rows_of(first, high), :], right[:, cols]).astype(BF)
                value = value.reshape(X, self.rows, tile)
                self.grad[rows_of(first, X), :, cols] = value

            loop(self.cols // tile, one)

        def along_x(self, k):
            first = self.there(k)
            for dx in range(1, X):
                other = up_x(dx)
                send(
                    self.grad.at[first * X + other],
                    self.fromx.at[dx - 1, k],
                    (z * X + other, n),
                    self.xi[k * (X - 1) + dx - 1],
                )

        def along_z(self, k):
            block = self.there(k) * X + x
            for dx in range(1, X):
                arrive(self.fromx.at[dx - 1, k], self.xi[k * (X - 1) + dx - 1])

            def add(i):
                rows = rows_of(i, self.chunk)
                total = self.grad[block, rows, :].astype(F32)
                for dx in range(1, X):
                    total = total + self.fromx[dx - 1, k, rows, :].astype(F32)
                self.sums[k, rows, :] = total.astype(BF)

            loop(self.rows // self.chunk, add)
            if k == Z - 1:
                return
            if not m.line:
                self.to_z(k, block, k)
            elif k == 2:
                self.to_z(k, mate * X + x, 2)
            else:
                self.to_z(k, mate * X + x, k, z != jnp.where(z < 2, 1, 2))

        def to_z(self, k, block, slot, only=None):
            send(self.sums.at[k], self.fromz.at[slot], (block, n), self.zi + slot, self.out[k], only)

        def join(self, k):
            if not m.line:
                return

            @pl.when(inner)
            def _():
                arrive(self.fromz.at[k], self.zi + k)

                def add(i):
                    rows = rows_of(i, self.chunk)
                    total = self.sums[k, rows, :].astype(F32) + self.fromz[k, rows, :].astype(F32)
                    self.sums[k, rows, :] = total.astype(BF)

                loop(self.rows // self.chunk, add)
                copy(
                    self.sums.at[k], self.fromz.at[3], (self.there(k) * X + x, n), self.zi + 3, self.out[k]
                ).start()

            sent.append(
                (
                    copy(
                        self.sums.at[k], self.fromz.at[3], (self.there(k) * X + x, n), self.zi + 3, self.out[k]
                    ),
                    inner,
                )
            )

        def last(self):
            return [2, 3] if m.line else list(range(Z - 1))

        def finish(self):
            for slot in self.last():
                arrive(self.fromz.at[slot], self.zi + slot)

        def total(self, rows):
            total = self.sums[Z - 1, rows, :].astype(F32)
            for slot in self.last():
                total = total + self.fromz[slot, rows, :].astype(F32)
            return total

    class Deal:
        def __init__(self, name, scatter, out):
            self.scatter, self.out = scatter, out
            if m.inside:
                self.turn = getattr(r, "T" + name)
                self.got = getattr(r, "N" + name)
                self.ni = fresh(T - 1)

        def start(self):
            self.scatter.finish()
            if not m.inside:
                def store(i):
                    rows = rows_of(i, self.scatter.chunk)
                    self.out[rows, :] = self.scatter.total(rows).astype(BF)

                loop(self.scatter.rows // self.scatter.chunk, store)
                return

            def add(i):
                self.turn[i] = self.scatter.total(rows_of(i, m.RD)).astype(BF)

            loop(T, add)
            for step in range(1, T):
                other = up_n(step)
                send(self.turn.at[other], self.got.at[step], (w, other), self.ni[step - 1])

        def finish(self):
            if not m.inside:
                return
            self.out[n] = self.turn[n]
            for step in range(1, T):
                arrive(self.got.at[step], self.ni[step - 1])
                self.out[down_n(step)] = self.got[step]

    def transpose(target, source, count_rows, count_cols):
        def tile(k):
            i, j = k // count_cols, lax.rem(k, count_cols)
            target[rows_of(j, 128), rows_of(i, 128)] = source(rows_of(i, 128), rows_of(j, 128)).T

        loop(count_rows * count_cols, tile)

    if m.inside:
        for k in range(T):
            r.po[k] = r.fo[:, k * m.Q : (k + 1) * m.Q].astype(BF)
            for b in range(3):
                first = b * D + k * m.Q
                r.pq[k, :, b * m.Q : (b + 1) * m.Q] = r.fq[:, first : first + m.Q].astype(BF)
            for j in range(m.W):
                first = (j * T + k) * m.FD
                r.pu[k, :, j * m.FD : (j + 1) * m.FD] = r.fu[:, first : first + m.FD].astype(BF)

    barrier = pltpu.get_barrier_semaphore()
    peers = [(w, up_n(k)) for k in range(1, T)]
    peers += [(up_z(k) * X + x, n) for k in range(1, Z)]
    peers += [(z * X + up_x(k), n) for k in range(1, X)]
    for peer in peers:
        pl.semaphore_signal(barrier, inc=1, device_id=peer, device_id_type=MESH)
    pl.semaphore_wait(barrier, len(peers))

    gv, gq, gu, gd = Gather(r.wv), Gather(r.wq), Gather(r.wu), Gather(r.wd)
    go = Gather(r.wo.at[n])
    tokens = Share(lambda k: r.tok.at[rows_of(k, S)])
    cotangents = Share(lambda k: r.dya.at[rows_of(k, S)])
    outs = Share(lambda k: r.wo.at[k])
    mixes = Share(lambda k: r.oa.at[k])
    seconds = Share(lambda k: r.ca.at[rows_of(k, S)])
    ty, tc, tin = Total("y"), Total("c"), Total("n")
    sd, su = Scatter("d", m.FD, D), Scatter("u", m.RG, m.F)
    so, sq = Scatter("o", m.RG, m.Q), Scatter("q", m.RG, m.NQ)

    vi, si = fresh(T - 1), fresh(T - 1)
    for step in range(1, T):
        send(r.pv, r.vn.at[step - 1], (w, up_n(step)), vi[step - 1])
    r.wd[w] = r.fd[...].astype(BF) if m.inside else r.pd[...]
    gd.forward(0)

    class Rows:
        def __init__(self, part, target):
            self.part, self.target = part, target
            self.ids = fresh(T - 1) if m.inside else []

        def at(self, k, rows):
            return r.wo.at[k, w, rows] if self.target is None else self.target.at[w, rows]

        def start(self):
            if m.inside:
                own = pl.ds(pl.multiple_of(n * m.RD, m.RD), m.RD)
                for step in range(1, T):
                    other = up_n(step)
                    send(self.part.at[other], self.at(other, own), (w, other), self.ids[step - 1])
                self.at(n, own)[...] = self.part[n]
            elif self.target is None:
                r.wo[n, w] = self.part[...]
            else:
                self.target[w] = self.part[...]

        def finish(self):
            if m.inside:
                for step in range(1, T):
                    got = pl.ds(pl.multiple_of(down_n(step) * m.RD, m.RD), m.RD)
                    arrive(self.at(n, got), self.ids[step - 1])

    ro, rq, ru = Rows(r.po, None), Rows(r.pq, r.wq), Rows(r.pu, r.wu)
    ro.start()
    rq.start()
    own_rows = rows_of(n, S)
    r.tok[own_rows, :] = r.x[...]
    tokens.start()
    r.sg[n] = jnp.broadcast_to(r.seg[...].astype(F32), (8, S))
    for step in range(1, T):
        send(r.sg.at[n], r.sg.at[n], (w, up_n(step)), si[step - 1])
    ru.start()
    r.dya[own_rows, :] = r.dy[...]
    cotangents.start()

    vector = r.pv[...].astype(F32)
    for step in range(1, T):
        arrive(r.vn.at[step - 1], vi[step - 1])
        vector = vector + r.vn[step - 1].astype(F32)
    r.wv[w] = vector.astype(BF)
    early, late = range(1, Z - 1), range(Z - 1, Z)
    gv.along_z()
    gv.forward(0)
    ro.finish()
    go.along_z()
    go.forward(0)
    gv.inside(early)
    rq.finish()
    gq.along_z()
    gq.forward(0)
    go.inside(early)
    tokens.middle()
    ru.finish()
    gv.inside(late)
    gv.ends(range(1, Z))
    tokens.close()
    gv.finish()
    if m.compact:
        for k in range(m.W):
            vector = r.wv[k].astype(F32)
            r.vec[0:8, k * m.V : (k + 1) * m.V] = vector[0:8]
            for part in range(FF // D):
                first = (part * (D // (T * m.FD)) + k // T) * m.FD
                r.vec[8 + k % T : 9 + k % T, first : first + m.FD] = vector[8 + part : 9 + part]
    else:
        vector = r.wv[0].astype(F32)
        for k in range(1, m.W):
            vector = vector + r.wv[k].astype(F32)
        r.vec[...] = vector

    heads = rows_of(n, m.Q)
    r.bias[...] = jnp.zeros_like(r.bias)
    r.bias[0:1, 0 : m.Q] = r.vec[2:3, heads]
    r.bias[0:1, 2 * m.Q : 3 * m.Q] = r.vec[3:4, heads]

    def first_norm(i):
        rows = rows_of(i, 16)
        unit, _ = normalize(r.tok[rows, :].astype(F32))
        r.a[rows, :] = (unit * r.vec[0:1, :] + r.vec[1:2, :]).astype(BF)

    half = L // 32
    gq.inside(early)
    gu.along_z()
    go.inside(late)
    go.ends(range(1, Z))
    loop(half, first_norm)
    cotangents.middle()
    gq.inside(late)
    gq.ends(range(1, 2))
    go.finish()
    outs.start()
    loop(half, first_norm, half)
    gq.ends(range(2, Z - 1))
    transpose(r.at, lambda i, j: r.a[i, j], L // 128, D // 128)
    gq.ends(late)
    gu.forward(0)
    cotangents.close()
    gq.finish()

    tile_q = 256 if m.NQ % 256 == 0 else 128

    def project(j):
        cols = rows_of(j, tile_q)
        value = nn(r.a[...], r.wq[:, :, cols].reshape(D, tile_q)) + r.bias[0:1, cols]
        r.qkv[:, cols] = value.astype(BF)

    loop(m.NQ // tile_q, project)
    for step in range(1, T):
        arrive(r.sg.at[down_n(step)], si[step - 1])
    gu.inside(early)
    gd.along_z()
    gu.ends(range(1, 2))
    outs.middle()

    lane = lax.broadcasted_iota(jnp.int32, (1, 128), 1)
    halves = [(lane // HEAD == k).astype(F32) for k in range(128 // HEAD)]
    scale = HEAD ** (-0.5)
    per = 128 // HEAD

    def pick(values):
        total = values[0] * halves[0]
        for k in range(1, per):
            total = total + values[k] * halves[k]
        return total

    def attend(s):
        rows = rows_of(s, S)
        keys = jnp.broadcast_to(r.sg[s, 0:1, :], (S, S))
        same = keys == keys.T
        for pair in range(m.Q // 128):
            q = r.qkv[rows, pair * 128 : pair * 128 + 128]
            k = r.qkv[rows, m.Q + pair * 128 : m.Q + pair * 128 + 128]
            v = r.qkv[rows, 2 * m.Q + pair * 128 : 2 * m.Q + pair * 128 + 128]
            mixed = []
            for half in range(per):
                score = nt(q * halves[half].astype(BF), k) * scale
                score = jnp.where(same, score, MASK_VALUE)
                power = jnp.exp(score - jnp.max(score, axis=-1, keepdims=True))
                weight = power / jnp.sum(power, axis=-1, keepdims=True)
                r.prob[s * m.NH + pair * per + half] = weight
                mixed.append(nn(weight.astype(BF), v))
            r.oa[n, rows, pair * 128 : pair * 128 + 128] = pick(mixed).astype(BF)

    loop(T, attend)
    mixes.start()
    gu.inside(late)
    gu.ends(range(2, Z - 1))
    outs.close()
    mixes.middle()
    gd.inside(early)
    gu.ends(late)
    mixes.close()

    for t in range(T):
        r.oo[:, t * m.Q : (t + 1) * m.Q] = r.oa[t, own_rows, :]
    for t in range(T):
        cols = slice(t * m.Q, (t + 1) * m.Q)
        value = nn(r.oo[...], r.wo[t].reshape(D, m.Q))
        r.r1[:, cols] = r.x[:, cols].astype(F32) + value + r.vec[4:5, cols]

    def second_norm(i):
        rows = rows_of(i, 16)
        unit, _ = normalize(r.r1[rows, :])
        there = pl.ds(pl.multiple_of(n * S + i * 16, 16), 16)
        r.ca[there, :] = (unit * r.vec[5:6, :] + r.vec[6:7, :]).astype(BF)

    loop(S // 16, second_norm)
    seconds.start()
    gd.ends(range(1, 2))
    for t in range(T):
        for k in range(m.Q // 128):
            base = t * m.Q + k * 128

            def turn(i, t=t, k=k, base=base):
                value = r.oa[t, rows_of(i, 128), k * 128 : k * 128 + 128].astype(F32)
                r.ot[base : base + 128, rows_of(i, 128)] = value.T.astype(BF)

            loop(L // 128, turn)
    seconds.middle()
    seconds.close()
    gd.inside(late)
    gd.ends(range(2, Z - 1))
    gu.finish()

    def expand(j):
        cols = rows_of(j, 256)
        value = nn(r.ca[...], r.wu[:, :, cols].reshape(D, 256))
        r.u[:, cols] = value + r.vec[pl.ds(8 + n, 1), cols]

    loop(m.F // 256, expand)

    def activate(i):
        rows = rows_of(i, 16)
        value = r.u[rows, :]
        phi = 0.5 * (1.0 + lax.erf(value * (0.5**0.5)))
        r.h[rows, :] = (value * phi).astype(BF)
        r.u[rows, :] = phi + value * (jnp.exp(-0.5 * value * value) * 0.3989422804014327)

    loop(L // 16, activate)
    gd.ends(late)
    transpose(r.ht, lambda i, j: r.h[i, j], L // 128, m.F // 128)
    sd.multiply(sd.order()[0], r.ht, r.dya)
    sd.along_x(sd.order()[0])
    for step in sd.order()[1:]:
        sd.multiply(step, r.ht, r.dya)
        sd.along_x(step)
    transpose(r.ct, lambda i, j: r.ca[i, j], L // 128, D // 128)
    sd.along_z(0)
    gd.finish()
    early_sends = len(sent)

    group = 256 // m.FD

    def expand_back(j):
        cols = rows_of(j, 256)
        value = nt(r.dya[...], r.wd[rows_of(j, group)].reshape(256, D)) * r.u[:, cols]
        low = value.astype(BF)
        r.du[:, cols] = low
        r.sums[5, 0:1, cols] = jnp.sum(low.astype(F32), axis=0, keepdims=True)

    loop(m.F // 256, expand_back)
    width = 256 // m.RG

    def up_back(j):
        value = nt(r.du[...], r.wu[rows_of(j, width)].reshape(256, m.F))
        r.Pc[:, rows_of(j, 256)] = value.astype(BF)

    loop(D // 256, up_back)
    tc.start()
    for step in su.order():
        su.multiply(step, r.ct, r.du)
        su.along_x(step)
    tc.middle()

    def contract(j):
        cols = rows_of(j, 256)
        r.Py[:, cols] = nn(r.h[...], r.wd[:, :, cols].reshape(m.F, 256)).astype(BF)

    loop(D // 256, contract)
    ty.start()
    sd.along_z(1)
    tc.finish()
    r.sums[0:4] = jnp.zeros((4, 16, D), F32)

    def second_back(i):
        rows = rows_of(i, 16)
        grad = tc.rows(rows)
        cot = r.dy[rows, :].astype(F32)
        unit, inverse = normalize(r.r1[rows, :])
        total = cot + norm_back(grad, unit, inverse, r.vec[5:6, :])
        r.dr[rows, :] = total
        r.da[rows, :] = total.astype(BF)
        r.sums[0] += total
        r.sums[1] += grad * unit
        r.sums[2] += grad
        r.sums[3] += cot

    loop(S // 16, second_back)
    oi, ai = fresh(T - 1), fresh(T - 1)
    share = m.Q // m.RG
    for step in list(range(1, T)) + [0]:
        other = up_n(step) if step else n
        value = jnp.zeros((S, m.Q), F32)
        for t in range(T):
            block = r.wo[t, rows_of(other, share)].reshape(m.Q, m.Q)
            value = value + nt(r.da[:, t * m.Q : (t + 1) * m.Q], block)
        if step:
            r.dob[step] = value.astype(BF)
            send(r.dob.at[step], r.dof.at[own_rows], (w, other), oi[step - 1])
        else:
            r.dof[own_rows, :] = value.astype(BF)
    for step in range(1, T):
        other = up_n(step)
        r.dab[step] = r.da[:, rows_of(other, m.Q)]
        send(r.dab.at[step], r.daq.at[own_rows], (w, other), ai[step - 1])
    r.daq[own_rows, :] = r.da[:, rows_of(n, m.Q)]
    for step in sd.order()[2:-1]:
        sd.along_z(step)
    sd.join(0)
    for step in range(1, T):
        arrive(r.dof.at[rows_of(down_n(step), S)], oi[step - 1])

    def attend_back(s):
        rows = rows_of(s, S)
        for pair in range(m.Q // 128):
            at = [pl.ds(b * m.Q + pair * 128, 128) for b in range(3)]
            q, k, v = r.qkv[rows, at[0]], r.qkv[rows, at[1]], r.qkv[rows, at[2]]
            cot = r.dof[rows, pair * 128 : pair * 128 + 128]
            dq, dk, dv = [], [], []
            for half in range(per):
                weight = r.prob[s * m.NH + pair * per + half]
                grad = nt(cot * halves[half].astype(BF), v)
                inner = jnp.sum(weight * grad, axis=-1, keepdims=True)
                ds = (weight * (grad - inner)).astype(BF)
                dq.append(nn(ds, k))
                dk.append(tn(ds, q))
                dv.append(tn(weight.astype(BF), cot))
            r.dqkv[rows, at[0]] = (pick(dq) * scale).astype(BF)
            r.dqkv[rows, at[1]] = (pick(dk) * scale).astype(BF)
            r.dqkv[rows, at[2]] = pick(dv).astype(BF)

    loop(T // 2, attend_back)
    su.along_z(su.order()[0])
    loop(T - T // 2, attend_back, T // 2)
    sd.along_z(sd.order()[-1])
    sd.join(1)
    ty.middle()

    def project_back(j):
        value = nt(r.dqkv[...], r.wq[rows_of(j, width)].reshape(256, m.NQ))
        r.Pn[:, rows_of(j, 256)] = value.astype(BF)

    loop(D // 256, project_back)
    tin.start()
    for step in range(1, T):
        arrive(r.daq.at[rows_of(down_n(step), S)], ai[step - 1])
    tin.middle()
    su.along_z(1)
    for step in sq.order():
        sq.multiply(step, r.at, r.dqkv)
        sq.along_x(step)
    for step in su.order()[2:-1]:
        su.along_z(step)
    su.join(0)

    r.vg[0] = jnp.zeros((16, D), F32)
    for k, row in enumerate((4, 5, 6, 7)):
        r.vg[0, row : row + 1, :] = jnp.sum(r.sums[k], axis=0, keepdims=True)
    r.vg[0, pl.ds(8 + n, 1), 0 : m.F] = r.sums[5, 0:1, 0 : m.F]

    def column(j):
        cols = rows_of(j, 128)
        there = pl.ds(pl.multiple_of(n * m.Q + j * 128, 128), 128)
        tail = pl.ds(pl.multiple_of(2 * m.Q + j * 128, 128), 128)
        r.vg[0, 2:3, there] = jnp.sum(r.dqkv[:, cols].astype(F32), axis=0, keepdims=True)
        r.vg[0, 3:4, there] = jnp.sum(r.dqkv[:, tail].astype(F32), axis=0, keepdims=True)

    loop(m.Q // 128, column)
    tin.finish()
    r.sums[0:2] = jnp.zeros((2, 16, D), F32)

    def first_back(i):
        rows = rows_of(i, 16)
        grad = tin.rows(rows)
        unit, inverse = normalize(r.x[rows, :].astype(F32))
        r.ig[rows, :] = r.dr[rows, :] + norm_back(grad, unit, inverse, r.vec[0:1, :])
        r.sums[0] += grad * unit
        r.sums[1] += grad

    loop(S // 16, first_back)
    put("ig").start()
    r.vg[0, 0:1, :] = jnp.sum(r.sums[0], axis=0, keepdims=True)
    r.vg[0, 1:2, :] = jnp.sum(r.sums[1], axis=0, keepdims=True)
    r.vb[0] = r.vg[0].astype(BF)
    vxi, vzi, vti = fresh(X - 1), fresh(Z - 1), fresh(T - 1)
    for dx in range(1, X):
        send(r.vb.at[0], r.vx.at[dx - 1], (z * X + up_x(dx), n), vxi[dx - 1])

    for step in so.order():
        so.multiply(step, r.ot, r.daq)
        so.along_x(step)
    su.join(1)
    su.along_z(su.order()[-1])
    ty.finish()

    def close(i):
        rows = rows_of(i, 16)
        r.bo[rows, :] = (r.r1[rows, :] + ty.rows(rows) + r.vec[7:8, :]).astype(BF)

    loop(S // 16, close)
    put("bo").start()
    drain(early_sends)
    sd.finish()

    def keep(i):
        rows = rows_of(i, 16)
        r.gd[rows, :] = sd.total(rows)

    loop(m.FD // 16, keep)
    put("gd").start()
    du, do, dq = Deal("u", su, r.gu), Deal("o", so, r.go), Deal("q", sq, r.gq)
    for step in sq.order()[:2]:
        sq.along_z(step)
    sq.join(0)
    for step in sq.order()[2:-1]:
        sq.along_z(step)
    sq.join(1)
    du.start()
    sq.along_z(Z - 1)
    for step in so.order()[:-1]:
        so.along_z(step)
    so.join(0)
    so.join(1)
    so.along_z(Z - 1)
    total = r.vg[0]
    for dx in range(1, X):
        arrive(r.vx.at[dx - 1], vxi[dx - 1])
        total = total + r.vx[dx - 1].astype(F32)
    r.vg[1] = total
    r.vb[1] = total.astype(BF)
    for step in range(1, Z):
        send(r.vb.at[1], r.vz.at[step - 1], (up_z(step) * X + x, n), vzi[step - 1])
    dq.start()
    do.start()
    total = r.vg[1]
    for step in range(1, Z):
        arrive(r.vz.at[step - 1], vzi[step - 1])
        total = total + r.vz[step - 1].astype(F32)
    r.vg[2] = total
    r.vb[2] = total.astype(BF)
    for step in range(1, T):
        send(r.vb.at[2], r.vt.at[step - 1], (w, up_n(step)), vti[step - 1])
    du.finish()
    put("gu").start()
    dq.finish()
    put("gq").start()
    do.finish()
    put("go").start()
    total = r.vg[2]
    for step in range(1, T):
        arrive(r.vt.at[step - 1], vti[step - 1])
        total = total + r.vt[step - 1].astype(F32)
    if m.compact:
        r.vg[0] = total
        r.gv[...] = jnp.zeros_like(r.gv)
        r.gv[0:8, :] = r.vg[0, 0:8, rows_of(w, m.V)]
        for part in range(FF // D):
            block = part * (D // (T * m.FD)) + w // T
            several = r.vg[0, 8:16, rows_of(block, m.FD)]
            row = lax.broadcasted_iota(jnp.int32, several.shape, 0)
            mine = jnp.where(row == lax.rem(w, T), several, 0.0)
            r.gv[8 + part : 9 + part, :] = jnp.sum(mine, axis=0, keepdims=True)
    else:
        r.gv[...] = total
    put("gv").start()
    drain(len(sent))
    for name in outputs:
        put(name).wait()


def block_step(m, args):
    scratch = scratch_of(m)
    kept = {"q": m.NQ, "o": m.Q, "u": m.F}
    grads = [
        jax.ShapeDtypeStruct((m.T, m.RD, cols) if m.inside else (m.RG, cols), BF)
        for cols in kept.values()
    ]
    vmem = pl.BlockSpec(memory_space=pltpu.VMEM)

    def kernel(*refs):
        block_kernel(m, list(scratch), *refs)

    return pl.pallas_call(
        kernel,
        out_shape=[
            jax.ShapeDtypeStruct((m.S, D), BF),
            jax.ShapeDtypeStruct((m.S, D), F32),
            *grads,
            jax.ShapeDtypeStruct((m.FD, D), F32),
            jax.ShapeDtypeStruct((16, m.V), F32),
        ],
        in_specs=[vmem] * len(args),
        out_specs=[pl.BlockSpec(memory_space=pl.ANY)] * 7,
        scratch_shapes=[pltpu.VMEM(shape, kind) for shape, kind in scratch.values()]
        + [pltpu.SemaphoreType.DMA((semaphores_of(m),)), pltpu.SemaphoreType.DMA((7,))],
        compiler_params=pltpu.CompilerParams(
            collective_id=0, has_side_effects=True, vmem_limit_bytes=62 * 1024 * 1024
        ),
        name="block_step",
    )(*args)


def update_kernel(pieces, passed, *refs):
    count = len(pieces)
    ins, outs = refs[: 3 * count + passed], refs[3 * count + passed :]
    for k, parts in enumerate(pieces):
        grad, master, moments = ins[3 * k : 3 * k + 3]
        new, state, low = outs[3 * k : 3 * k + 3]
        rows = min(16, master.shape[0])

        def one(i, parts=parts, grad=grad, master=master, moments=moments, new=new, state=state, low=low, rows=rows):
            own = pl.ds(pl.multiple_of(i * rows, rows), rows)
            for block, source, column, width in parts:
                cols = pl.ds(column, width)
                value = grad[block, own, pl.ds(source, width)].astype(F32)
                first = MOMENT_DECAY * moments[0, own, cols] + (1.0 - MOMENT_DECAY) * value
                second = MOMENT_DECAY * moments[1, own, cols] + (1.0 - MOMENT_DECAY) * value * value
                correction = 1.0 - MOMENT_DECAY**STEP
                scaled = first / correction / (jnp.sqrt(second / correction) + ADAM_EPSILON)
                old = master[own, cols]
                updated = old - RATE_MATRIX * (scaled + WEIGHT_DECAY * old)
                new[own, cols] = updated
                state[0, own, cols] = first
                state[1, own, cols] = second
                low[own, cols] = updated.astype(BF)

        loop(master.shape[0] // rows, one)
    for source, target in zip(ins[3 * count :], outs[3 * count :]):
        target[...] = source[...]


def update_step(m, grads, masters, moments, passed):
    pieces = [
        [(t, b * m.Q, b * D + t * m.Q, m.Q) for b in range(3) for t in range(m.T)],
        [(t, 0, t * m.Q, m.Q) for t in range(m.T)],
        [(t, k * m.FD, (k * m.T + t) * m.FD, m.FD) for t in range(m.T) for k in range(m.W)],
        [(0, k * 256, k * 256, 256) for k in range(D // 256)],
    ]
    if m.FD % 128:
        pieces[2] = [(0, k * 256, k * 256, 256) for k in range(FF // 256)]
    steps = 2 if m.RD % 32 == 0 else 1
    args, specs, outs, out_specs = [], [], [], []

    def spec(shape):
        axis = len(shape) - 2
        block = tuple(s // steps if k == axis else s for k, s in enumerate(shape))
        return pl.BlockSpec(block, lambda i: tuple(i if k == axis else 0 for k in range(axis + 2)))

    for grad, master, moment in zip(grads, masters, moments):
        args += [grad, master, moment]
        specs += [spec(a.shape) for a in (grad, master, moment)]
        for shape, kind in ((master.shape, F32), (moment.shape, F32), (master.shape, BF)):
            outs.append(jax.ShapeDtypeStruct(shape, kind))
            out_specs.append(spec(shape))
    for one in passed:
        args.append(one)
        specs.append(spec(one.shape))
        outs.append(jax.ShapeDtypeStruct(one.shape, one.dtype))
        out_specs.append(spec(one.shape))

    def kernel(*refs):
        update_kernel(pieces, len(passed), *refs)

    return pl.pallas_call(
        kernel,
        grid=(steps,),
        out_shape=outs,
        in_specs=specs,
        out_specs=out_specs,
        name="update_step",
    )(*args)


def body(
    tokens,
    cotangent,
    segment_ids,
    w_qkv,
    w_out,
    w_up,
    w_down,
    vectors,
    moments_qkv,
    moments_out,
    moments_up,
    moments_down,
    moments_vec,
):
    wide, narrow = lax.axis_size("wide"), lax.axis_size("narrow")
    m = layout(wide, narrow, tokens.shape[0])
    device = lax.axis_index("wide") * narrow + lax.axis_index("narrow")
    first_row = device * m.RD

    parts = [w_qkv, w_out, w_up, w_down]
    if not m.inside:
        pq = w_qkv.astype(BF).reshape(m.RD, 3, m.T, m.Q).transpose(2, 0, 1, 3)
        po = w_out.astype(BF).reshape(m.RD, m.T, m.Q).transpose(1, 0, 2)
        pu = w_up.astype(BF).reshape(m.RD, m.W, m.T, m.FD).transpose(2, 0, 1, 3)
        parts = [pq.reshape(m.T, m.RD, m.NQ), po, pu.reshape(m.T, m.RD, m.F)]
        parts = [
            lax.all_to_all(part, "narrow", 0, 0).reshape(m.RG, part.shape[2]) for part in parts
        ]
        parts.append(w_down.astype(BF))
    low = vectors.astype(BF).T
    place = lax.axis_index("narrow") * m.RD if m.compact else first_row
    spot = lax.dynamic_update_slice(jnp.zeros((16, m.V), BF), low, (0, place))
    packed = spot
    if not m.compact:
        rise = spot[8:12].reshape(m.W, m.T, m.FD).transpose(1, 0, 2).reshape(m.T, m.F)
        rise = jnp.pad(rise, ((0, 8 - m.T), (0, D - m.F)))
        packed = jnp.concatenate([spot[:8], rise], axis=0)

    block_out, input_grad, gq, go, gu, gd, gv = block_step(
        m, (tokens, cotangent, segment_ids, *parts, packed)
    )
    if not m.inside:
        gq, go, gu = [
            lax.all_to_all(g.reshape(m.T, m.RD, g.shape[1]), "narrow", 0, 0) for g in (gq, go, gu)
        ]
    if m.FD % 128:
        gu = gu.reshape(m.T, m.RD, m.W, m.FD).transpose(1, 2, 0, 3).reshape(1, m.RD, FF)
    if not m.compact:
        rise = gv[8 : 8 + m.T, : m.F].reshape(m.T, m.W, m.FD).transpose(1, 0, 2).reshape(FF // D, D)
        gv = jnp.concatenate([gv[:8], rise], axis=0)
    grad_vec = lax.dynamic_slice(gv, (0, place), (12, m.RD)).T

    results = update_step(
        m,
        (gq, go, gu, gd.reshape(1, m.FD, D)),
        (w_qkv, w_out, w_up, w_down),
        (moments_qkv, moments_out, moments_up, moments_down),
        (block_out, input_grad),
    )
    new_qkv, state_qkv, copy_qkv, new_out, state_out, copy_out = results[:6]
    new_up, state_up, copy_up, new_down, state_down, copy_down = results[6:12]
    block_out, input_grad = results[12:]
    new_vectors, state_vectors, copy_vectors = adam_update(
        vectors, moments_vec, grad_vec, RATE_VECTOR, 0.0
    )
    return (
        block_out,
        input_grad,
        new_qkv,
        new_out,
        new_up,
        new_down,
        new_vectors,
        state_qkv,
        state_out,
        state_up,
        state_down,
        state_vectors,
        copy_qkv,
        copy_out,
        copy_up,
        copy_down,
        copy_vectors,
    )


def solution(mesh):
    flat = P(("wide", "narrow"), None)
    pair = P(None, ("wide", "narrow"), None)
    return jax.shard_map(
        body,
        mesh=mesh,
        in_specs=(flat,) * 8 + (pair,) * 5,
        out_specs=(flat,) * 7 + (pair,) * 5 + (flat,) * 5,
        check_vma=False,
    )
```
